128 devices in a mesh: slab: 32 (over y, x, core), probe: 4 (over z).
Axes of the slice: x: 4, y: 4, z: 4, core: 2. Of those that a mesh axis runs over, the one named last changes fastest.
Arguments:
- probe_fields: bfloat16 [256, 128, 8192], P('probe', 'slab'), may hold values from -6 to 6
- sensor_rows: int32 [4096], replicated, may hold values from 0 to 126, as said below
- sensor_cols: int32 [4096], replicated, may hold values from 0 to 8190
- row_frac: float32 [4096], replicated, may hold values from 0 to 1
- col_frac: float32 [4096], replicated, may hold values from 0 to 1
- sensor_weights: float32 [4096], replicated, may hold values from 0.05 to 1
- owner_order: int32 [4096], replicated, may hold values from 0 to 4095, as said below
Outputs:
- adjoint_sources: bfloat16 [256, 128, 8192], P('probe', 'slab')
- observed: float32 [256, 4096], P('probe', 'slab')
- trace_mean: float32 [], replicated
The draws below stay inside these ranges and needn't reach their ends.
Inputs may be any that keep to these rules, and one draw needn't show every extreme that they name: `sensor_rows`: rows run from 0 to 126. The sensors whose row lies in one slab of 4 rows number at most 512, and some slab holds exactly 512. `owner_order`: A permutation. The 4096 // 32 slots of one owner name at most 16 sensors whose row lies in any one slab, and every owner reaches 16 for some slab.
All inputs are finite; a program needn't handle non-finite values.
Results may differ from the reference program's by a relative error of at most 0.0068.
Values sent between devices are 32-bit elements; how exact they have to be, the bound alone decides.
A program may use at most 64 MiB of HBM per device.

```python
import math
import jax
import jax.numpy as jnp
from jax import lax

ROWS_DEV = 4
NCOL = 8192
SENSORS = 4096
NX = 128
PROBES = 256


def sensor_layout(key):
    slab_total = NX // ROWS_DEV
    slab_most = 4 * SENSORS // slab_total
    own_count = SENSORS // slab_total
    busiest = jax.random.randint(jax.random.fold_in(key, 11), (), 0, slab_total)
    position = jnp.arange(SENSORS, dtype=jnp.int32)
    others = (position - slab_most) % (slab_total - 1)
    others = others + (others >= busiest).astype(jnp.int32)
    slab_seq = jnp.sort(jnp.where(position < slab_most, busiest, others))
    row_inside = jax.random.randint(jax.random.fold_in(key, 12), (SENSORS,), 0, ROWS_DEV)
    row_inside = jnp.where((slab_seq == slab_total - 1) & (row_inside == ROWS_DEV - 1), row_inside - 1, row_inside)
    rows_seq = (slab_seq * ROWS_DEV + row_inside).astype(jnp.int32)
    sensor_ids = jax.random.permutation(jax.random.fold_in(key, 13), SENSORS).astype(jnp.int32)
    sensor_rows = jnp.zeros((SENSORS,), jnp.int32).at[sensor_ids].set(rows_seq)
    owner_perm = jax.random.permutation(jax.random.fold_in(key, 14), slab_total).astype(jnp.int32)
    shuffle = jax.random.permutation(jax.random.fold_in(key, 15), own_count).astype(jnp.int32)
    rotate = jax.random.randint(jax.random.fold_in(key, 16), (slab_total,), 0, own_count)
    owner_of = owner_perm[position % slab_total]
    inside = (shuffle[position // slab_total] + rotate[owner_of]) % own_count
    slot_of = (owner_of * own_count + inside).astype(jnp.int32)
    owner_order = jnp.zeros((SENSORS,), jnp.int32).at[slot_of].set(sensor_ids)
    return (sensor_rows, owner_order)


def draw_sensor_rows(key, part):
    return sensor_layout(key)[0]


def draw_owner_order(key, part):
    return sensor_layout(key)[1]


def with_ends(result, key, low, top_value):
    longest = result.shape.index(max(result.shape))
    spots = []
    for shift in (0, 1):
        where = [jax.random.randint(jax.random.fold_in(key, axis), (), 0, length) for axis, length in enumerate(result.shape)]
        where[longest] = (where[longest] + shift) % result.shape[longest]
        spots.append(tuple(where))
    return result.at[spots[0]].set(low).at[spots[1]].set(top_value)


def block_levels(rng, dims, split, least, high):
    def one(dim, shards_of):
        steps = jax.random.uniform(jax.random.fold_in(jax.random.fold_in(rng, 6), dim), (shards_of,), jnp.float32, least / len(split), high / len(split))
        return jnp.repeat(jnp.exp(steps), dims[dim] // shards_of).reshape((-1,) + (1,) * (len(dims) - dim - 1))

    loudness = one(*split[0])
    for cut in split[1:]:
        loudness = loudness * one(*cut)
    return loudness


def bell_draw(rng, extent, scale, most, pieces=(), kind=jnp.bfloat16):
    level = block_levels(rng, extent, pieces, -0.22, 0.18) if pieces else 1.0
    entries = jax.random.normal(rng, extent, jnp.float32) * scale * level
    return jnp.minimum(jnp.maximum(entries, -most), most).astype(kind)


def setup_inputs(seed: int = 0) -> dict:
    keys = jax.random.split(jax.random.key(seed), 8)
    return {
        "probe_fields": bell_draw(keys[0], (PROBES, NX, NCOL), 1.0, 6.0, ((0, 4), (1, 32))),
        "sensor_rows": draw_sensor_rows(jax.random.fold_in(keys[7], 71), 0),
        "sensor_cols": with_ends(jax.random.randint(keys[2], (SENSORS,), 0, NCOL - 1), jax.random.fold_in(keys[2], 1), 0, (NCOL - 1) - 1).astype(jnp.int32),
        "row_frac": jnp.clip(jax.random.uniform(keys[3], (SENSORS,), jnp.float32, 0.0, 1.0), 0.0, 1.0),
        "col_frac": jnp.clip(jax.random.uniform(keys[4], (SENSORS,), jnp.float32, 0.0, 1.0), 0.0, 1.0),
        "sensor_weights": jnp.clip(jnp.exp(jax.random.uniform(keys[5], (SENSORS,), jnp.float32, math.log(0.05), math.log(1.0))), 0.05, 1.0),
        "owner_order": draw_owner_order(jax.random.fold_in(keys[7], 71), 0),
    }


def reference(probe_fields, sensor_rows, sensor_cols, row_frac, col_frac, sensor_weights, owner_order):
    rlow = 1.0 - row_frac
    rhigh = row_frac
    clow = lax.optimization_barrier((1.0 - col_frac).astype(jnp.bfloat16)).astype(jnp.float32)
    chigh = lax.optimization_barrier(col_frac.astype(jnp.bfloat16)).astype(jnp.float32)
    rows_next = sensor_rows + 1
    cols_next = sensor_cols + 1

    def sample(field):
        field = field.astype(jnp.float32)
        top = clow * field[sensor_rows, sensor_cols] + chigh * field[sensor_rows, cols_next]
        bottom = clow * field[rows_next, sensor_cols] + chigh * field[rows_next, cols_next]
        return rlow * top + rhigh * bottom

    values = lax.map(sample, probe_fields)
    observed = values[:, owner_order]
    weights = sensor_weights[owner_order]
    spread = observed * weights[None, :]
    trace_mean = jnp.sum(spread * observed) / (PROBES * SENSORS)
    owned_rows = sensor_rows[owner_order]
    owned_cols = sensor_cols[owner_order]
    owned_low = rlow[owner_order]
    owned_high = rhigh[owner_order]
    clow_owned = clow[owner_order]
    chigh_owned = chigh[owner_order]

    def place(spread_row):
        lower = (spread_row * owned_low).astype(jnp.bfloat16).astype(jnp.float32)
        upper = (spread_row * owned_high).astype(jnp.bfloat16).astype(jnp.float32)
        grid = jnp.zeros((NX, NCOL), jnp.float32)
        grid = grid.at[owned_rows, owned_cols].add(lower * clow_owned)
        grid = grid.at[owned_rows, owned_cols + 1].add(lower * chigh_owned)
        grid = grid.at[owned_rows + 1, owned_cols].add(upper * clow_owned)
        grid = grid.at[owned_rows + 1, owned_cols + 1].add(upper * chigh_owned)
        return grid.astype(jnp.bfloat16)

    adjoint_sources = lax.map(place, spread)
    return adjoint_sources, observed, trace_mean
```

```python
import jax
import jax.numpy as jnp
from jax import lax
from jax.experimental import pallas as pl
from jax.experimental.pallas import tpu as pltpu
from jax.sharding import PartitionSpec as P

F32 = jnp.float32
BF = jnp.bfloat16
I32 = jnp.int32
MESH = pl.DeviceIdType.MESH

OWN = 32
RANK = 16
LIST = OWN * RANK
HALF = LIST // 2


def iota(shape, dim):
    return lax.broadcasted_iota(I32, shape, dim)


def mm(a, b):
    return lax.dot_general(a, b, (((1,), (0,)), ((), ())), preferred_element_type=F32)


def mm_nt(a, b):
    return lax.dot_general(a, b, (((1,), (1,)), ((), ())), preferred_element_type=F32)


def two(x):
    high = x.astype(BF)
    return high, (x - high.astype(F32)).astype(BF)


def mm_two(a, x):
    high, low = two(x)
    return mm(a, high) + mm(a, low)


def table(block, width, col, clo, chi):
    start = block * width
    at = jnp.clip(col - start, -2, width).astype(F32).astype(BF)
    after = jnp.clip(col + 1 - start, -2, width).astype(F32).astype(BF)
    here = iota((width, 128), 0).astype(F32).astype(BF)
    pieces = []
    for t in range(col.shape[1] // 128):
        cut = slice(t * 128, t * 128 + 128)
        low = jnp.where(here == at[:, cut], clo[:, cut], jnp.zeros((), BF))
        pieces.append(jnp.where(here == after[:, cut], chi[:, cut], low))
    return pieces


def row_weights(row, rhi):
    sub = iota((8, row.shape[1]), 0) % 4
    return jnp.where(sub == row, 1.0 - rhi, 0.0) + jnp.where(sub == row + 1, rhi, 0.0)


def times_rows(x, weights8):
    rows, slots = x.shape
    return (x.reshape(rows // 8, 8, slots) * weights8[None]).reshape(rows, slots)


def prep(s, ord_ref, line_ref, rows_ref, cols_ref, rf_ref, cf_ref, w_ref, rscr, rkscr):
    line = line_ref[...]
    onehot = (iota((128, 4096), 0) == (line & 127)).astype(F32).astype(BF)
    found = mm(rows_ref[...].astype(F32).astype(BF), onehot)
    picked = jnp.where(iota((32, 4096), 0) == (line >> 7), found, 0.0)
    slot_rows = jnp.sum(picked, axis=0, keepdims=True)
    for o in range(OWN):
        rscr[o : o + 1, :] = slot_rows[:, o * 128 : o * 128 + 128]
    rows = rscr[...].astype(I32)
    slab = rows >> 2
    upper = (iota((128, 128), 0) < iota((128, 128), 1)).astype(F32).astype(BF)
    sel = []
    for which in range(2):
        mask = slab == s - which
        maskf = jnp.where(mask, 1.0, 0.0)
        rank = mm(maskf.astype(BF), upper)
        rkscr[which] = jnp.where(mask, rank, -1.0)
    lane8 = iota((8, 128), 0).astype(F32)
    for which in range(2):
        for jh in range(2):
            for o in range(OWN):
                sel.append(jnp.where(rkscr[which, o : o + 1, :] == lane8 + 8.0 * jh, 1.0, 0.0))
    sel = jnp.concatenate(sel, axis=0).astype(BF)
    ids = ord_ref[...]
    parts = jnp.concatenate(
        [(ids >> 7).astype(F32), (ids & 127).astype(F32), jnp.ones((32, 128), F32)], axis=0
    ).astype(BF)
    got = mm_nt(parts, sel)
    mine = iota((32, 1024), 0) == ((iota((32, 1024), 1) & 255) >> 3)
    high = jnp.sum(jnp.where(mine, got[0:32], 0.0), axis=0, keepdims=True)
    low = jnp.sum(jnp.where(mine, got[32:64], 0.0), axis=0, keepdims=True)
    valid = jnp.sum(jnp.where(mine, got[64:96], 0.0), axis=0, keepdims=True) > 0.5
    onehot = (iota((128, 1024), 0).astype(F32) == low).astype(F32).astype(BF)
    cols = cols_ref[...]
    rf_hi, rf_lo = two(rf_ref[...])
    w_hi, w_lo = two(w_ref[...])
    cf = cf_ref[...]
    parts = jnp.concatenate(
        [
            (cols >> 7).astype(F32).astype(BF),
            (cols & 127).astype(F32).astype(BF),
            (1.0 - cf).astype(BF),
            cf.astype(BF),
            rf_hi,
            rf_lo,
            w_hi,
            w_lo,
            rows_ref[...].astype(F32).astype(BF),
        ],
        axis=0,
    )
    got = mm(parts, onehot)
    mine = iota((32, 1024), 0).astype(F32) == high
    vals = [
        jnp.sum(jnp.where(mine, got[32 * i : 32 * i + 32], 0.0), axis=0, keepdims=True)
        for i in range(9)
    ]
    rhi = vals[4] + vals[5]
    weight = vals[6] + vals[7]
    grid_row = vals[8].astype(I32) - 4 * s
    second = iota((1, 1024), 1) >= LIST
    use = valid & ((~second) | (grid_row == -1))
    col = jnp.where(use, (vals[0] * 128.0 + vals[1]).astype(I32), -8)
    grid_row = jnp.where(use, grid_row, -8)
    return col, vals[2], vals[3], grid_row, rhi, weight, rows, slab


def expand_matrix():
    a = iota((128, 512), 0)
    b = iota((128, 512), 1)
    return (a == ((b >> 8) * 64 + ((b & 255) >> 2))).astype(F32).astype(BF)


def fields_chunk(xv, first, count):
    return jnp.concatenate([xv[first + i].reshape(256, 128) for i in range(count)], axis=1)


def forward_kernel(
    s_ref, x_ref, ord_ref, line_ref, rows_ref, cols_ref, rf_ref, cf_ref, w_ref,
    out_ref, par_ref, info_ref,
    xv, acc, rscr, rkscr, tab, sem,
):
    s = s_ref[0]
    for c in range(64):
        pltpu.make_async_copy(
            x_ref.at[:, :, pl.ds(c * 128, 128)], xv.at[c], sem.at[c // 8]
        ).start()
    col, clo, chi, grid_row, rhi, weight, rows, slab = prep(
        s, ord_ref, line_ref, rows_ref, cols_ref, rf_ref, cf_ref, w_ref, rscr, rkscr
    )
    par_ref[0:1, :] = col.astype(F32)
    par_ref[1:2, :] = clo
    par_ref[2:3, :] = chi
    par_ref[3:4, :] = grid_row.astype(F32)
    par_ref[4:5, :] = rhi
    par_ref[5:6, :] = weight
    slabf = slab.astype(F32)
    own = jnp.sum(jnp.where(iota((32, 128), 0) == s, slabf, 0.0), axis=0, keepdims=True)
    square = jnp.broadcast_to(own, (128, 128))
    same = (square.T == square) & (iota((128, 128), 0) < iota((128, 128), 1))
    rank = jnp.sum(jnp.where(same, 1.0, 0.0), axis=0, keepdims=True)
    info_ref[0:1, :] = own
    info_ref[1:2, :] = rank

    clo = clo.astype(BF)
    chi = chi.astype(BF)
    acc[...] = jnp.zeros_like(acc)

    def chunk(i, carry):
        for j in range(8):
            pltpu.make_async_copy(
                x_ref.at[:, :, pl.ds(0, 128)], xv.at[8 * i + j], sem.at[i]
            ).wait()
        for j in range(4):
            pieces = table(4 * i + j, 256, col, clo, chi)
            for t in range(8):
                tab[j * 256 : j * 256 + 256, t * 128 : t * 128 + 128] = pieces[t]
        acc[...] += mm(fields_chunk(xv, 8 * i, 8), tab[...])
        return carry

    lax.fori_loop(0, 8, chunk, 0)
    weights8 = row_weights(grid_row, rhi)
    expand = expand_matrix()
    for which in range(2):
        both = []
        for jh in range(2):
            cut = slice(which * LIST + jh * HALF, which * LIST + jh * HALF + HALF)
            both.append(times_rows(acc[:, cut], weights8[:, cut]))
        part = mm_two(expand, jnp.concatenate(both, axis=0))
        out_ref[:, which] = part.T.reshape(OWN, 8, 128)


def exchange_kernel(
    mine, par_ref, info_ref, obs_ref, full_ref, trace_ref,
    box, next_box, prev_box, sums, group, ready, group_ready,
    send_sem, recv_sem, halo_send, halo_recv, sum_send, sum_recv, group_send, group_recv,
):
    s = lax.axis_index("slab")
    z = lax.axis_index("probe")
    after = lax.rem(s + 1, OWN)
    before = lax.rem(s + OWN - 1, OWN)
    barrier = pltpu.get_barrier_semaphore()
    for d in range(1, OWN):
        pl.semaphore_signal(
            barrier, inc=1, device_id={"slab": lax.rem(s + d, OWN)}, device_id_type=MESH
        )
    for d in range(1, 4):
        pl.semaphore_signal(
            barrier, inc=1, device_id={"probe": lax.rem(z + d, 4)}, device_id_type=MESH
        )
    pl.semaphore_wait(barrier, OWN + 2)
    to_next = pltpu.make_async_remote_copy(
        mine.at[:, 0], prev_box, halo_send.at[0], halo_recv.at[0], {"slab": after}, MESH
    )
    to_prev = pltpu.make_async_remote_copy(
        mine.at[:, 1], next_box, halo_send.at[1], halo_recv.at[1], {"slab": before}, MESH
    )
    to_next.start()
    to_prev.start()
    sends = []
    for d in range(1, OWN):
        t = lax.rem(s + d, OWN)
        copy = pltpu.make_async_remote_copy(
            mine.at[t], box.at[s], send_sem.at[d], recv_sem, {"slab": t}, MESH
        )
        copy.start()
        sends.append(copy)
    box[s] = mine[s]
    to_next.wait_recv()
    to_prev.wait_recv()
    own = (mine[:, 0] + next_box[...]).reshape(HALF, 128).T
    bnd = (mine[:, 1] + prev_box[...]).reshape(HALF, 128).T
    full_ref[0] = own
    full_ref[1] = bnd
    weight = par_ref[5:6, 0:LIST]
    square = own * own
    total = jnp.sum(square[0:64] * weight[:, 0:HALF]) + jnp.sum(square[64:128] * weight[:, HALF:LIST])
    ready[...] = jnp.full((8, 128), 1.0, F32) * total
    sum_sends = []
    for d in range(1, OWN):
        t = lax.rem(s + d, OWN)
        copy = pltpu.make_async_remote_copy(
            ready, sums.at[s], sum_send.at[d], sum_recv, {"slab": t}, MESH
        )
        copy.start()
        sum_sends.append(copy)
    sums[s] = ready[...]
    pltpu.make_async_copy(box.at[pl.ds(0, OWN - 1)], box.at[pl.ds(0, OWN - 1)], recv_sem).wait()
    shifted = jnp.concatenate([box[1:OWN, 1], jnp.zeros((1, 8, 128), F32)], axis=0)
    full = (box[:, 0] + shifted).reshape(HALF, 128).T
    slot_slab = info_ref[0:1, :].astype(I32)
    slot_rank = info_ref[1:2, :].astype(I32)
    sub = iota((HALF, 128), 0)
    pick = ((sub >> 3) == slot_slab) & ((sub & 7) == (slot_rank & 7))
    pick = jnp.where(pick, 1.0, 0.0).astype(BF)
    high, low = two(full)
    got = mm(high, pick) + mm(low, pick)
    obs_ref[...] = jnp.where(slot_rank < 8, got[0:64], got[64:128])
    pltpu.make_async_copy(sums.at[pl.ds(0, OWN - 1)], sums.at[pl.ds(0, OWN - 1)], sum_recv).wait()
    group_ready[...] = jnp.sum(sums[...], axis=0)
    group_sends = []
    for d in range(1, 4):
        t = lax.rem(z + d, 4)
        copy = pltpu.make_async_remote_copy(
            group_ready, group.at[z], group_send.at[d], group_recv, {"probe": t}, MESH
        )
        copy.start()
        group_sends.append(copy)
    group[z] = group_ready[...]
    pltpu.make_async_copy(group.at[pl.ds(0, 3)], group.at[pl.ds(0, 3)], group_recv).wait()
    trace_ref[...] = jnp.sum(group[...], axis=0) * (1.0 / 1048576.0)
    to_next.wait_send()
    to_prev.wait_send()
    for copy in sends + sum_sends + group_sends:
        copy.wait_send()


def adjoint_kernel(full_ref, par_ref, out_ref, ov, src, tab, sem):
    col = par_ref[0:1, :].astype(I32)
    clo = par_ref[1:2, :].astype(BF)
    chi = par_ref[2:3, :].astype(BF)
    grid_row = par_ref[3:4, :].astype(I32)
    rhi = par_ref[4:5, :]
    weight = par_ref[5:6, :]
    weights8 = row_weights(grid_row, rhi)
    a = iota((256, 128), 0)
    b = iota((256, 128), 1)
    for which in range(2):
        for jh in range(2):
            cut = slice(which * LIST + jh * HALF, which * LIST + jh * HALF + HALF)
            pick = (b == (jh * 64 + (a >> 2))).astype(F32).astype(BF)
            value = mm_two(pick, full_ref[which] * weight[:, cut])
            src[:, cut] = times_rows(value, weights8[:, cut]).astype(BF)

    def chunk(i, carry):
        for j in range(4):
            pieces = table(4 * i + j, 256, col, clo, chi)
            for t in range(8):
                tab[j, :, t * 128 : t * 128 + 128] = pieces[t]
        for j in range(4):
            got = mm_nt(src[...], tab[j]).astype(BF)
            for h in range(2):
                c = 8 * i + 2 * j + h
                ov[c] = got[:, h * 128 : h * 128 + 128].reshape(64, 4, 128)
                pltpu.make_async_copy(
                    ov.at[c], out_ref.at[:, :, pl.ds(pl.multiple_of(c * 128, 128), 128)], sem
                ).start()
        return carry

    lax.fori_loop(0, 8, chunk, 0)
    pltpu.make_async_copy(ov, ov, sem).wait()


def run_forward(s, fields, rows, cols, rf, cf, w, order):
    vm = pl.BlockSpec(memory_space=pltpu.VMEM)
    sq = lambda x: x.reshape(32, 128)
    return pl.pallas_call(
        forward_kernel,
        out_shape=(
            jax.ShapeDtypeStruct((OWN, 2, 8, 128), F32),
            jax.ShapeDtypeStruct((8, 1024), F32),
            jax.ShapeDtypeStruct((8, 128), F32),
        ),
        in_specs=[pl.BlockSpec(memory_space=pltpu.SMEM), pl.BlockSpec(memory_space=pl.ANY)] + [vm] * 7,
        out_specs=(vm, vm, vm),
        scratch_shapes=[
            pltpu.VMEM((64, 64, 4, 128), BF),
            pltpu.VMEM((256, 1024), F32),
            pltpu.VMEM((32, 128), F32),
            pltpu.VMEM((2, 32, 128), F32),
            pltpu.VMEM((1024, 1024), BF),
            pltpu.SemaphoreType.DMA((8,)),
        ],
        name="forward",
    )(s, fields, sq(order), order.reshape(1, 4096), sq(rows), sq(cols), sq(rf), sq(cf), sq(w))


def run_exchange(mine, par, info):
    vm = pl.BlockSpec(memory_space=pltpu.VMEM)
    dma = pltpu.SemaphoreType.DMA
    return pl.pallas_call(
        exchange_kernel,
        out_shape=(
            jax.ShapeDtypeStruct((64, 128), F32),
            jax.ShapeDtypeStruct((2, 128, HALF), F32),
            jax.ShapeDtypeStruct((8, 128), F32),
        ),
        in_specs=[vm] * 3,
        out_specs=(vm, vm, vm),
        scratch_shapes=[
            pltpu.VMEM((OWN, 2, 8, 128), F32),
            pltpu.VMEM((OWN, 8, 128), F32),
            pltpu.VMEM((OWN, 8, 128), F32),
            pltpu.VMEM((OWN, 8, 128), F32),
            pltpu.VMEM((4, 8, 128), F32),
            pltpu.VMEM((8, 128), F32),
            pltpu.VMEM((8, 128), F32),
            dma((OWN,)), dma, dma((2,)), dma((2,)), dma((OWN,)), dma, dma((4,)), dma,
        ],
        compiler_params=pltpu.CompilerParams(collective_id=0, has_side_effects=True),
        name="exchange",
    )(mine, par, info)


def run_adjoint(full, par):
    vm = pl.BlockSpec(memory_space=pltpu.VMEM)
    return pl.pallas_call(
        adjoint_kernel,
        out_shape=jax.ShapeDtypeStruct((64, 4, 8192), BF),
        in_specs=[vm] * 2,
        out_specs=pl.BlockSpec(memory_space=pl.ANY),
        scratch_shapes=[
            pltpu.VMEM((64, 64, 4, 128), BF),
            pltpu.VMEM((256, 1024), BF),
            pltpu.VMEM((4, 256, 1024), BF),
            pltpu.SemaphoreType.DMA,
        ],
        name="adjoint",
    )(full, par)


def body(fields, rows, cols, rf, cf, w, order):
    s = lax.axis_index("slab").astype(I32).reshape(1)
    mine, par, info = run_forward(s, fields, rows, cols, rf, cf, w, order)
    observed, full, trace = run_exchange(mine, par, info)
    adjoint = run_adjoint(full, par)
    return adjoint, observed, trace[0, 0]


def solution(mesh):
    return jax.shard_map(
        body,
        mesh=mesh,
        in_specs=(P("probe", "slab", None), P(), P(), P(), P(), P(), P()),
        out_specs=(P("probe", "slab", None), P("probe", "slab"), P()),
        check_vma=False,
    )
```

```python
import jax
import jax.numpy as jnp
from jax import lax
from jax.experimental import pallas as pl
from jax.experimental.pallas import tpu as pltpu
from jax.sharding import PartitionSpec as P

F32 = jnp.float32
BF = jnp.bfloat16
I32 = jnp.int32
MESH = pl.DeviceIdType.MESH

OWN = 32
RANK = 16
LIST = OWN * RANK
HALF = LIST // 2


def iota(shape, dim):
    return lax.broadcasted_iota(I32, shape, dim)


def mm(a, b):
    return lax.dot_general(a, b, (((1,), (0,)), ((), ())), preferred_element_type=F32)


def mm_nt(a, b):
    return lax.dot_general(a, b, (((1,), (1,)), ((), ())), preferred_element_type=F32)


def two(x):
    high = x.astype(BF)
    return high, (x - high.astype(F32)).astype(BF)


def mm_two(a, x):
    high, low = two(x)
    return mm(a, high) + mm(a, low)


def table_rows(block, col, clo, chi):
    after = col + 1
    low = jnp.where((col >> 8) == block, clo, 0.0).astype(BF)
    high = jnp.where((after >> 8) == block, chi, 0.0).astype(BF)
    return low, high


def column_spots(col):
    at = (col & 255).astype(F32).astype(BF)
    after = ((col + 1) & 255).astype(F32).astype(BF)
    return at, after


def row_weights(row, rhi):
    sub = iota((8, row.shape[1]), 0) % 4
    return jnp.where(sub == row, 1.0 - rhi, 0.0) + jnp.where(sub == row + 1, rhi, 0.0)


def times_rows(x, weights8):
    rows, slots = x.shape
    return (x.reshape(rows // 8, 8, slots) * weights8[None]).reshape(rows, slots)


def prep(s, ord_ref, line_ref, rows_ref, cols_ref, rf_ref, cf_ref, w_ref, rscr, rkscr):
    line = line_ref[...]
    onehot = (iota((128, 4096), 0) == (line & 127)).astype(F32).astype(BF)
    found = mm(rows_ref[...].astype(F32).astype(BF), onehot)
    picked = jnp.where(iota((32, 4096), 0) == (line >> 7), found, 0.0)
    slot_rows = jnp.sum(picked, axis=0, keepdims=True)
    for o in range(OWN):
        rscr[o : o + 1, :] = slot_rows[:, o * 128 : o * 128 + 128]
    rows = rscr[...].astype(I32)
    slab = rows >> 2
    upper = (iota((128, 128), 0) < iota((128, 128), 1)).astype(F32).astype(BF)
    sel = []
    for which in range(2):
        mask = slab == s - which
        maskf = jnp.where(mask, 1.0, 0.0)
        rank = mm(maskf.astype(BF), upper)
        rkscr[which] = jnp.where(mask, rank, -1.0)
    lane8 = iota((8, 128), 0).astype(F32)
    for which in range(2):
        for jh in range(2):
            for o in range(OWN):
                sel.append(jnp.where(rkscr[which, o : o + 1, :] == lane8 + 8.0 * jh, 1.0, 0.0))
    sel = jnp.concatenate(sel, axis=0).astype(BF)
    ids = ord_ref[...]
    parts = jnp.concatenate(
        [(ids >> 7).astype(F32), (ids & 127).astype(F32), jnp.ones((32, 128), F32)], axis=0
    ).astype(BF)
    got = mm_nt(parts, sel)
    mine = iota((32, 1024), 0) == ((iota((32, 1024), 1) & 255) >> 3)
    high = jnp.sum(jnp.where(mine, got[0:32], 0.0), axis=0, keepdims=True)
    low = jnp.sum(jnp.where(mine, got[32:64], 0.0), axis=0, keepdims=True)
    valid = jnp.sum(jnp.where(mine, got[64:96], 0.0), axis=0, keepdims=True) > 0.5
    onehot = (iota((128, 1024), 0).astype(F32) == low).astype(F32).astype(BF)
    cols = cols_ref[...]
    rf_hi, rf_lo = two(rf_ref[...])
    w_hi, w_lo = two(w_ref[...])
    cf = cf_ref[...]
    parts = jnp.concatenate(
        [
            (cols >> 7).astype(F32).astype(BF),
            (cols & 127).astype(F32).astype(BF),
            (1.0 - cf).astype(BF),
            cf.astype(BF),
            rf_hi,
            rf_lo,
            w_hi,
            w_lo,
            rows_ref[...].astype(F32).astype(BF),
        ],
        axis=0,
    )
    got = mm(parts, onehot)
    mine = iota((32, 1024), 0).astype(F32) == high
    vals = [
        jnp.sum(jnp.where(mine, got[32 * i : 32 * i + 32], 0.0), axis=0, keepdims=True)
        for i in range(9)
    ]
    rhi = vals[4] + vals[5]
    weight = vals[6] + vals[7]
    grid_row = vals[8].astype(I32) - 4 * s
    second = iota((1, 1024), 1) >= LIST
    use = valid & ((~second) | (grid_row == -1))
    col = jnp.where(use, (vals[0] * 128.0 + vals[1]).astype(I32), -8)
    grid_row = jnp.where(use, grid_row, -8)
    return col, vals[2], vals[3], grid_row, rhi, weight, rows, slab


def expand_matrix():
    a = iota((128, 512), 0)
    b = iota((128, 512), 1)
    return (a == ((b >> 8) * 64 + ((b & 255) >> 2))).astype(F32).astype(BF)


def fields_chunk(xv, first, count):
    return jnp.concatenate([xv[first + i].reshape(256, 128) for i in range(count)], axis=1)


def weighted_source(full, weight, weights8, dst):
    a = iota((256, 128), 0)
    b = iota((256, 128), 1)
    for jh in range(2):
        cut = slice(jh * HALF, jh * HALF + HALF)
        pick = (b == (jh * 64 + (a >> 2))).astype(F32).astype(BF)
        value = mm_two(pick, full * weight[:, cut])
        dst[:, cut] = times_rows(value, weights8[:, cut]).astype(BF)


def main_kernel(
    x_ref, ord_ref, line_ref, rows_ref, cols_ref, rf_ref, cf_ref, w_ref,
    ov, obs_ref, trace_ref,
    xv, acc, tabs, partial, src, rscr, rkscr,
    ordv, linev, rowsv, colsv, rfv, cfv, wv,
    mine_a, mine_b, full_a, next_box, prev_box, box, sums, ready,
    x_sem, in_sem, halo_send, halo_recv, own_send, own_recv, sum_send, sum_recv,
):
    s = lax.axis_index("slab")
    z = lax.axis_index("probe")
    me = s * 4 + z
    small = [
        (ord_ref, ordv), (line_ref, linev), (rows_ref, rowsv), (cols_ref, colsv),
        (rf_ref, rfv), (cf_ref, cfv), (w_ref, wv),
    ]
    small = [pltpu.make_async_copy(a, b, in_sem.at[i]) for i, (a, b) in enumerate(small)]
    for copy in small:
        copy.start()
    for c in range(64):
        pltpu.make_async_copy(
            x_ref.at[:, :, pl.ds(c * 128, 128)], xv.at[c], x_sem.at[c // 8]
        ).start()
    barrier = pltpu.get_barrier_semaphore()

    def greet(d, carry):
        t = lax.rem(me + d, 128)
        pl.semaphore_signal(
            barrier, inc=1, device_id={"slab": t // 4, "probe": lax.rem(t, 4)}, device_id_type=MESH
        )
        return carry

    lax.fori_loop(1, 128, greet, 0)
    for copy in small:
        copy.wait()
    col, clo, chi, grid_row, rhi, weight, rows, slab = prep(
        s, ordv, linev, rowsv, colsv, rfv, cfv, wv, rscr, rkscr
    )
    slabf = slab.astype(F32)
    slot_slab = jnp.sum(jnp.where(iota((32, 128), 0) == s, slabf, 0.0), axis=0, keepdims=True)
    square = jnp.broadcast_to(slot_slab, (128, 128))
    same = (square.T == square) & (iota((128, 128), 0) < iota((128, 128), 1))
    slot_rank = jnp.sum(jnp.where(same, 1.0, 0.0), axis=0, keepdims=True).astype(I32)
    slot_slab = slot_slab.astype(I32)
    weights8 = row_weights(grid_row, rhi)
    here = iota((256, 128), 0).astype(F32).astype(BF)
    expand = expand_matrix()
    zero = jnp.zeros((), BF)

    def forward(which, first):
        cut = slice(which * LIST, which * LIST + LIST)
        at, after = column_spots(col[:, cut])
        acc[...] = jnp.zeros_like(acc)

        def chunk(i, carry):
            if first:
                view = xv.at[pl.ds(8 * i, 8)]
                pltpu.make_async_copy(view, view, x_sem.at[i]).wait()
            for j in range(4):
                low, high = table_rows(4 * i + j, col[:, cut], clo[:, cut], chi[:, cut])
                for t in range(4):
                    c = slice(t * 128, t * 128 + 128)
                    upper = jnp.where(here == after[:, c], high[:, c], zero)
                    tabs[which, 4 * i + j, :, c] = jnp.where(here == at[:, c], low[:, c], upper)
            tab = tabs[which, pl.ds(4 * i, 4)].reshape(1024, LIST)
            acc[...] += mm(fields_chunk(xv, 8 * i, 8), tab)
            return carry

        lax.fori_loop(0, 8, chunk, 0)
        both = []
        for jh in range(2):
            both.append(
                times_rows(
                    acc[:, jh * HALF : jh * HALF + HALF],
                    weights8[:, which * LIST + jh * HALF : which * LIST + jh * HALF + HALF],
                )
            )
        return mm_two(expand, jnp.concatenate(both, axis=0))

    part_b = forward(1, True)
    mine_b[...] = part_b.T.reshape(OWN, 8, 128)
    pl.semaphore_wait(barrier, 127)
    to_prev = pltpu.make_async_remote_copy(
        mine_b, next_box, halo_send.at[0], halo_recv.at[0],
        {"slab": lax.rem(s + OWN - 1, OWN), "probe": z}, MESH,
    )
    to_prev.start()
    part_a = forward(0, False)
    mine_a[...] = part_a.T.reshape(OWN, 8, 128)
    to_next = pltpu.make_async_remote_copy(
        mine_a, prev_box, halo_send.at[1], halo_recv.at[1],
        {"slab": lax.rem(s + 1, OWN), "probe": z}, MESH,
    )
    to_next.start()
    to_prev.wait_recv()
    complete = mine_a[...] + next_box[...]
    full_a[...] = complete
    value_a = complete.reshape(HALF, 128).T
    square = value_a * value_a
    total = jnp.sum(square[0:64] * weight[:, 0:HALF]) + jnp.sum(
        square[64:128] * weight[:, HALF:LIST]
    )
    ready[...] = jnp.full((1, 128), 1.0, F32) * total

    def send_sum(d, carry):
        t = lax.rem(me + d, 128)
        pltpu.make_async_remote_copy(
            ready, sums.at[me], sum_send, sum_recv,
            {"slab": t // 4, "probe": lax.rem(t, 4)}, MESH,
        ).start()
        return carry

    lax.fori_loop(1, 128, send_sum, 0)
    sums[me] = ready[...]

    def send_own(d, carry):
        t = lax.rem(s + d, OWN)
        pltpu.make_async_remote_copy(
            full_a.at[t], box.at[s], own_send, own_recv, {"slab": t, "probe": z}, MESH
        ).start()
        return carry

    lax.fori_loop(1, OWN, send_own, 0)
    box[s] = full_a[s]
    weighted_source(value_a, weight[:, 0:LIST], weights8[:, 0:LIST], src)

    def adjoint_a(i, carry):
        for j in range(4):
            partial[4 * i + j] = mm_nt(src[...], tabs[0, 4 * i + j])
        return carry

    lax.fori_loop(0, 8, adjoint_a, 0)
    to_next.wait_recv()
    value_b = (mine_b[...] + prev_box[...]).reshape(HALF, 128).T
    weighted_source(value_b, weight[:, LIST:], weights8[:, LIST:], src)

    def adjoint_b(i, carry):
        for j in range(4):
            got = (partial[4 * i + j] + mm_nt(src[...], tabs[1, 4 * i + j])).astype(BF)
            for h in range(2):
                ov[8 * i + 2 * j + h] = got[:, h * 128 : h * 128 + 128].reshape(64, 4, 128)
        return carry

    lax.fori_loop(0, 8, adjoint_b, 0)
    view = box.at[pl.ds(0, OWN - 1)]
    pltpu.make_async_copy(view, view, own_recv).wait()
    full = box[...].reshape(HALF, 128).T
    sub = iota((HALF, 128), 0)
    pick = ((sub >> 3) == slot_slab) & ((sub & 7) == (slot_rank & 7))
    pick = jnp.where(pick, 1.0, 0.0).astype(BF)
    high, low = two(full)
    got = mm(high, pick) + mm(low, pick)
    obs_ref[...] = jnp.where(slot_rank < 8, got[0:64], got[64:128])
    view = sums.at[pl.ds(0, 127)]
    pltpu.make_async_copy(view, view, sum_recv).wait()
    trace_ref[...] = jnp.sum(sums[...], axis=0) * (1.0 / 1048576.0)
    to_prev.wait_send()
    to_next.wait_send()
    pltpu.make_async_copy(view, view, sum_send).wait()
    view = box.at[pl.ds(0, OWN - 1)]
    pltpu.make_async_copy(view, view, own_send).wait()


def store_kernel(ov, obs_in, trace_in, out_ref, obs_ref, trace_ref, sem):
    for c in range(64):
        pltpu.make_async_copy(ov.at[c], out_ref.at[:, :, pl.ds(c * 128, 128)], sem).start()
    obs_ref[...] = obs_in[...]
    trace_ref[0, 0] = trace_in[0, 0]
    pltpu.make_async_copy(ov, ov, sem).wait()


def run_main(fields, rows, cols, rf, cf, w, order):
    vm = pl.BlockSpec(memory_space=pltpu.VMEM)
    anywhere = pl.BlockSpec(memory_space=pl.ANY)
    dma = pltpu.SemaphoreType.DMA
    sq = lambda x: x.reshape(32, 128)
    block = pltpu.VMEM((OWN, 8, 128), F32)
    return pl.pallas_call(
        main_kernel,
        out_shape=(
            pltpu.VMEM((64, 64, 4, 128), BF),
            pltpu.VMEM((64, 128), F32),
            pltpu.VMEM((1, 128), F32),
        ),
        in_specs=[anywhere] * 8,
        out_specs=(vm, vm, vm),
        scratch_shapes=[
            pltpu.VMEM((64, 64, 4, 128), BF),
            pltpu.VMEM((256, LIST), F32),
            pltpu.VMEM((2, 32, 256, LIST), BF),
            pltpu.VMEM((32, 256, 256), F32),
            pltpu.VMEM((256, LIST), BF),
            pltpu.VMEM((32, 128), F32),
            pltpu.VMEM((2, 32, 128), F32),
            pltpu.VMEM((32, 128), I32),
            pltpu.VMEM((1, 4096), I32),
            pltpu.VMEM((32, 128), I32),
            pltpu.VMEM((32, 128), I32),
            pltpu.VMEM((32, 128), F32),
            pltpu.VMEM((32, 128), F32),
            pltpu.VMEM((32, 128), F32),
            block, block, block, block, block, block,
            pltpu.VMEM((128, 1, 128), F32),
            pltpu.VMEM((1, 128), F32),
            dma((8,)), dma((7,)), dma((2,)), dma((2,)), dma, dma, dma, dma,
        ],
        compiler_params=pltpu.CompilerParams(
            collective_id=0, has_side_effects=True, vmem_limit_bytes=60000000
        ),
        name="main",
    )(fields, sq(order), order.reshape(1, 4096), sq(rows), sq(cols), sq(rf), sq(cf), sq(w))


def run_store(ov, obs, trace):
    vm = pl.BlockSpec(memory_space=pltpu.VMEM)
    anywhere = pl.BlockSpec(memory_space=pl.ANY)
    return pl.pallas_call(
        store_kernel,
        out_shape=(
            jax.ShapeDtypeStruct((64, 4, 8192), BF),
            jax.ShapeDtypeStruct((64, 128), F32),
            jax.ShapeDtypeStruct((1, 1), F32),
        ),
        in_specs=[vm] * 3,
        out_specs=(anywhere, vm, pl.BlockSpec(memory_space=pltpu.SMEM)),
        scratch_shapes=[pltpu.SemaphoreType.DMA],
        compiler_params=pltpu.CompilerParams(vmem_limit_bytes=8 * 1024 * 1024),
        name="store",
    )(ov, obs, trace)


def body(fields, rows, cols, rf, cf, w, order):
    ov, obs, trace = run_main(fields, rows, cols, rf, cf, w, order)
    adjoint, observed, trace = run_store(ov, obs, trace)
    return adjoint, observed, trace.reshape(())


def solution(mesh):
    return jax.shard_map(
        body,
        mesh=mesh,
        in_specs=(P("probe", "slab", None), P(), P(), P(), P(), P(), P()),
        out_specs=(P("probe", "slab", None), P("probe", "slab"), P()),
        check_vma=False,
    )
```

```python
import jax
import jax.numpy as jnp
from jax import lax
from jax.experimental import pallas as pl
from jax.experimental.pallas import tpu as pltpu
from jax.sharding import PartitionSpec as P

F32 = jnp.float32
BF = jnp.bfloat16
I32 = jnp.int32
MESH = pl.DeviceIdType.MESH

OWN = 32
RANK = 16
LIST = OWN * RANK
HALF = LIST // 2


def iota(shape, dim):
    return lax.broadcasted_iota(I32, shape, dim)


def mm(a, b):
    return lax.dot_general(a, b, (((1,), (0,)), ((), ())), preferred_element_type=F32)


def mm_nt(a, b):
    return lax.dot_general(a, b, (((1,), (1,)), ((), ())), preferred_element_type=F32)


def two(x):
    high = x.astype(BF)
    return high, (x - high.astype(F32)).astype(BF)


def mm_two(a, x):
    high, low = two(x)
    return mm(a, high) + mm(a, low)


def relative(block, col):
    start = block * 256
    at = jnp.clip(col - start, -2, 256).astype(F32).astype(BF)
    after = jnp.clip(col + 1 - start, -2, 256).astype(F32).astype(BF)
    return at, after


def row_weights(row, rhi):
    sub = iota((8, row.shape[1]), 0) % 4
    return jnp.where(sub == row, 1.0 - rhi, 0.0) + jnp.where(sub == row + 1, rhi, 0.0)


def times_rows(x, weights8):
    rows, slots = x.shape
    return (x.reshape(rows // 8, 8, slots) * weights8[None]).reshape(rows, slots)


def prep(s, ord_ref, line_ref, rows_ref, cols_ref, rf_ref, cf_ref, w_ref, rscr, rkscr):
    line = line_ref[...]
    onehot = (iota((128, 4096), 0) == (line & 127)).astype(F32).astype(BF)
    found = mm(rows_ref[...].astype(F32).astype(BF), onehot)
    picked = jnp.where(iota((32, 4096), 0) == (line >> 7), found, 0.0)
    slot_rows = jnp.sum(picked, axis=0, keepdims=True)
    for o in range(OWN):
        rscr[o : o + 1, :] = slot_rows[:, o * 128 : o * 128 + 128]
    rows = rscr[...].astype(I32)
    slab = rows >> 2
    upper = (iota((128, 128), 0) < iota((128, 128), 1)).astype(F32).astype(BF)
    sel = []
    for which in range(2):
        mask = slab == s - which
        maskf = jnp.where(mask, 1.0, 0.0)
        rank = mm(maskf.astype(BF), upper)
        rkscr[which] = jnp.where(mask, rank, -1.0)
    lane8 = iota((8, 128), 0).astype(F32)
    for which in range(2):
        for jh in range(2):
            for o in range(OWN):
                sel.append(jnp.where(rkscr[which, o : o + 1, :] == lane8 + 8.0 * jh, 1.0, 0.0))
    sel = jnp.concatenate(sel, axis=0).astype(BF)
    ids = ord_ref[...]
    parts = jnp.concatenate(
        [(ids >> 7).astype(F32), (ids & 127).astype(F32), jnp.ones((32, 128), F32)], axis=0
    ).astype(BF)
    got = mm_nt(parts, sel)
    mine = iota((32, 1024), 0) == ((iota((32, 1024), 1) & 255) >> 3)
    high = jnp.sum(jnp.where(mine, got[0:32], 0.0), axis=0, keepdims=True)
    low = jnp.sum(jnp.where(mine, got[32:64], 0.0), axis=0, keepdims=True)
    valid = jnp.sum(jnp.where(mine, got[64:96], 0.0), axis=0, keepdims=True) > 0.5
    onehot = (iota((128, 1024), 0).astype(F32) == low).astype(F32).astype(BF)
    cols = cols_ref[...]
    rf_hi, rf_lo = two(rf_ref[...])
    w_hi, w_lo = two(w_ref[...])
    cf = cf_ref[...]
    parts = jnp.concatenate(
        [
            (cols >> 7).astype(F32).astype(BF),
            (cols & 127).astype(F32).astype(BF),
            (1.0 - cf).astype(BF),
            cf.astype(BF),
            rf_hi,
            rf_lo,
            w_hi,
            w_lo,
            rows_ref[...].astype(F32).astype(BF),
        ],
        axis=0,
    )
    got = mm(parts, onehot)
    mine = iota((32, 1024), 0).astype(F32) == high
    vals = [
        jnp.sum(jnp.where(mine, got[32 * i : 32 * i + 32], 0.0), axis=0, keepdims=True)
        for i in range(9)
    ]
    rhi = vals[4] + vals[5]
    weight = vals[6] + vals[7]
    grid_row = vals[8].astype(I32) - 4 * s
    second = iota((1, 1024), 1) >= LIST
    use = valid & ((~second) | (grid_row == -1))
    col = jnp.where(use, (vals[0] * 128.0 + vals[1]).astype(I32), -8)
    grid_row = jnp.where(use, grid_row, -8)
    return col, vals[2], vals[3], grid_row, rhi, weight, rows, slab


def expand_matrix():
    a = iota((128, 512), 0)
    b = iota((128, 512), 1)
    return (a == ((b >> 8) * 64 + ((b & 255) >> 2))).astype(F32).astype(BF)


def fields_chunk(xv, first, count):
    return jnp.concatenate([xv[first + i] for i in range(count)], axis=1)


def table_block(tabs, which, block):
    return jnp.concatenate([tabs[which, block, t] for t in range(4)], axis=1)


def weighted_source(full, weight, weights8, dst):
    a = iota((256, 128), 0)
    b = iota((256, 128), 1)
    for jh in range(2):
        cut = slice(jh * HALF, jh * HALF + HALF)
        pick = (b == (jh * 64 + (a >> 2))).astype(F32).astype(BF)
        value = mm_two(pick, full * weight[:, cut])
        dst[:, cut] = times_rows(value, weights8[:, cut]).astype(BF)


def main_kernel(
    x_ref, ord_ref, line_ref, rows_ref, cols_ref, rf_ref, cf_ref, w_ref,
    ov, obs_ref, trace_ref,
    xv, acc, tabs, partial, src, rscr, rkscr,
    ordv, linev, rowsv, colsv, rfv, cfv, wv,
    mine_a, mine_b, full_a, next_box, prev_box, box, sums, ready, group, group_ready,
    x_sem, in_sem, halo_send, halo_recv, own_send, own_recv, sum_send, sum_recv,
    group_send, group_recv,
):
    s = lax.axis_index("slab")
    z = lax.axis_index("probe")
    small = [
        (ord_ref, ordv), (line_ref, linev), (rows_ref, rowsv), (cols_ref, colsv),
        (rf_ref, rfv), (cf_ref, cfv), (w_ref, wv),
    ]
    small = [pltpu.make_async_copy(a, b, in_sem.at[i]) for i, (a, b) in enumerate(small)]
    for copy in small:
        copy.start()
    flat = x_ref.reshape(256, 8192)
    for c in range(64):
        pltpu.make_async_copy(
            flat.at[:, pl.ds(c * 128, 128)], xv.at[c], x_sem.at[c // 32]
        ).start()
    barrier = pltpu.get_barrier_semaphore()

    def greet(d, carry):
        t = lax.rem(s + d, OWN)
        pl.semaphore_signal(
            barrier, inc=1, device_id={"slab": t, "probe": z}, device_id_type=MESH
        )
        return carry

    lax.fori_loop(1, OWN, greet, 0)
    for d in range(1, 4):
        pl.semaphore_signal(
            barrier, inc=1, device_id={"slab": s, "probe": lax.rem(z + d, 4)}, device_id_type=MESH
        )
    for copy in small:
        copy.wait()
    col, clo, chi, grid_row, rhi, weight, rows, slab = prep(
        s, ordv, linev, rowsv, colsv, rfv, cfv, wv, rscr, rkscr
    )
    slabf = slab.astype(F32)
    slot_slab = jnp.sum(jnp.where(iota((32, 128), 0) == s, slabf, 0.0), axis=0, keepdims=True)
    square = jnp.broadcast_to(slot_slab, (128, 128))
    same = (square.T == square) & (iota((128, 128), 0) < iota((128, 128), 1))
    slot_rank = jnp.sum(jnp.where(same, 1.0, 0.0), axis=0, keepdims=True).astype(I32)
    slot_slab = slot_slab.astype(I32)
    weights8 = row_weights(grid_row, rhi)
    here = iota((256, 128), 0).astype(F32).astype(BF)
    expand = expand_matrix()
    zero = jnp.zeros((), BF)

    def forward(which, first):
        cut = slice(which * LIST, which * LIST + LIST)
        columns = col[:, cut]
        low = clo[:, cut].astype(BF)
        high = chi[:, cut].astype(BF)

        def build(i):
            for j in range(4):
                at, after = relative(4 * i + j, columns)
                for t in range(4):
                    c = slice(t * 128, t * 128 + 128)
                    upper = jnp.where(here == after[:, c], high[:, c], zero)
                    tabs[which, 4 * i + j, t] = jnp.where(here == at[:, c], low[:, c], upper)

        def product(i):
            tab = jnp.concatenate([table_block(tabs, which, 4 * i + j) for j in range(4)], axis=0)
            return mm(fields_chunk(xv, 8 * i, 8), tab)

        def arrive(i):
            view = xv.at[pl.ds(32 * i, 32)]
            pltpu.make_async_copy(view, view, x_sem.at[i]).wait()

        build(0)
        total = None
        for i in range(8):
            if first and i % 4 == 0:
                arrive(i // 4)
            if i < 7:
                build(i + 1)
            part = product(i)
            total = part if total is None else total + part
        acc[...] = total
        both = []
        for jh in range(2):
            both.append(
                times_rows(
                    acc[:, jh * HALF : jh * HALF + HALF],
                    weights8[:, which * LIST + jh * HALF : which * LIST + jh * HALF + HALF],
                )
            )
        return mm_two(expand, jnp.concatenate(both, axis=0))

    part_b = forward(1, True)
    mine_b[...] = part_b.T.reshape(OWN, 8, 128)
    pl.semaphore_wait(barrier, OWN + 2)
    to_prev = pltpu.make_async_remote_copy(
        mine_b, next_box, halo_send.at[0], halo_recv.at[0],
        {"slab": lax.rem(s + OWN - 1, OWN), "probe": z}, MESH,
    )
    to_prev.start()
    part_a = forward(0, False)
    mine_a[...] = part_a.T.reshape(OWN, 8, 128)
    to_next = pltpu.make_async_remote_copy(
        mine_a, prev_box, halo_send.at[1], halo_recv.at[1],
        {"slab": lax.rem(s + 1, OWN), "probe": z}, MESH,
    )
    to_next.start()
    to_prev.wait_recv()
    complete = mine_a[...] + next_box[...]
    full_a[...] = complete
    value_a = complete.reshape(HALF, 128).T
    square = value_a * value_a
    total = jnp.sum(square[0:64] * weight[:, 0:HALF]) + jnp.sum(
        square[64:128] * weight[:, HALF:LIST]
    )
    ready[...] = jnp.full((1, 128), 1.0, F32) * total

    for d in range(1, 4):
        pltpu.make_async_remote_copy(
            ready, group.at[z], group_send, group_recv,
            {"slab": s, "probe": lax.rem(z + d, 4)}, MESH,
        ).start()
    group[z] = ready[...]

    def send_own(d, carry):
        t = lax.rem(s + d, OWN)
        pltpu.make_async_remote_copy(
            full_a.at[t], box.at[s], own_send, own_recv, {"slab": t, "probe": z}, MESH
        ).start()
        return carry

    lax.fori_loop(1, OWN, send_own, 0)
    box[s] = full_a[s]
    weighted_source(value_a, weight[:, 0:LIST], weights8[:, 0:LIST], src)

    def adjoint_a(i, carry):
        for j in range(4):
            partial[4 * i + j] = mm_nt(src[...], table_block(tabs, 0, 4 * i + j))
        return carry

    lax.fori_loop(0, 8, adjoint_a, 0)
    view = group.at[pl.ds(0, 3)]
    pltpu.make_async_copy(view, view, group_recv).wait()
    group_ready[...] = jnp.sum(group[...], axis=0)

    def send_sum(d, carry):
        t = lax.rem(s + d, OWN)
        pltpu.make_async_remote_copy(
            group_ready, sums.at[s], sum_send, sum_recv, {"slab": t, "probe": z}, MESH
        ).start()
        return carry

    lax.fori_loop(1, OWN, send_sum, 0)
    sums[s] = group_ready[...]
    to_next.wait_recv()
    value_b = (mine_b[...] + prev_box[...]).reshape(HALF, 128).T
    weighted_source(value_b, weight[:, LIST:], weights8[:, LIST:], src)

    def adjoint_b(i, carry):
        for j in range(4):
            got = (partial[4 * i + j] + mm_nt(src[...], table_block(tabs, 1, 4 * i + j))).astype(BF)
            for h in range(2):
                ov[8 * i + 2 * j + h] = got[:, h * 128 : h * 128 + 128]
        return carry

    lax.fori_loop(0, 8, adjoint_b, 0)
    view = box.at[pl.ds(0, OWN - 1)]
    pltpu.make_async_copy(view, view, own_recv).wait()
    full = box[...].reshape(HALF, 128).T
    sub = iota((HALF, 128), 0)
    pick = ((sub >> 3) == slot_slab) & ((sub & 7) == (slot_rank & 7))
    pick = jnp.where(pick, 1.0, 0.0).astype(BF)
    high, low = two(full)
    got = mm(high, pick) + mm(low, pick)
    obs_ref[...] = jnp.where(slot_rank < 8, got[0:64], got[64:128])
    view = sums.at[pl.ds(0, OWN - 1)]
    pltpu.make_async_copy(view, view, sum_recv).wait()
    trace_ref[...] = jnp.sum(sums[...], axis=0) * (1.0 / 1048576.0)
    to_prev.wait_send()
    to_next.wait_send()
    pltpu.make_async_copy(view, view, sum_send).wait()
    view = group.at[pl.ds(0, 3)]
    pltpu.make_async_copy(view, view, group_send).wait()
    view = box.at[pl.ds(0, OWN - 1)]
    pltpu.make_async_copy(view, view, own_send).wait()


def store_kernel(ov, obs_in, trace_in, out_ref, obs_ref, trace_ref, sem):
    flat = out_ref.reshape(256, 8192)
    for c in range(64):
        pltpu.make_async_copy(ov.at[c], flat.at[:, pl.ds(c * 128, 128)], sem).start()
    obs_ref[...] = obs_in[...]
    trace_ref[0, 0] = trace_in[0, 0]
    pltpu.make_async_copy(ov, ov, sem).wait()


def run_main(fields, rows, cols, rf, cf, w, order):
    vm = pl.BlockSpec(memory_space=pltpu.VMEM)
    anywhere = pl.BlockSpec(memory_space=pl.ANY)
    dma = pltpu.SemaphoreType.DMA
    sq = lambda x: x.reshape(32, 128)
    block = pltpu.VMEM((OWN, 8, 128), F32)
    return pl.pallas_call(
        main_kernel,
        out_shape=(
            pltpu.VMEM((64, 256, 128), BF),
            pltpu.VMEM((64, 128), F32),
            pltpu.VMEM((1, 128), F32),
        ),
        in_specs=[anywhere] * 8,
        out_specs=(vm, vm, vm),
        scratch_shapes=[
            pltpu.VMEM((64, 256, 128), BF),
            pltpu.VMEM((256, LIST), F32),
            pltpu.VMEM((2, 32, 4, 256, 128), BF),
            pltpu.VMEM((32, 256, 256), F32),
            pltpu.VMEM((256, LIST), BF),
            pltpu.VMEM((32, 128), F32),
            pltpu.VMEM((2, 32, 128), F32),
            pltpu.VMEM((32, 128), I32),
            pltpu.VMEM((1, 4096), I32),
            pltpu.VMEM((32, 128), I32),
            pltpu.VMEM((32, 128), I32),
            pltpu.VMEM((32, 128), F32),
            pltpu.VMEM((32, 128), F32),
            pltpu.VMEM((32, 128), F32),
            block, block, block, block, block, block,
            pltpu.VMEM((OWN, 1, 128), F32),
            pltpu.VMEM((1, 128), F32),
            pltpu.VMEM((4, 1, 128), F32),
            pltpu.VMEM((1, 128), F32),
            dma((2,)), dma((7,)), dma((2,)), dma((2,)), dma, dma, dma, dma, dma, dma,
        ],
        compiler_params=pltpu.CompilerParams(
            collective_id=0, has_side_effects=True, vmem_limit_bytes=60000000
        ),
        name="main",
    )(fields, sq(order), order.reshape(1, 4096), sq(rows), sq(cols), sq(rf), sq(cf), sq(w))


def run_store(ov, obs, trace):
    vm = pl.BlockSpec(memory_space=pltpu.VMEM)
    anywhere = pl.BlockSpec(memory_space=pl.ANY)
    return pl.pallas_call(
        store_kernel,
        out_shape=(
            jax.ShapeDtypeStruct((64, 4, 8192), BF),
            jax.ShapeDtypeStruct((64, 128), F32),
            jax.ShapeDtypeStruct((1, 1), F32),
        ),
        in_specs=[vm] * 3,
        out_specs=(anywhere, vm, pl.BlockSpec(memory_space=pltpu.SMEM)),
        scratch_shapes=[pltpu.SemaphoreType.DMA],
        compiler_params=pltpu.CompilerParams(vmem_limit_bytes=8 * 1024 * 1024),
        name="store",
    )(ov, obs, trace)


def body(fields, rows, cols, rf, cf, w, order):
    ov, obs, trace = run_main(fields, rows, cols, rf, cf, w, order)
    adjoint, observed, trace = run_store(ov, obs, trace)
    return adjoint, observed, trace.reshape(())


def solution(mesh):
    return jax.shard_map(
        body,
        mesh=mesh,
        in_specs=(P("probe", "slab", None), P(), P(), P(), P(), P(), P()),
        out_specs=(P("probe", "slab", None), P("probe", "slab"), P()),
        check_vma=False,
    )
```

```python
import jax
import jax.numpy as jnp
from jax import lax
from jax.experimental import pallas as pl
from jax.experimental.pallas import tpu as pltpu
from jax.sharding import PartitionSpec as P

F32 = jnp.float32
BF = jnp.bfloat16
I32 = jnp.int32
MESH = pl.DeviceIdType.MESH

OWN = 32
RANK = 16
LIST = OWN * RANK
HALF = LIST // 2


def iota(shape, dim):
    return lax.broadcasted_iota(I32, shape, dim)


def mm(a, b):
    return lax.dot_general(a, b, (((1,), (0,)), ((), ())), preferred_element_type=F32)


def mm_nt(a, b):
    return lax.dot_general(a, b, (((1,), (1,)), ((), ())), preferred_element_type=F32)


def two(x):
    high = x.astype(BF)
    return high, (x - high.astype(F32)).astype(BF)


def mm_two(a, x):
    high, low = two(x)
    return mm(a, high) + mm(a, low)


def row_weights(row, rhi):
    sub = iota((8, row.shape[1]), 0) % 4
    return jnp.where(sub == row, 1.0 - rhi, 0.0) + jnp.where(sub == row + 1, rhi, 0.0)


def times_rows(x, weights8):
    rows, slots = x.shape
    return (x.reshape(rows // 8, 8, slots) * weights8[None]).reshape(rows, slots)


def prep(s, ord_ref, line_ref, rows_ref, cols_ref, rf_ref, cf_ref, w_ref, rscr, rkscr):
    line = line_ref[...]
    onehot = (iota((128, 4096), 0) == (line & 127)).astype(F32).astype(BF)
    found = mm(rows_ref[...].astype(F32).astype(BF), onehot)
    picked = jnp.where(iota((32, 4096), 0) == (line >> 7), found, 0.0)
    slot_rows = jnp.sum(picked, axis=0, keepdims=True)
    for o in range(OWN):
        rscr[o : o + 1, :] = slot_rows[:, o * 128 : o * 128 + 128]
    rows = rscr[...].astype(I32)
    slab = rows >> 2
    upper = (iota((128, 128), 0) < iota((128, 128), 1)).astype(F32).astype(BF)
    sel = []
    for which in range(2):
        mask = slab == s - which
        maskf = jnp.where(mask, 1.0, 0.0)
        rank = mm(maskf.astype(BF), upper)
        rkscr[which] = jnp.where(mask, rank, -1.0)
    lane8 = iota((8, 128), 0).astype(F32)
    for which in range(2):
        for jh in range(2):
            for o in range(OWN):
                sel.append(jnp.where(rkscr[which, o : o + 1, :] == lane8 + 8.0 * jh, 1.0, 0.0))
    sel = jnp.concatenate(sel, axis=0).astype(BF)
    ids = ord_ref[...]
    parts = jnp.concatenate(
        [(ids >> 7).astype(F32), (ids & 127).astype(F32), jnp.ones((32, 128), F32)], axis=0
    ).astype(BF)
    got = mm_nt(parts, sel)
    mine = iota((32, 1024), 0) == ((iota((32, 1024), 1) & 255) >> 3)
    high = jnp.sum(jnp.where(mine, got[0:32], 0.0), axis=0, keepdims=True)
    low = jnp.sum(jnp.where(mine, got[32:64], 0.0), axis=0, keepdims=True)
    valid = jnp.sum(jnp.where(mine, got[64:96], 0.0), axis=0, keepdims=True) > 0.5
    onehot = (iota((128, 1024), 0).astype(F32) == low).astype(F32).astype(BF)
    cols = cols_ref[...]
    rf_hi, rf_lo = two(rf_ref[...])
    w_hi, w_lo = two(w_ref[...])
    cf = cf_ref[...]
    parts = jnp.concatenate(
        [
            (cols >> 7).astype(F32).astype(BF),
            (cols & 127).astype(F32).astype(BF),
            (1.0 - cf).astype(BF),
            cf.astype(BF),
            rf_hi,
            rf_lo,
            w_hi,
            w_lo,
            rows_ref[...].astype(F32).astype(BF),
        ],
        axis=0,
    )
    got = mm(parts, onehot)
    mine = iota((32, 1024), 0).astype(F32) == high
    vals = [
        jnp.sum(jnp.where(mine, got[32 * i : 32 * i + 32], 0.0), axis=0, keepdims=True)
        for i in range(9)
    ]
    rhi = vals[4] + vals[5]
    weight = vals[6] + vals[7]
    grid_row = vals[8].astype(I32) - 4 * s
    second = iota((1, 1024), 1) >= LIST
    use = valid & ((~second) | (grid_row == -1))
    col = jnp.where(use, (vals[0] * 128.0 + vals[1]).astype(I32), -8)
    grid_row = jnp.where(use, grid_row, -8)
    return col, vals[2], vals[3], grid_row, rhi, weight, rows, slab


def reduce_matrix():
    a = iota((512, 128), 0)
    b = iota((512, 128), 1)
    return (b == ((a >> 8) * 64 + ((a & 255) >> 2))).astype(F32).astype(BF)


def fields_chunk(xv, first, count):
    return jnp.concatenate([xv[first + i] for i in range(count)], axis=1)


def spread_out(rows):
    flat = [r for group in rows for r in group]
    where = [i for i, group in enumerate(rows) for _ in group]
    stack = jnp.concatenate([r.astype(F32) for r in flat], axis=0)
    pad = 16 - len(flat)
    stack = jnp.concatenate([stack, jnp.zeros((pad, stack.shape[1]), F32)], axis=0).astype(BF)
    width = 128 * len(rows)
    a = iota((16, width), 0)
    group = jnp.full((16, width), -1, I32)
    for i, g in enumerate(where):
        group = jnp.where(a == i, g, group)
    pick = (group == (iota((16, width), 1) >> 7)).astype(F32).astype(BF)
    out = lax.dot_general(stack, pick, (((0,), (0,)), ((), ())), preferred_element_type=F32)
    return [out[:, 128 * i : 128 * i + 128] for i in range(len(rows))]


def weighted_source(full, weight, weights8, dst):
    a = iota((256, 128), 0)
    b = iota((256, 128), 1)
    high, low = two(full)
    for jh in range(2):
        cut = slice(jh * HALF, jh * HALF + HALF)
        pick = (b == (jh * 64 + (a >> 2))).astype(F32).astype(BF)
        value = mm_nt(pick, high) + mm_nt(pick, low)
        value = value * weight[:, cut]
        dst[:, cut] = times_rows(value, weights8[:, cut]).astype(BF)


def main_kernel(
    x_ref, ord_ref, line_ref, rows_ref, cols_ref, rf_ref, cf_ref, w_ref,
    ov, obs_ref, trace_ref,
    xv, reps, tabs, partial, src, rscr, rkscr,
    ordv, linev, rowsv, colsv, rfv, cfv, wv,
    mine_a, mine_b, full_a, next_box, prev_box, box, sums, ready, group, group_ready,
    x_sem, in_sem, halo_send, halo_recv, own_send, own_recv, sum_send, sum_recv,
    group_send, group_recv,
):
    s = lax.axis_index("slab")
    z = lax.axis_index("probe")
    small = [
        (ord_ref, ordv), (line_ref, linev), (rows_ref, rowsv), (cols_ref, colsv),
        (rf_ref, rfv), (cf_ref, cfv), (w_ref, wv),
    ]
    small = [pltpu.make_async_copy(a, b, in_sem.at[i]) for i, (a, b) in enumerate(small)]
    for copy in small:
        copy.start()
    barrier = pltpu.get_barrier_semaphore()

    def greet(d, carry):
        t = lax.rem(s + d, OWN)
        pl.semaphore_signal(
            barrier, inc=1, device_id={"slab": t, "probe": z}, device_id_type=MESH
        )
        return carry

    lax.fori_loop(1, OWN, greet, 0)
    for d in range(1, 4):
        pl.semaphore_signal(
            barrier, inc=1, device_id={"slab": s, "probe": lax.rem(z + d, 4)}, device_id_type=MESH
        )
    flat = x_ref.reshape(256, 8192)
    for c in range(64):
        pltpu.make_async_copy(
            flat.at[:, pl.ds(c * 128, 128)], xv.at[c], x_sem.at[c // 32]
        ).start()
    for copy in small:
        copy.wait()
    col, clo, chi, grid_row, rhi, weight, rows, slab = prep(
        s, ordv, linev, rowsv, colsv, rfv, cfv, wv, rscr, rkscr
    )
    slabf = slab.astype(F32)
    slot_slab = jnp.sum(jnp.where(iota((32, 128), 0) == s, slabf, 0.0), axis=0, keepdims=True)
    square = jnp.broadcast_to(slot_slab, (128, 128))
    same = (square.T == square) & (iota((128, 128), 0) < iota((128, 128), 1))
    slot_rank = jnp.sum(jnp.where(same, 1.0, 0.0), axis=0, keepdims=True).astype(I32)
    slot_slab = slot_slab.astype(I32)
    weights8 = row_weights(grid_row, rhi)
    reduce = reduce_matrix()
    zero = jnp.zeros((), BF)

    def prepare(which):
        cut = slice(which * LIST, which * LIST + LIST)
        columns = col[:, cut]
        rhi_high, rhi_low = two(rhi[:, cut])
        block, lane, low, high, row, upper = spread_out(
            [
                [(columns >> 8).astype(F32).astype(BF)],
                [(columns & 255).astype(F32).astype(BF)],
                [clo[:, cut].astype(BF)],
                [chi[:, cut].astype(BF)],
                [grid_row[:, cut].astype(F32).astype(BF)],
                [rhi_high, rhi_low],
            ]
        )
        block, lane, low, high = [
            jnp.concatenate([x, x], axis=1) for x in (block, lane, low, high)
        ]
        here = iota((LIST, 256), 1).astype(F32)
        reps[which, 0] = block.astype(BF)
        reps[which, 1] = jnp.where(
            here == lane, low, jnp.where(here == lane + 1.0, high, 0.0)
        ).astype(BF)
        reps[which, 2] = jnp.where((lane == 255.0) & (here == 0.0), high, 0.0).astype(BF)
        quarter = (iota((LIST, 128), 1) & 3).astype(F32)
        factor = jnp.where(quarter == row, 1.0 - upper, jnp.where(quarter == row + 1.0, upper, 0.0))
        return factor

    def forward(which, factor, between):
        def build(i):
            for g in range(0, LIST, 64):
                rows = slice(g, g + 64)
                at = reps[which, 0, rows]
                inside = reps[which, 1, rows]
                over = reps[which, 2, rows]
                for j in range(4):
                    b = 4 * i + j
                    tabs[which, b, rows] = jnp.where(
                        at == b, inside, jnp.where(at == b - 1, over, zero)
                    )

        def product(i, half):
            rows = slice(half * HALF, half * HALF + HALF)
            tab = jnp.concatenate([tabs[which, 4 * i + j, rows] for j in range(4)], axis=1)
            return mm_nt(tab, fields_chunk(xv, 8 * i, 8))

        def arrive(i):
            view = xv.at[pl.ds(32 * i, 32)]
            pltpu.make_async_copy(view, view, x_sem.at[i]).wait()

        build(0)
        total = [None, None]
        for i in range(8):
            if which == 1 and i % 4 == 0:
                arrive(i // 4)
            if i < 7:
                build(i + 1)
            if i == 4 and between is not None:
                between()
            for half in range(2):
                part = product(i, half)
                total[half] = part if i == 0 else total[half] + part
        both = []
        for half in range(2):
            scale = factor[half * HALF : half * HALF + HALF]
            both.append(total[half] * jnp.concatenate([scale, scale], axis=1))
        both = jnp.concatenate(both, axis=1)
        high, low = two(both)
        return (mm(high, reduce) + mm(low, reduce)).reshape(OWN, 8, 128)

    factor_b = prepare(1)
    factor_a = []
    mine_b[...] = forward(1, factor_b, lambda: factor_a.append(prepare(0)))
    pl.semaphore_wait(barrier, OWN + 2)
    to_prev = pltpu.make_async_remote_copy(
        mine_b, next_box, halo_send.at[0], halo_recv.at[0],
        {"slab": lax.rem(s + OWN - 1, OWN), "probe": z}, MESH,
    )
    to_prev.start()
    mine_a[...] = forward(0, factor_a[0], None)
    to_next = pltpu.make_async_remote_copy(
        mine_a, prev_box, halo_send.at[1], halo_recv.at[1],
        {"slab": lax.rem(s + 1, OWN), "probe": z}, MESH,
    )
    to_next.start()
    to_prev.wait_recv()
    complete = mine_a[...] + next_box[...]
    full_a[...] = complete
    value_a = complete.reshape(HALF, 128)
    side = (iota((8, 128), 0) == (iota((8, 128), 1) >> 6)).astype(F32).astype(BF)
    high, low = two(value_a * value_a)
    squares = mm_nt(side, high) + mm_nt(side, low)
    total = jnp.sum(
        squares[0:1] * weight[:, 0:HALF] + squares[1:2] * weight[:, HALF:LIST]
    )
    ready[...] = jnp.full((1, 128), 1.0, F32) * total

    for d in range(1, 4):
        pltpu.make_async_remote_copy(
            ready, group.at[z], group_send, group_recv,
            {"slab": s, "probe": lax.rem(z + d, 4)}, MESH,
        ).start()
    group[z] = ready[...]

    def send_own(d, carry):
        t = lax.rem(s + d, OWN)
        pltpu.make_async_remote_copy(
            full_a.at[t], box.at[s], own_send, own_recv, {"slab": t, "probe": z}, MESH
        ).start()
        return carry

    lax.fori_loop(1, OWN, send_own, 0)
    box[s] = full_a[s]
    weighted_source(value_a, weight[:, 0:LIST], weights8[:, 0:LIST], src)

    def adjoint_a(i, carry):
        for j in range(4):
            partial[4 * i + j] = mm(src[...], tabs[0, 4 * i + j])
        return carry

    lax.fori_loop(0, 8, adjoint_a, 0)
    view = group.at[pl.ds(0, 3)]
    pltpu.make_async_copy(view, view, group_recv).wait()
    group_ready[...] = jnp.sum(group[...], axis=0)

    def send_sum(d, carry):
        t = lax.rem(s + d, OWN)
        pltpu.make_async_remote_copy(
            group_ready, sums.at[s], sum_send, sum_recv, {"slab": t, "probe": z}, MESH
        ).start()
        return carry

    lax.fori_loop(1, OWN, send_sum, 0)
    sums[s] = group_ready[...]
    to_next.wait_recv()
    value_b = (mine_b[...] + prev_box[...]).reshape(HALF, 128)
    weighted_source(value_b, weight[:, LIST:], weights8[:, LIST:], src)

    def adjoint_b(i, carry):
        for j in range(4):
            got = (partial[4 * i + j] + mm(src[...], tabs[1, 4 * i + j])).astype(BF)
            ov[4 * i + j] = got
        return carry

    lax.fori_loop(0, 8, adjoint_b, 0)
    view = box.at[pl.ds(0, OWN - 1)]
    pltpu.make_async_copy(view, view, own_recv).wait()
    full = box[...].reshape(HALF, 128).T
    sub = iota((HALF, 128), 0)
    pick = ((sub >> 3) == slot_slab) & ((sub & 7) == (slot_rank & 7))
    pick = jnp.where(pick, 1.0, 0.0).astype(BF)
    high, low = two(full)
    got = mm(high, pick) + mm(low, pick)
    obs_ref[...] = jnp.where(slot_rank < 8, got[0:64], got[64:128])
    view = sums.at[pl.ds(0, OWN - 1)]
    pltpu.make_async_copy(view, view, sum_recv).wait()
    trace_ref[...] = jnp.sum(sums[...], axis=0) * (1.0 / 1048576.0)
    to_prev.wait_send()
    to_next.wait_send()
    pltpu.make_async_copy(view, view, sum_send).wait()
    view = group.at[pl.ds(0, 3)]
    pltpu.make_async_copy(view, view, group_send).wait()
    view = box.at[pl.ds(0, OWN - 1)]
    pltpu.make_async_copy(view, view, own_send).wait()


def store_kernel(ov, obs_in, trace_in, out_ref, obs_ref, trace_ref, sem):
    flat = out_ref.reshape(256, 8192)
    for c in range(64):
        half = ov.at[c // 2, :, pl.ds((c % 2) * 128, 128)]
        pltpu.make_async_copy(half, flat.at[:, pl.ds(c * 128, 128)], sem).start()
    obs_ref[...] = obs_in[...]
    trace_ref[0, 0] = trace_in[0, 0]
    pltpu.make_async_copy(ov, ov, sem).wait()


def run_main(fields, rows, cols, rf, cf, w, order):
    vm = pl.BlockSpec(memory_space=pltpu.VMEM)
    anywhere = pl.BlockSpec(memory_space=pl.ANY)
    dma = pltpu.SemaphoreType.DMA
    sq = lambda x: x.reshape(32, 128)
    block = pltpu.VMEM((OWN, 8, 128), F32)
    return pl.pallas_call(
        main_kernel,
        out_shape=(
            pltpu.VMEM((32, 256, 256), BF),
            pltpu.VMEM((64, 128), F32),
            pltpu.VMEM((1, 128), F32),
        ),
        in_specs=[anywhere] * 8,
        out_specs=(vm, vm, vm),
        scratch_shapes=[
            pltpu.VMEM((64, 256, 128), BF),
            pltpu.VMEM((2, 3, LIST, 256), BF),
            pltpu.VMEM((2, 32, LIST, 256), BF),
            pltpu.VMEM((32, 256, 256), F32),
            pltpu.VMEM((256, LIST), BF),
            pltpu.VMEM((32, 128), F32),
            pltpu.VMEM((2, 32, 128), F32),
            pltpu.VMEM((32, 128), I32),
            pltpu.VMEM((1, 4096), I32),
            pltpu.VMEM((32, 128), I32),
            pltpu.VMEM((32, 128), I32),
            pltpu.VMEM((32, 128), F32),
            pltpu.VMEM((32, 128), F32),
            pltpu.VMEM((32, 128), F32),
            block, block, block, block, block, block,
            pltpu.VMEM((OWN, 1, 128), F32),
            pltpu.VMEM((1, 128), F32),
            pltpu.VMEM((4, 1, 128), F32),
            pltpu.VMEM((1, 128), F32),
            dma((2,)), dma((7,)), dma((2,)), dma((2,)), dma, dma, dma, dma, dma, dma,
        ],
        compiler_params=pltpu.CompilerParams(
            collective_id=0, has_side_effects=True, vmem_limit_bytes=60000000
        ),
        name="main",
    )(fields, sq(order), order.reshape(1, 4096), sq(rows), sq(cols), sq(rf), sq(cf), sq(w))


def run_store(ov, obs, trace):
    vm = pl.BlockSpec(memory_space=pltpu.VMEM)
    anywhere = pl.BlockSpec(memory_space=pl.ANY)
    return pl.pallas_call(
        store_kernel,
        out_shape=(
            jax.ShapeDtypeStruct((64, 4, 8192), BF),
            jax.ShapeDtypeStruct((64, 128), F32),
            jax.ShapeDtypeStruct((1, 1), F32),
        ),
        in_specs=[vm] * 3,
        out_specs=(anywhere, vm, pl.BlockSpec(memory_space=pltpu.SMEM)),
        scratch_shapes=[pltpu.SemaphoreType.DMA],
        compiler_params=pltpu.CompilerParams(vmem_limit_bytes=8 * 1024 * 1024),
        name="store",
    )(ov, obs, trace)


def body(fields, rows, cols, rf, cf, w, order):
    ov, obs, trace = run_main(fields, rows, cols, rf, cf, w, order)
    adjoint, observed, trace = run_store(ov, obs, trace)
    return adjoint, observed, trace.reshape(())


def solution(mesh):
    return jax.shard_map(
        body,
        mesh=mesh,
        in_specs=(P("probe", "slab", None), P(), P(), P(), P(), P(), P()),
        out_specs=(P("probe", "slab", None), P("probe", "slab"), P()),
        check_vma=False,
    )
```

```python
import jax
import jax.numpy as jnp
from jax import lax
from jax.experimental import pallas as pl
from jax.experimental.pallas import tpu as pltpu
from jax.sharding import PartitionSpec as P

F32 = jnp.float32
BF = jnp.bfloat16
I32 = jnp.int32
MESH = pl.DeviceIdType.MESH

OWN = 32
RANK = 16
LIST = OWN * RANK
HALF = LIST // 2


def iota(shape, dim):
    return lax.broadcasted_iota(I32, shape, dim)


def mm(a, b):
    return lax.dot_general(a, b, (((1,), (0,)), ((), ())), preferred_element_type=F32)


def mm_nt(a, b):
    return lax.dot_general(a, b, (((1,), (1,)), ((), ())), preferred_element_type=F32)


def two(x):
    high = x.astype(BF)
    return high, (x - high.astype(F32)).astype(BF)


def mm_two(a, x):
    high, low = two(x)
    return mm(a, high) + mm(a, low)


def row_weights(row, rhi):
    sub = iota((8, row.shape[1]), 0) % 4
    return jnp.where(sub == row, 1.0 - rhi, 0.0) + jnp.where(sub == row + 1, rhi, 0.0)


def times_rows(x, weights8):
    rows, slots = x.shape
    return (x.reshape(rows // 8, 8, slots) * weights8[None]).reshape(rows, slots)


def prep(s, ord_ref, line_ref, rows_ref, cols_ref, rf_ref, cf_ref, w_ref, rscr, rkscr):
    line = line_ref[...]
    onehot = (iota((128, 4096), 0) == (line & 127)).astype(F32).astype(BF)
    found = mm(rows_ref[...].astype(F32).astype(BF), onehot)
    picked = jnp.where(iota((32, 4096), 0) == (line >> 7), found, 0.0)
    slot_rows = jnp.sum(picked, axis=0, keepdims=True)
    for o in range(OWN):
        rscr[o : o + 1, :] = slot_rows[:, o * 128 : o * 128 + 128]
    rows = rscr[...].astype(I32)
    slab = rows >> 2
    upper = (iota((128, 128), 0) < iota((128, 128), 1)).astype(F32).astype(BF)
    sel = []
    for which in range(2):
        mask = slab == s - which
        maskf = jnp.where(mask, 1.0, 0.0)
        rank = mm(maskf.astype(BF), upper)
        rkscr[which] = jnp.where(mask, rank, -1.0)
    lane8 = iota((8, 128), 0).astype(F32)
    for which in range(2):
        for jh in range(2):
            for o in range(OWN):
                sel.append(jnp.where(rkscr[which, o : o + 1, :] == lane8 + 8.0 * jh, 1.0, 0.0))
    sel = jnp.concatenate(sel, axis=0).astype(BF)
    ids = ord_ref[...]
    parts = jnp.concatenate(
        [(ids >> 7).astype(F32), (ids & 127).astype(F32), jnp.ones((32, 128), F32)], axis=0
    ).astype(BF)
    got = mm_nt(parts, sel)
    mine = iota((32, 1024), 0) == ((iota((32, 1024), 1) & 255) >> 3)
    high = jnp.sum(jnp.where(mine, got[0:32], 0.0), axis=0, keepdims=True)
    low = jnp.sum(jnp.where(mine, got[32:64], 0.0), axis=0, keepdims=True)
    valid = jnp.sum(jnp.where(mine, got[64:96], 0.0), axis=0, keepdims=True) > 0.5
    onehot = (iota((128, 1024), 0).astype(F32) == low).astype(F32).astype(BF)
    cols = cols_ref[...]
    rf_hi, rf_lo = two(rf_ref[...])
    w_hi, w_lo = two(w_ref[...])
    cf = cf_ref[...]
    parts = jnp.concatenate(
        [
            (cols >> 7).astype(F32).astype(BF),
            (cols & 127).astype(F32).astype(BF),
            (1.0 - cf).astype(BF),
            cf.astype(BF),
            rf_hi,
            rf_lo,
            w_hi,
            w_lo,
            rows_ref[...].astype(F32).astype(BF),
        ],
        axis=0,
    )
    got = mm(parts, onehot)
    mine = iota((32, 1024), 0).astype(F32) == high
    vals = [
        jnp.sum(jnp.where(mine, got[32 * i : 32 * i + 32], 0.0), axis=0, keepdims=True)
        for i in range(9)
    ]
    rhi = vals[4] + vals[5]
    weight = vals[6] + vals[7]
    grid_row = vals[8].astype(I32) - 4 * s
    second = iota((1, 1024), 1) >= LIST
    use = valid & ((~second) | (grid_row == -1))
    col = jnp.where(use, (vals[0] * 128.0 + vals[1]).astype(I32), -8)
    grid_row = jnp.where(use, grid_row, -8)
    return col, vals[2], vals[3], grid_row, rhi, weight, rows, slab


def reduce_matrix():
    a = iota((512, 128), 0)
    b = iota((512, 128), 1)
    return (b == ((a >> 8) * 64 + ((a & 255) >> 2))).astype(F32).astype(BF)


def fields_chunk(xv, first, count):
    return jnp.concatenate([xv[first + i] for i in range(count)], axis=1)


def spread_out(rows):
    flat = [r for group in rows for r in group]
    where = [i for i, group in enumerate(rows) for _ in group]
    stack = jnp.concatenate([r.astype(F32) for r in flat], axis=0)
    pad = 16 - len(flat)
    stack = jnp.concatenate([stack, jnp.zeros((pad, stack.shape[1]), F32)], axis=0).astype(BF)
    width = 128 * len(rows)
    a = iota((16, width), 0)
    group = jnp.full((16, width), -1, I32)
    for i, g in enumerate(where):
        group = jnp.where(a == i, g, group)
    pick = (group == (iota((16, width), 1) >> 7)).astype(F32).astype(BF)
    out = lax.dot_general(stack, pick, (((0,), (0,)), ((), ())), preferred_element_type=F32)
    return [out[:, 128 * i : 128 * i + 128] for i in range(len(rows))]


def weighted_source(full, weight, weights8, dst):
    a = iota((256, 128), 0)
    b = iota((256, 128), 1)
    high, low = two(full)
    for jh in range(2):
        cut = slice(jh * HALF, jh * HALF + HALF)
        pick = (b == (jh * 64 + (a >> 2))).astype(F32).astype(BF)
        value = mm_nt(pick, high) + mm_nt(pick, low)
        value = value * weight[:, cut]
        dst[:, cut] = times_rows(value, weights8[:, cut]).astype(BF)


def far_first():
    hops = lambda d: min(d, 4 - d)
    steps = [
        (y, x, c, z) for y in range(4) for x in range(4) for c in range(2) for z in range(4)
    ][1:]
    return sorted(steps, key=lambda d: -(hops(d[0]) + hops(d[1]) + hops(d[3])))


STEPS = far_first()


def main_kernel(
    x_ref, ord_ref, line_ref, rows_ref, cols_ref, rf_ref, cf_ref, w_ref,
    ov, obs_ref, trace_ref,
    xv, reps, tabs, partial, src, rscr, rkscr,
    ordv, linev, rowsv, colsv, rfv, cfv, wv,
    mine_a, mine_b, full_a, next_box, prev_box, box, sums, ready,
    x_sem, in_sem, halo_send, halo_recv, own_send, own_recv, sum_send, sum_recv,
):
    s = lax.axis_index("slab")
    z = lax.axis_index("probe")
    small = [
        (ord_ref, ordv), (line_ref, linev), (rows_ref, rowsv), (cols_ref, colsv),
        (rf_ref, rfv), (cf_ref, cfv), (w_ref, wv),
    ]
    small = [pltpu.make_async_copy(a, b, in_sem.at[i]) for i, (a, b) in enumerate(small)]
    for copy in small:
        copy.start()
    barrier = pltpu.get_barrier_semaphore()

    place = (s // 8, lax.rem(s // 2, 4), lax.rem(s, 2), z)
    moved = [
        [lax.rem(at + d, length) for d in range(length)]
        for at, length in zip(place, (4, 4, 2, 4))
    ]

    def other(step):
        y, x, core, level = (m[d] for m, d in zip(moved, step))
        return {"slab": y * 8 + x * 2 + core, "probe": level}

    for step in STEPS:
        pl.semaphore_signal(barrier, inc=1, device_id=other(step), device_id_type=MESH)
    flat = x_ref.reshape(256, 8192)
    for c in range(64):
        pltpu.make_async_copy(
            flat.at[:, pl.ds(c * 128, 128)], xv.at[c], x_sem.at[c // 32]
        ).start()
    for copy in small:
        copy.wait()
    col, clo, chi, grid_row, rhi, weight, rows, slab = prep(
        s, ordv, linev, rowsv, colsv, rfv, cfv, wv, rscr, rkscr
    )
    slabf = slab.astype(F32)
    slot_slab = jnp.sum(jnp.where(iota((32, 128), 0) == s, slabf, 0.0), axis=0, keepdims=True)
    square = jnp.broadcast_to(slot_slab, (128, 128))
    same = (square.T == square) & (iota((128, 128), 0) < iota((128, 128), 1))
    slot_rank = jnp.sum(jnp.where(same, 1.0, 0.0), axis=0, keepdims=True).astype(I32)
    slot_slab = slot_slab.astype(I32)
    weights8 = row_weights(grid_row, rhi)
    reduce = reduce_matrix()
    zero = jnp.zeros((), BF)

    def prepare(which):
        cut = slice(which * LIST, which * LIST + LIST)
        columns = col[:, cut]
        rhi_high, rhi_low = two(rhi[:, cut])
        block, lane, low, high, row, upper = spread_out(
            [
                [(columns >> 8).astype(F32).astype(BF)],
                [(columns & 255).astype(F32).astype(BF)],
                [clo[:, cut].astype(BF)],
                [chi[:, cut].astype(BF)],
                [grid_row[:, cut].astype(F32).astype(BF)],
                [rhi_high, rhi_low],
            ]
        )
        block, lane, low, high = [
            jnp.concatenate([x, x], axis=1) for x in (block, lane, low, high)
        ]
        here = iota((LIST, 256), 1).astype(F32)
        reps[which, 0] = block.astype(BF)
        reps[which, 1] = jnp.where(
            here == lane, low, jnp.where(here == lane + 1.0, high, 0.0)
        ).astype(BF)
        reps[which, 2] = jnp.where((lane == 255.0) & (here == 0.0), high, 0.0).astype(BF)
        quarter = (iota((LIST, 128), 1) & 3).astype(F32)
        factor = jnp.where(quarter == row, 1.0 - upper, jnp.where(quarter == row + 1.0, upper, 0.0))
        return factor

    def forward(which, factor, between):
        def build(i):
            for g in range(0, LIST, 64):
                rows = slice(g, g + 64)
                at = reps[which, 0, rows]
                inside = reps[which, 1, rows]
                over = reps[which, 2, rows]
                for j in range(4):
                    b = 4 * i + j
                    tabs[which, b, rows] = jnp.where(
                        at == b, inside, jnp.where(at == b - 1, over, zero)
                    )

        def product(i, half):
            rows = slice(half * HALF, half * HALF + HALF)
            tab = jnp.concatenate([tabs[which, 4 * i + j, rows] for j in range(4)], axis=1)
            return mm_nt(tab, fields_chunk(xv, 8 * i, 8))

        def arrive(i):
            view = xv.at[pl.ds(32 * i, 32)]
            pltpu.make_async_copy(view, view, x_sem.at[i]).wait()

        build(0)
        total = [None, None]
        for i in range(8):
            if which == 1 and i % 4 == 0:
                arrive(i // 4)
            if i < 7:
                build(i + 1)
            if i == 4 and between is not None:
                between()
            for half in range(2):
                part = product(i, half)
                total[half] = part if i == 0 else total[half] + part
        both = []
        for half in range(2):
            scale = factor[half * HALF : half * HALF + HALF]
            both.append(total[half] * jnp.concatenate([scale, scale], axis=1))
        both = jnp.concatenate(both, axis=1)
        high, low = two(both)
        return (mm(high, reduce) + mm(low, reduce)).reshape(OWN, 8, 128)

    factor_b = prepare(1)
    factor_a = []
    mine_b[...] = forward(1, factor_b, lambda: factor_a.append(prepare(0)))
    pl.semaphore_wait(barrier, 127)
    to_prev = pltpu.make_async_remote_copy(
        mine_b, next_box, halo_send.at[0], halo_recv.at[0],
        {"slab": lax.rem(s + OWN - 1, OWN), "probe": z}, MESH,
    )
    to_prev.start()
    mine_a[...] = forward(0, factor_a[0], None)
    to_next = pltpu.make_async_remote_copy(
        mine_a, prev_box, halo_send.at[1], halo_recv.at[1],
        {"slab": lax.rem(s + 1, OWN), "probe": z}, MESH,
    )
    to_next.start()
    to_prev.wait_recv()
    complete = mine_a[...] + next_box[...]
    full_a[...] = complete
    value_a = complete.reshape(HALF, 128)
    side = (iota((8, 128), 0) == (iota((8, 128), 1) >> 6)).astype(F32).astype(BF)
    high, low = two(value_a * value_a)
    squares = mm_nt(side, high) + mm_nt(side, low)
    total = jnp.sum(
        squares[0:1] * weight[:, 0:HALF] + squares[1:2] * weight[:, HALF:LIST]
    )
    ready[...] = jnp.full((1, 128), 1.0, F32) * total

    me = s * 4 + z
    for step in STEPS:
        pltpu.make_async_remote_copy(
            ready, sums.at[me], sum_send, sum_recv, other(step), MESH
        ).start()
    sums[me] = ready[...]
    to_prev.wait_send()

    def send_own(d):
        t = lax.rem(s + d, OWN)
        pltpu.make_async_remote_copy(
            full_a.at[t], box.at[s], own_send, own_recv, {"slab": t, "probe": z}, MESH
        ).start()

    box[s] = full_a[s]
    weighted_source(value_a, weight[:, 0:LIST], weights8[:, 0:LIST], src)

    for i in range(32):
        partial[i] = mm(src[...], tabs[0, i])
        if i < OWN - 1:
            send_own(i + 1)
    to_next.wait_recv()
    value_b = (mine_b[...] + prev_box[...]).reshape(HALF, 128)
    weighted_source(value_b, weight[:, LIST:], weights8[:, LIST:], src)

    for i in range(32):
        ov[i] = (partial[i] + mm(src[...], tabs[1, i])).astype(BF)
    view = box.at[pl.ds(0, OWN - 1)]
    pltpu.make_async_copy(view, view, own_recv).wait()
    full = box[...].reshape(HALF, 128).T
    sub = iota((HALF, 128), 0)
    pick = ((sub >> 3) == slot_slab) & ((sub & 7) == (slot_rank & 7))
    pick = jnp.where(pick, 1.0, 0.0).astype(BF)
    high, low = two(full)
    got = mm(high, pick) + mm(low, pick)
    obs_ref[...] = jnp.where(slot_rank < 8, got[0:64], got[64:128])
    view = sums.at[pl.ds(0, 127)]
    pltpu.make_async_copy(view, view, sum_recv).wait()
    trace_ref[...] = jnp.sum(sums[...], axis=0) * (1.0 / 1048576.0)
    to_next.wait_send()
    pltpu.make_async_copy(view, view, sum_send).wait()
    view = box.at[pl.ds(0, OWN - 1)]
    pltpu.make_async_copy(view, view, own_send).wait()


def store_kernel(ov, obs_in, trace_in, out_ref, obs_ref, trace_ref, sem):
    flat = out_ref.reshape(256, 8192)
    for c in range(64):
        half = ov.at[c // 2, :, pl.ds((c % 2) * 128, 128)]
        pltpu.make_async_copy(half, flat.at[:, pl.ds(c * 128, 128)], sem).start()
    obs_ref[...] = obs_in[...]
    trace_ref[0, 0] = trace_in[0, 0]
    pltpu.make_async_copy(ov, ov, sem).wait()


def run_main(fields, rows, cols, rf, cf, w, order):
    vm = pl.BlockSpec(memory_space=pltpu.VMEM)
    anywhere = pl.BlockSpec(memory_space=pl.ANY)
    dma = pltpu.SemaphoreType.DMA
    sq = lambda x: x.reshape(32, 128)
    block = pltpu.VMEM((OWN, 8, 128), F32)
    return pl.pallas_call(
        main_kernel,
        out_shape=(
            pltpu.VMEM((32, 256, 256), BF),
            pltpu.VMEM((64, 128), F32),
            pltpu.VMEM((1, 128), F32),
        ),
        in_specs=[anywhere] * 8,
        out_specs=(vm, vm, vm),
        scratch_shapes=[
            pltpu.VMEM((64, 256, 128), BF),
            pltpu.VMEM((2, 3, LIST, 256), BF),
            pltpu.VMEM((2, 32, LIST, 256), BF),
            pltpu.VMEM((32, 256, 256), F32),
            pltpu.VMEM((256, LIST), BF),
            pltpu.VMEM((32, 128), F32),
            pltpu.VMEM((2, 32, 128), F32),
            pltpu.VMEM((32, 128), I32),
            pltpu.VMEM((1, 4096), I32),
            pltpu.VMEM((32, 128), I32),
            pltpu.VMEM((32, 128), I32),
            pltpu.VMEM((32, 128), F32),
            pltpu.VMEM((32, 128), F32),
            pltpu.VMEM((32, 128), F32),
            block, block, block, block, block, block,
            pltpu.VMEM((128, 1, 128), F32),
            pltpu.VMEM((1, 128), F32),
            dma((2,)), dma((7,)), dma((2,)), dma((2,)), dma, dma, dma, dma,
        ],
        compiler_params=pltpu.CompilerParams(
            collective_id=0, has_side_effects=True, vmem_limit_bytes=60000000
        ),
        name="main",
    )(fields, sq(order), order.reshape(1, 4096), sq(rows), sq(cols), sq(rf), sq(cf), sq(w))


def run_store(ov, obs, trace):
    vm = pl.BlockSpec(memory_space=pltpu.VMEM)
    anywhere = pl.BlockSpec(memory_space=pl.ANY)
    return pl.pallas_call(
        store_kernel,
        out_shape=(
            jax.ShapeDtypeStruct((64, 4, 8192), BF),
            jax.ShapeDtypeStruct((64, 128), F32),
            jax.ShapeDtypeStruct((1, 1), F32),
        ),
        in_specs=[vm] * 3,
        out_specs=(anywhere, vm, pl.BlockSpec(memory_space=pltpu.SMEM)),
        scratch_shapes=[pltpu.SemaphoreType.DMA],
        compiler_params=pltpu.CompilerParams(vmem_limit_bytes=8 * 1024 * 1024),
        name="store",
    )(ov, obs, trace)


def body(fields, rows, cols, rf, cf, w, order):
    ov, obs, trace = run_main(fields, rows, cols, rf, cf, w, order)
    adjoint, observed, trace = run_store(ov, obs, trace)
    return adjoint, observed, trace.reshape(())


def solution(mesh):
    return jax.shard_map(
        body,
        mesh=mesh,
        in_specs=(P("probe", "slab", None), P(), P(), P(), P(), P(), P()),
        out_specs=(P("probe", "slab", None), P("probe", "slab"), P()),
        check_vma=False,
    )
```

```python
import jax
import jax.numpy as jnp
from jax import lax
from jax.experimental import pallas as pl
from jax.experimental.pallas import tpu as pltpu
from jax.sharding import PartitionSpec as P

F32 = jnp.float32
BF = jnp.bfloat16
I32 = jnp.int32
MESH = pl.DeviceIdType.MESH

OWN = 32
RANK = 16
LIST = OWN * RANK
HALF = LIST // 2


def iota(shape, dim):
    return lax.broadcasted_iota(I32, shape, dim)


def mm(a, b):
    return lax.dot_general(a, b, (((1,), (0,)), ((), ())), preferred_element_type=F32)


def mm_nt(a, b):
    return lax.dot_general(a, b, (((1,), (1,)), ((), ())), preferred_element_type=F32)


def two(x):
    high = x.astype(BF)
    return high, (x - high.astype(F32)).astype(BF)


def mm_two(a, x):
    high, low = two(x)
    return mm(a, high) + mm(a, low)


def row_weights(row, rhi):
    sub = iota((8, row.shape[1]), 0) % 4
    return jnp.where(sub == row, 1.0 - rhi, 0.0) + jnp.where(sub == row + 1, rhi, 0.0)


def times_rows(x, weights8):
    rows, slots = x.shape
    return (x.reshape(rows // 8, 8, slots) * weights8[None]).reshape(rows, slots)


def prep(s, ord_ref, line_ref, rows_ref, cols_ref, rf_ref, cf_ref, w_ref, rscr, rkscr):
    line = line_ref[...]
    onehot = (iota((128, 4096), 0) == (line & 127)).astype(F32).astype(BF)
    found = mm(rows_ref[...].astype(F32).astype(BF), onehot)
    picked = jnp.where(iota((32, 4096), 0) == (line >> 7), found, 0.0)
    slot_rows = jnp.sum(picked, axis=0, keepdims=True)
    for o in range(OWN):
        rscr[o : o + 1, :] = slot_rows[:, o * 128 : o * 128 + 128]
    rows = rscr[...].astype(I32)
    slab = rows >> 2
    upper = (iota((128, 128), 0) < iota((128, 128), 1)).astype(F32).astype(BF)
    sel = []
    for which in range(2):
        mask = slab == s - which
        maskf = jnp.where(mask, 1.0, 0.0)
        rank = mm(maskf.astype(BF), upper)
        rkscr[which] = jnp.where(mask, rank, -1.0)
    lane8 = iota((8, 128), 0).astype(F32)
    for which in range(2):
        for jh in range(2):
            for o in range(OWN):
                sel.append(jnp.where(rkscr[which, o : o + 1, :] == lane8 + 8.0 * jh, 1.0, 0.0))
    sel = jnp.concatenate(sel, axis=0).astype(BF)
    ids = ord_ref[...]
    parts = jnp.concatenate(
        [(ids >> 7).astype(F32), (ids & 127).astype(F32), jnp.ones((32, 128), F32)], axis=0
    ).astype(BF)
    got = mm_nt(parts, sel)
    mine = iota((32, 1024), 0) == ((iota((32, 1024), 1) & 255) >> 3)
    high = jnp.sum(jnp.where(mine, got[0:32], 0.0), axis=0, keepdims=True)
    low = jnp.sum(jnp.where(mine, got[32:64], 0.0), axis=0, keepdims=True)
    valid = jnp.sum(jnp.where(mine, got[64:96], 0.0), axis=0, keepdims=True) > 0.5
    onehot = (iota((128, 1024), 0).astype(F32) == low).astype(F32).astype(BF)
    cols = cols_ref[...]
    rf_hi, rf_lo = two(rf_ref[...])
    w_hi, w_lo = two(w_ref[...])
    cf = cf_ref[...]
    parts = jnp.concatenate(
        [
            (cols >> 7).astype(F32).astype(BF),
            (cols & 127).astype(F32).astype(BF),
            (1.0 - cf).astype(BF),
            cf.astype(BF),
            rf_hi,
            rf_lo,
            w_hi,
            w_lo,
            rows_ref[...].astype(F32).astype(BF),
        ],
        axis=0,
    )
    got = mm(parts, onehot)
    mine = iota((32, 1024), 0).astype(F32) == high
    vals = [
        jnp.sum(jnp.where(mine, got[32 * i : 32 * i + 32], 0.0), axis=0, keepdims=True)
        for i in range(9)
    ]
    rhi = vals[4] + vals[5]
    weight = vals[6] + vals[7]
    grid_row = vals[8].astype(I32) - 4 * s
    second = iota((1, 1024), 1) >= LIST
    use = valid & ((~second) | (grid_row == -1))
    col = jnp.where(use, (vals[0] * 128.0 + vals[1]).astype(I32), -8)
    grid_row = jnp.where(use, grid_row, -8)
    return col, vals[2], vals[3], grid_row, rhi, weight, rows, slab


def reduce_matrix():
    a = iota((512, 128), 0)
    b = iota((512, 128), 1)
    return (b == ((a >> 8) * 64 + ((a & 255) >> 2))).astype(F32).astype(BF)


def fields_chunk(xv, first, count):
    return jnp.concatenate([xv[first + i] for i in range(count)], axis=1)


def spread_out(rows):
    flat = [r for group in rows for r in group]
    where = [i for i, group in enumerate(rows) for _ in group]
    stack = jnp.concatenate([r.astype(F32) for r in flat], axis=0)
    pad = 16 - len(flat)
    stack = jnp.concatenate([stack, jnp.zeros((pad, stack.shape[1]), F32)], axis=0).astype(BF)
    width = 128 * len(rows)
    a = iota((16, width), 0)
    group = jnp.full((16, width), -1, I32)
    for i, g in enumerate(where):
        group = jnp.where(a == i, g, group)
    pick = (group == (iota((16, width), 1) >> 7)).astype(F32).astype(BF)
    out = lax.dot_general(stack, pick, (((0,), (0,)), ((), ())), preferred_element_type=F32)
    return [out[:, 128 * i : 128 * i + 128] for i in range(len(rows))]


def weighted_source(full, weight, weights8, dst):
    a = iota((256, 128), 0)
    b = iota((256, 128), 1)
    high, low = two(full)
    for jh in range(2):
        cut = slice(jh * HALF, jh * HALF + HALF)
        pick = (b == (jh * 64 + (a >> 2))).astype(F32).astype(BF)
        value = mm_nt(pick, high) + mm_nt(pick, low)
        value = value * weight[:, cut]
        dst[:, cut] = times_rows(value, weights8[:, cut]).astype(BF)


def far_first():
    hops = lambda d: min(d, 4 - d)
    steps = [(y, x, c) for y in range(4) for x in range(4) for c in range(2)][1:]
    return sorted(steps, key=lambda d: -(hops(d[0]) + hops(d[1])))


STEPS = far_first()


def main_kernel(
    x_ref, ord_ref, line_ref, rows_ref, cols_ref, rf_ref, cf_ref, w_ref,
    ov, obs_ref, trace_ref,
    xv, reps, tabs, partial, src, rscr, rkscr,
    ordv, linev, rowsv, colsv, rfv, cfv, wv,
    mine_a, mine_b, full_a, next_box, prev_box, box, sums, ready, group, group_ready,
    x_sem, in_sem, halo_send, halo_recv, own_send, own_recv, sum_send, sum_recv,
    group_send, group_recv,
):
    s = lax.axis_index("slab")
    z = lax.axis_index("probe")
    small = [
        (ord_ref, ordv), (line_ref, linev), (rows_ref, rowsv), (cols_ref, colsv),
        (rf_ref, rfv), (cf_ref, cfv), (w_ref, wv),
    ]
    small = [pltpu.make_async_copy(a, b, in_sem.at[i]) for i, (a, b) in enumerate(small)]
    for copy in small:
        copy.start()
    barrier = pltpu.get_barrier_semaphore()

    place = (s // 8, lax.rem(s // 2, 4), lax.rem(s, 2))
    moved = [
        [lax.rem(at + d, length) for d in range(length)] for at, length in zip(place, (4, 4, 2))
    ]

    def other(step):
        y, x, core = (m[d] for m, d in zip(moved, step))
        return y * 8 + x * 2 + core

    slabs = [other(step) for step in STEPS]
    levels = [lax.rem(z + d, 4) for d in (2, 1, 3)]
    for t in slabs:
        pl.semaphore_signal(barrier, inc=1, device_id={"slab": t, "probe": z}, device_id_type=MESH)
    for t in levels:
        pl.semaphore_signal(barrier, inc=1, device_id={"slab": s, "probe": t}, device_id_type=MESH)
    flat = x_ref.reshape(256, 8192)
    for c in range(64):
        pltpu.make_async_copy(
            flat.at[:, pl.ds(c * 128, 128)], xv.at[c], x_sem
        ).start()
    for copy in small:
        copy.wait()
    col, clo, chi, grid_row, rhi, weight, rows, slab = prep(
        s, ordv, linev, rowsv, colsv, rfv, cfv, wv, rscr, rkscr
    )
    slabf = slab.astype(F32)
    slot_slab = jnp.sum(jnp.where(iota((32, 128), 0) == s, slabf, 0.0), axis=0, keepdims=True)
    square = jnp.broadcast_to(slot_slab, (128, 128))
    same = (square.T == square) & (iota((128, 128), 0) < iota((128, 128), 1))
    slot_rank = jnp.sum(jnp.where(same, 1.0, 0.0), axis=0, keepdims=True).astype(I32)
    slot_slab = slot_slab.astype(I32)
    weights8 = row_weights(grid_row, rhi)
    reduce = reduce_matrix()
    zero = jnp.zeros((), BF)

    def prepare(which):
        cut = slice(which * LIST, which * LIST + LIST)
        columns = col[:, cut]
        rhi_high, rhi_low = two(rhi[:, cut])
        block, lane, low, high, row, upper = spread_out(
            [
                [(columns >> 8).astype(F32).astype(BF)],
                [(columns & 255).astype(F32).astype(BF)],
                [clo[:, cut].astype(BF)],
                [chi[:, cut].astype(BF)],
                [grid_row[:, cut].astype(F32).astype(BF)],
                [rhi_high, rhi_low],
            ]
        )
        block, lane, low, high = [
            jnp.concatenate([x, x], axis=1) for x in (block, lane, low, high)
        ]
        here = iota((LIST, 256), 1).astype(F32)
        reps[which, 0] = block.astype(BF)
        reps[which, 1] = jnp.where(
            here == lane, low, jnp.where(here == lane + 1.0, high, 0.0)
        ).astype(BF)
        reps[which, 2] = jnp.where((lane == 255.0) & (here == 0.0), high, 0.0).astype(BF)
        quarter = (iota((LIST, 128), 1) & 3).astype(F32)
        factor = jnp.where(quarter == row, 1.0 - upper, jnp.where(quarter == row + 1.0, upper, 0.0))
        return factor

    def forward(which, factor, between, mine, done):
        def pieces(half):
            return [slice(jh * HALF + half * 128, jh * HALF + half * 128 + 128) for jh in range(2)]

        def build(i, half):
            for piece in pieces(half):
                for g in (piece.start, piece.start + 64):
                    rows = slice(g, g + 64)
                    at = reps[which, 0, rows]
                    inside = reps[which, 1, rows]
                    over = reps[which, 2, rows]
                    for j in range(4):
                        b = 4 * i + j
                        tabs[which, b, rows] = jnp.where(
                            at == b, inside, jnp.where(at == b - 1, over, zero)
                        )

        def product(i, half):
            tab = jnp.concatenate(
                [
                    jnp.concatenate([tabs[which, 4 * i + j, rows] for rows in pieces(half)], axis=0)
                    for j in range(4)
                ],
                axis=1,
            )
            return mm_nt(tab, fields_chunk(xv, 8 * i, 8))

        build(0, 0)
        build(4, 0)
        if which == 1:
            pltpu.make_async_copy(xv, xv, x_sem).wait()
        for half in range(2):
            total = [None, None]
            for i in range(4):
                if i < 3:
                    build(i + 1, half)
                    build(i + 5, half)
                elif half == 0:
                    build(0, 1)
                    build(4, 1)
                if half == 1 and i == 1 and between is not None:
                    between()
                for k in range(2):
                    part = product(i + 4 * k, half)
                    total[k] = part if i == 0 else total[k] + part
            both = []
            for jh, piece in enumerate(pieces(half)):
                scale = jnp.concatenate([factor[piece]] * 2, axis=1)
                rows = slice(jh * 128, jh * 128 + 128)
                both.append(total[0][rows] * scale + total[1][rows] * scale)
            high, low = two(jnp.concatenate(both, axis=1))
            mine[16 * half : 16 * half + 16] = (mm(high, reduce) + mm(low, reduce)).reshape(16, 8, 128)
            done(half)

    def send_half(mine, box_there, link, t, half):
        rows = pl.ds(16 * half, 16)
        return pltpu.make_async_remote_copy(
            mine.at[rows], box_there.at[rows], halo_send.at[link, half], halo_recv.at[link, half],
            {"slab": t, "probe": z}, MESH,
        )

    after = lax.rem(s + 1, OWN)
    before = lax.rem(s + OWN - 1, OWN)
    to_prev = [send_half(mine_b, next_box, 0, before, half) for half in range(2)]
    to_next = [send_half(mine_a, prev_box, 1, after, half) for half in range(2)]

    def done_b(half):
        if half == 0:
            pl.semaphore_wait(barrier, OWN + 2)
        to_prev[half].start()

    factor_b = prepare(1)
    factor_a = []
    forward(1, factor_b, lambda: factor_a.append(prepare(0)), mine_b, done_b)
    forward(0, factor_a[0], None, mine_a, lambda half: to_next[half].start())
    for copy in to_prev:
        copy.wait_recv()
    complete = mine_a[...] + next_box[...]
    full_a[...] = complete
    value_a = complete.reshape(HALF, 128)
    side = (iota((8, 128), 0) == (iota((8, 128), 1) >> 6)).astype(F32).astype(BF)
    high, low = two(value_a * value_a)
    squares = mm_nt(side, high) + mm_nt(side, low)
    total = jnp.sum(
        squares[0:1] * weight[:, 0:HALF] + squares[1:2] * weight[:, HALF:LIST]
    )
    ready[...] = jnp.full((1, 128), 1.0, F32) * total

    for t in levels:
        pltpu.make_async_remote_copy(
            ready, group.at[z], group_send, group_recv, {"slab": s, "probe": t}, MESH
        ).start()
    group[z] = ready[...]
    for t in slabs:
        pltpu.make_async_remote_copy(
            full_a.at[t], box.at[s], own_send, own_recv, {"slab": t, "probe": z}, MESH
        ).start()
    for copy in to_prev:
        copy.wait_send()
    box[s] = full_a[s]
    weighted_source(value_a, weight[:, 0:LIST], weights8[:, 0:LIST], src)

    for i in range(32):
        partial[i] = mm(src[...], tabs[0, i])
    view = group.at[pl.ds(0, 3)]
    pltpu.make_async_copy(view, view, group_recv).wait()
    group_ready[...] = jnp.sum(group[...], axis=0)
    for t in slabs:
        pltpu.make_async_remote_copy(
            group_ready, sums.at[s], sum_send, sum_recv, {"slab": t, "probe": z}, MESH
        ).start()
    sums[s] = group_ready[...]
    for copy in to_next:
        copy.wait_recv()
    value_b = (mine_b[...] + prev_box[...]).reshape(HALF, 128)
    weighted_source(value_b, weight[:, LIST:], weights8[:, LIST:], src)

    for i in range(32):
        ov[i] = (partial[i] + mm(src[...], tabs[1, i])).astype(BF)
    view = box.at[pl.ds(0, OWN - 1)]
    pltpu.make_async_copy(view, view, own_recv).wait()
    full = box[...].reshape(HALF, 128).T
    sub = iota((HALF, 128), 0)
    pick = ((sub >> 3) == slot_slab) & ((sub & 7) == (slot_rank & 7))
    pick = jnp.where(pick, 1.0, 0.0).astype(BF)
    high, low = two(full)
    got = mm(high, pick) + mm(low, pick)
    obs_ref[...] = jnp.where(slot_rank < 8, got[0:64], got[64:128])
    view = sums.at[pl.ds(0, OWN - 1)]
    pltpu.make_async_copy(view, view, sum_recv).wait()
    trace_ref[...] = jnp.sum(sums[...], axis=0) * (1.0 / 1048576.0)
    for copy in to_next:
        copy.wait_send()
    pltpu.make_async_copy(view, view, sum_send).wait()
    view = group.at[pl.ds(0, 3)]
    pltpu.make_async_copy(view, view, group_send).wait()
    view = box.at[pl.ds(0, OWN - 1)]
    pltpu.make_async_copy(view, view, own_send).wait()


def store_kernel(ov, obs_in, trace_in, out_ref, obs_ref, trace_ref, sem):
    flat = out_ref.reshape(256, 8192)
    for c in range(64):
        half = ov.at[c // 2, :, pl.ds((c % 2) * 128, 128)]
        pltpu.make_async_copy(half, flat.at[:, pl.ds(c * 128, 128)], sem).start()
    obs_ref[...] = obs_in[...]
    trace_ref[0, 0] = trace_in[0, 0]
    pltpu.make_async_copy(ov, ov, sem).wait()


def run_main(fields, rows, cols, rf, cf, w, order):
    vm = pl.BlockSpec(memory_space=pltpu.VMEM)
    anywhere = pl.BlockSpec(memory_space=pl.ANY)
    dma = pltpu.SemaphoreType.DMA
    sq = lambda x: x.reshape(32, 128)
    block = pltpu.VMEM((OWN, 8, 128), F32)
    return pl.pallas_call(
        main_kernel,
        out_shape=(
            pltpu.VMEM((32, 256, 256), BF),
            pltpu.VMEM((64, 128), F32),
            pltpu.VMEM((1, 128), F32),
        ),
        in_specs=[anywhere] * 8,
        out_specs=(vm, vm, vm),
        scratch_shapes=[
            pltpu.VMEM((64, 256, 128), BF),
            pltpu.VMEM((2, 3, LIST, 256), BF),
            pltpu.VMEM((2, 32, LIST, 256), BF),
            pltpu.VMEM((32, 256, 256), F32),
            pltpu.VMEM((256, LIST), BF),
            pltpu.VMEM((32, 128), F32),
            pltpu.VMEM((2, 32, 128), F32),
            pltpu.VMEM((32, 128), I32),
            pltpu.VMEM((1, 4096), I32),
            pltpu.VMEM((32, 128), I32),
            pltpu.VMEM((32, 128), I32),
            pltpu.VMEM((32, 128), F32),
            pltpu.VMEM((32, 128), F32),
            pltpu.VMEM((32, 128), F32),
            block, block, block, block, block, block,
            pltpu.VMEM((OWN, 1, 128), F32),
            pltpu.VMEM((1, 128), F32),
            pltpu.VMEM((4, 1, 128), F32),
            pltpu.VMEM((1, 128), F32),
            dma, dma((7,)), dma((2, 2)), dma((2, 2)), dma, dma, dma, dma, dma, dma,
        ],
        compiler_params=pltpu.CompilerParams(
            collective_id=0, has_side_effects=True, vmem_limit_bytes=60000000
        ),
        name="main",
    )(fields, sq(order), order.reshape(1, 4096), sq(rows), sq(cols), sq(rf), sq(cf), sq(w))


def run_store(ov, obs, trace):
    vm = pl.BlockSpec(memory_space=pltpu.VMEM)
    anywhere = pl.BlockSpec(memory_space=pl.ANY)
    return pl.pallas_call(
        store_kernel,
        out_shape=(
            jax.ShapeDtypeStruct((64, 4, 8192), BF),
            jax.ShapeDtypeStruct((64, 128), F32),
            jax.ShapeDtypeStruct((1, 1), F32),
        ),
        in_specs=[vm] * 3,
        out_specs=(anywhere, vm, pl.BlockSpec(memory_space=pltpu.SMEM)),
        scratch_shapes=[pltpu.SemaphoreType.DMA],
        compiler_params=pltpu.CompilerParams(vmem_limit_bytes=8 * 1024 * 1024),
        name="store",
    )(ov, obs, trace)


def body(fields, rows, cols, rf, cf, w, order):
    ov, obs, trace = run_main(fields, rows, cols, rf, cf, w, order)
    adjoint, observed, trace = run_store(ov, obs, trace)
    return adjoint, observed, trace.reshape(())


def solution(mesh):
    return jax.shard_map(
        body,
        mesh=mesh,
        in_specs=(P("probe", "slab", None), P(), P(), P(), P(), P(), P()),
        out_specs=(P("probe", "slab", None), P("probe", "slab"), P()),
        check_vma=False,
    )
```

```python
import jax
import jax.numpy as jnp
from jax import lax
from jax.experimental import pallas as pl
from jax.experimental.pallas import tpu as pltpu
from jax.sharding import PartitionSpec as P

F32 = jnp.float32
BF = jnp.bfloat16
I32 = jnp.int32
MESH = pl.DeviceIdType.MESH

OWN = 32
RANK = 16
LIST = OWN * RANK
HALF = LIST // 2


def iota(shape, dim):
    return lax.broadcasted_iota(I32, shape, dim)


def mm(a, b):
    return lax.dot_general(a, b, (((1,), (0,)), ((), ())), preferred_element_type=F32)


def mm_nt(a, b):
    return lax.dot_general(a, b, (((1,), (1,)), ((), ())), preferred_element_type=F32)


def two(x):
    high = x.astype(BF)
    return high, (x - high.astype(F32)).astype(BF)


def mm_two(a, x):
    high, low = two(x)
    return mm(a, high) + mm(a, low)


def row_weights(row, rhi):
    sub = iota((8, row.shape[1]), 0) % 4
    return jnp.where(sub == row, 1.0 - rhi, 0.0) + jnp.where(sub == row + 1, rhi, 0.0)


def times_rows(x, weights8):
    rows, slots = x.shape
    return (x.reshape(rows // 8, 8, slots) * weights8[None]).reshape(rows, slots)


def prep(s, ord_ref, line_ref, rows_ref, cols_ref, rf_ref, cf_ref, w_ref, rscr, rkscr):
    line = line_ref[...]
    onehot = (iota((128, 4096), 0) == (line & 127)).astype(F32).astype(BF)
    found = mm(rows_ref[...].astype(F32).astype(BF), onehot)
    picked = jnp.where(iota((32, 4096), 0) == (line >> 7), found, 0.0)
    slot_rows = jnp.sum(picked, axis=0, keepdims=True)
    for o in range(OWN):
        rscr[o : o + 1, :] = slot_rows[:, o * 128 : o * 128 + 128]
    rows = rscr[...].astype(I32)
    slab = rows >> 2
    upper = (iota((128, 128), 0) < iota((128, 128), 1)).astype(F32).astype(BF)
    sel = []
    for which in range(2):
        mask = slab == s - which
        maskf = jnp.where(mask, 1.0, 0.0)
        rank = mm(maskf.astype(BF), upper)
        rkscr[which] = jnp.where(mask, rank, -1.0)
    lane8 = iota((8, 128), 0).astype(F32)
    for which in range(2):
        for jh in range(2):
            for o in range(OWN):
                sel.append(jnp.where(rkscr[which, o : o + 1, :] == lane8 + 8.0 * jh, 1.0, 0.0))
    sel = jnp.concatenate(sel, axis=0).astype(BF)
    ids = ord_ref[...]
    parts = jnp.concatenate(
        [(ids >> 7).astype(F32), (ids & 127).astype(F32), jnp.ones((32, 128), F32)], axis=0
    ).astype(BF)
    got = mm_nt(parts, sel)
    mine = iota((32, 1024), 0) == ((iota((32, 1024), 1) & 255) >> 3)
    high = jnp.sum(jnp.where(mine, got[0:32], 0.0), axis=0, keepdims=True)
    low = jnp.sum(jnp.where(mine, got[32:64], 0.0), axis=0, keepdims=True)
    valid = jnp.sum(jnp.where(mine, got[64:96], 0.0), axis=0, keepdims=True) > 0.5
    onehot = (iota((128, 1024), 0).astype(F32) == low).astype(F32).astype(BF)
    cols = cols_ref[...]
    rf_hi, rf_lo = two(rf_ref[...])
    w_hi, w_lo = two(w_ref[...])
    cf = cf_ref[...]
    parts = jnp.concatenate(
        [
            (cols >> 7).astype(F32).astype(BF),
            (cols & 127).astype(F32).astype(BF),
            (1.0 - cf).astype(BF),
            cf.astype(BF),
            rf_hi,
            rf_lo,
            w_hi,
            w_lo,
            rows_ref[...].astype(F32).astype(BF),
        ],
        axis=0,
    )
    got = mm(parts, onehot)
    mine = iota((32, 1024), 0).astype(F32) == high
    vals = [
        jnp.sum(jnp.where(mine, got[32 * i : 32 * i + 32], 0.0), axis=0, keepdims=True)
        for i in range(9)
    ]
    rhi = vals[4] + vals[5]
    weight = vals[6] + vals[7]
    grid_row = vals[8].astype(I32) - 4 * s
    second = iota((1, 1024), 1) >= LIST
    use = valid & ((~second) | (grid_row == -1))
    col = jnp.where(use, (vals[0] * 128.0 + vals[1]).astype(I32), -8)
    grid_row = jnp.where(use, grid_row, -8)
    return col, vals[2], vals[3], grid_row, rhi, weight, rows, slab


def reduce_matrix():
    a = iota((512, 128), 0)
    b = iota((512, 128), 1)
    return (b == ((a >> 8) * 64 + ((a & 255) >> 2))).astype(F32).astype(BF)


def fields_chunk(xv, first, count):
    return jnp.concatenate([xv[first + i] for i in range(count)], axis=1)


def spread_out(rows):
    flat = [r for group in rows for r in group]
    where = [i for i, group in enumerate(rows) for _ in group]
    stack = jnp.concatenate([r.astype(F32) for r in flat], axis=0)
    pad = 16 - len(flat)
    stack = jnp.concatenate([stack, jnp.zeros((pad, stack.shape[1]), F32)], axis=0).astype(BF)
    width = 128 * len(rows)
    a = iota((16, width), 0)
    group = jnp.full((16, width), -1, I32)
    for i, g in enumerate(where):
        group = jnp.where(a == i, g, group)
    pick = (group == (iota((16, width), 1) >> 7)).astype(F32).astype(BF)
    out = lax.dot_general(stack, pick, (((0,), (0,)), ((), ())), preferred_element_type=F32)
    return [out[:, 128 * i : 128 * i + 128] for i in range(len(rows))]


def weighted_source(full, weight, weights8, dst):
    a = iota((256, 128), 0)
    b = iota((256, 128), 1)
    high, low = two(full)
    for jh in range(2):
        cut = slice(jh * HALF, jh * HALF + HALF)
        pick = (b == (jh * 64 + (a >> 2))).astype(F32).astype(BF)
        value = mm_nt(pick, high) + mm_nt(pick, low)
        value = value * weight[:, cut]
        dst[:, cut] = times_rows(value, weights8[:, cut]).astype(BF)


def far_first():
    hops = lambda d: min(d, 4 - d)
    steps = [
        (y, x, c, z) for y in range(4) for x in range(4) for c in range(2) for z in range(4)
    ][1:]
    return sorted(steps, key=lambda d: -(hops(d[0]) + hops(d[1]) + hops(d[3])))


STEPS = far_first()
FAR = 71


def main_kernel(
    x_ref, ord_ref, line_ref, rows_ref, cols_ref, rf_ref, cf_ref, w_ref,
    ov, obs_ref, trace_ref,
    xv, reps, tabs, partial, src, rscr, rkscr,
    ordv, linev, rowsv, colsv, rfv, cfv, wv,
    mine_a, mine_b, full_a, next_box, prev_box, box, sums, ready,
    x_sem, in_sem, halo_send, halo_recv, own_send, own_recv, sum_send, sum_recv, plane,
):
    s = lax.axis_index("slab")
    z = lax.axis_index("probe")
    small = [
        (ord_ref, ordv), (line_ref, linev), (rows_ref, rowsv), (cols_ref, colsv),
        (rf_ref, rfv), (cf_ref, cfv), (w_ref, wv),
    ]
    small = [pltpu.make_async_copy(a, b, in_sem.at[i]) for i, (a, b) in enumerate(small)]
    for copy in small:
        copy.start(priority=1)
    flat = x_ref.reshape(256, 8192)
    for c in range(64):
        pltpu.make_async_copy(
            flat.at[:, pl.ds(c * 128, 128)], xv.at[c], x_sem.at[c // 32]
        ).start()
    barrier = pltpu.get_barrier_semaphore()

    place = (s // 8, lax.rem(s // 2, 4), lax.rem(s, 2), z)
    moved = [
        [lax.rem(at + d, length) for d in range(length)]
        for at, length in zip(place, (4, 4, 2, 4))
    ]

    def other(step):
        y, x, core, level = (m[d] for m, d in zip(moved, step))
        return {"slab": y * 8 + x * 2 + core, "probe": level}

    near = [step for step in STEPS if step[3] == 0 or step[:3] == (0, 0, 0)]
    for step in near:
        pl.semaphore_signal(barrier, inc=1, device_id=other(step), device_id_type=MESH)
    for copy in small:
        copy.wait()
    col, clo, chi, grid_row, rhi, weight, rows, slab = prep(
        s, ordv, linev, rowsv, colsv, rfv, cfv, wv, rscr, rkscr
    )
    slabf = slab.astype(F32)
    slot_slab = jnp.sum(jnp.where(iota((32, 128), 0) == s, slabf, 0.0), axis=0, keepdims=True)
    square = jnp.broadcast_to(slot_slab, (128, 128))
    same = (square.T == square) & (iota((128, 128), 0) < iota((128, 128), 1))
    slot_rank = jnp.sum(jnp.where(same, 1.0, 0.0), axis=0, keepdims=True).astype(I32)
    slot_slab = slot_slab.astype(I32)
    weights8 = row_weights(grid_row, rhi)
    reduce = reduce_matrix()
    zero = jnp.zeros((), BF)

    def prepare(which):
        cut = slice(which * LIST, which * LIST + LIST)
        columns = col[:, cut]
        rhi_high, rhi_low = two(rhi[:, cut])
        block, lane, low, high, row, upper = spread_out(
            [
                [(columns >> 8).astype(F32).astype(BF)],
                [(columns & 255).astype(F32).astype(BF)],
                [clo[:, cut].astype(BF)],
                [chi[:, cut].astype(BF)],
                [grid_row[:, cut].astype(F32).astype(BF)],
                [rhi_high, rhi_low],
            ]
        )
        block, lane, low, high = [
            jnp.concatenate([x, x], axis=1) for x in (block, lane, low, high)
        ]
        here = iota((LIST, 256), 1).astype(F32)
        reps[which, 0] = block.astype(BF)
        reps[which, 1] = jnp.where(
            here == lane, low, jnp.where(here == lane + 1.0, high, 0.0)
        ).astype(BF)
        reps[which, 2] = jnp.where((lane == 255.0) & (here == 0.0), high, 0.0).astype(BF)
        quarter = (iota((LIST, 128), 1) & 3).astype(F32)
        factor = jnp.where(quarter == row, 1.0 - upper, jnp.where(quarter == row + 1.0, upper, 0.0))
        return factor

    def forward(which, factor, between):
        def build(i):
            for g in range(0, LIST, 64):
                rows = slice(g, g + 64)
                at = reps[which, 0, rows]
                inside = reps[which, 1, rows]
                over = reps[which, 2, rows]
                for j in range(4):
                    b = 4 * i + j
                    tabs[which, b, rows] = jnp.where(
                        at == b, inside, jnp.where(at == b - 1, over, zero)
                    )

        def product(i, half):
            rows = slice(half * HALF, half * HALF + HALF)
            tab = jnp.concatenate([tabs[which, 4 * i + j, rows] for j in range(4)], axis=1)
            return mm_nt(tab, fields_chunk(xv, 8 * i, 8))

        def arrive(i):
            view = xv.at[pl.ds(32 * i, 32)]
            pltpu.make_async_copy(view, view, x_sem.at[i]).wait()

        build(0)
        total = [None, None]
        for i in range(8):
            if which == 1 and i % 4 == 0:
                arrive(i // 4)
            if i < 7:
                build(i + 1)
            if i == 4 and between is not None:
                between()
            for half in range(2):
                part = product(i, half)
                total[half] = part if i == 0 else total[half] + part
        both = []
        for half in range(2):
            scale = factor[half * HALF : half * HALF + HALF]
            both.append(total[half] * jnp.concatenate([scale, scale], axis=1))
        both = jnp.concatenate(both, axis=1)
        high, low = two(both)
        return (mm(high, reduce) + mm(low, reduce)).reshape(OWN, 8, 128)

    factor_b = prepare(1)
    factor_a = []
    mine_b[...] = forward(1, factor_b, lambda: factor_a.append(prepare(0)))
    pl.semaphore_wait(barrier, OWN + 2)
    for d in range(1, 4):
        pl.semaphore_signal(
            plane, inc=1, device_id={"slab": s, "probe": lax.rem(z + d, 4)}, device_id_type=MESH
        )
    to_prev = pltpu.make_async_remote_copy(
        mine_b, next_box, halo_send.at[0], halo_recv.at[0],
        {"slab": lax.rem(s + OWN - 1, OWN), "probe": z}, MESH,
    )
    to_prev.start()
    mine_a[...] = forward(0, factor_a[0], None)
    to_next = pltpu.make_async_remote_copy(
        mine_a, prev_box, halo_send.at[1], halo_recv.at[1],
        {"slab": lax.rem(s + 1, OWN), "probe": z}, MESH,
    )
    to_next.start()
    to_prev.wait_recv()
    complete = mine_a[...] + next_box[...]
    full_a[...] = complete
    value_a = complete.reshape(HALF, 128)
    side = (iota((8, 128), 0) == (iota((8, 128), 1) >> 6)).astype(F32).astype(BF)
    high, low = two(value_a * value_a)
    squares = mm_nt(side, high) + mm_nt(side, low)
    total = jnp.sum(
        squares[0:1] * weight[:, 0:HALF] + squares[1:2] * weight[:, HALF:LIST]
    )
    ready[...] = jnp.full((1, 128), 1.0, F32) * total

    me = s * 4 + z
    pl.semaphore_wait(plane, 3)

    def send_sum(step):
        pltpu.make_async_remote_copy(
            ready, sums.at[me], sum_send, sum_recv, other(step), MESH
        ).start()

    for step in STEPS[:FAR]:
        send_sum(step)
    sums[me] = ready[...]
    for step in near:
        if step[3] == 0:
            there = other(step)
            pltpu.make_async_remote_copy(
                full_a.at[there["slab"]], box.at[s], own_send, own_recv, there, MESH
            ).start()
    box[s] = full_a[s]
    weighted_source(value_a, weight[:, 0:LIST], weights8[:, 0:LIST], src)
    to_prev.wait_send()

    for i in range(32):
        partial[i] = mm(src[...], tabs[0, i])
        for step in STEPS[FAR + 2 * i : FAR + 2 * i + 2]:
            send_sum(step)
    to_next.wait_recv()
    value_b = (mine_b[...] + prev_box[...]).reshape(HALF, 128)
    weighted_source(value_b, weight[:, LIST:], weights8[:, LIST:], src)

    for i in range(32):
        ov[i] = (partial[i] + mm(src[...], tabs[1, i])).astype(BF)
    view = box.at[pl.ds(0, OWN - 1)]
    pltpu.make_async_copy(view, view, own_recv).wait()
    full = box[...].reshape(HALF, 128).T
    sub = iota((HALF, 128), 0)
    pick = ((sub >> 3) == slot_slab) & ((sub & 7) == (slot_rank & 7))
    pick = jnp.where(pick, 1.0, 0.0).astype(BF)
    high, low = two(full)
    got = mm(high, pick) + mm(low, pick)
    obs_ref[...] = jnp.where(slot_rank < 8, got[0:64], got[64:128])
    view = sums.at[pl.ds(0, 127)]
    pltpu.make_async_copy(view, view, sum_recv).wait()
    trace_ref[...] = jnp.sum(sums[...], axis=0) * (1.0 / 1048576.0)
    to_next.wait_send()
    pltpu.make_async_copy(view, view, sum_send).wait()
    view = box.at[pl.ds(0, OWN - 1)]
    pltpu.make_async_copy(view, view, own_send).wait()


def store_kernel(ov, obs_in, trace_in, out_ref, obs_ref, trace_ref, sem):
    flat = out_ref.reshape(256, 8192)
    for c in range(64):
        half = ov.at[c // 2, :, pl.ds((c % 2) * 128, 128)]
        pltpu.make_async_copy(half, flat.at[:, pl.ds(c * 128, 128)], sem).start()
    obs_ref[...] = obs_in[...]
    trace_ref[0, 0] = trace_in[0, 0]
    pltpu.make_async_copy(ov, ov, sem).wait()


def run_main(fields, rows, cols, rf, cf, w, order):
    vm = pl.BlockSpec(memory_space=pltpu.VMEM)
    anywhere = pl.BlockSpec(memory_space=pl.ANY)
    dma = pltpu.SemaphoreType.DMA
    sq = lambda x: x.reshape(32, 128)
    block = pltpu.VMEM((OWN, 8, 128), F32)
    return pl.pallas_call(
        main_kernel,
        out_shape=(
            pltpu.VMEM((32, 256, 256), BF),
            pltpu.VMEM((64, 128), F32),
            pltpu.VMEM((1, 128), F32),
        ),
        in_specs=[anywhere] * 8,
        out_specs=(vm, vm, vm),
        scratch_shapes=[
            pltpu.VMEM((64, 256, 128), BF),
            pltpu.VMEM((2, 3, LIST, 256), BF),
            pltpu.VMEM((2, 32, LIST, 256), BF),
            pltpu.VMEM((32, 256, 256), F32),
            pltpu.VMEM((256, LIST), BF),
            pltpu.VMEM((32, 128), F32),
            pltpu.VMEM((2, 32, 128), F32),
            pltpu.VMEM((32, 128), I32),
            pltpu.VMEM((1, 4096), I32),
            pltpu.VMEM((32, 128), I32),
            pltpu.VMEM((32, 128), I32),
            pltpu.VMEM((32, 128), F32),
            pltpu.VMEM((32, 128), F32),
            pltpu.VMEM((32, 128), F32),
            block, block, block, block, block, block,
            pltpu.VMEM((128, 1, 128), F32),
            pltpu.VMEM((1, 128), F32),
            dma((2,)), dma((7,)), dma((2,)), dma((2,)), dma, dma, dma, dma, pltpu.SemaphoreType.REGULAR,
        ],
        compiler_params=pltpu.CompilerParams(
            collective_id=0, has_side_effects=True, vmem_limit_bytes=60000000
        ),
        name="main",
    )(fields, sq(order), order.reshape(1, 4096), sq(rows), sq(cols), sq(rf), sq(cf), sq(w))


def run_store(ov, obs, trace):
    vm = pl.BlockSpec(memory_space=pltpu.VMEM)
    anywhere = pl.BlockSpec(memory_space=pl.ANY)
    return pl.pallas_call(
        store_kernel,
        out_shape=(
            jax.ShapeDtypeStruct((64, 4, 8192), BF),
            jax.ShapeDtypeStruct((64, 128), F32),
            jax.ShapeDtypeStruct((1, 1), F32),
        ),
        in_specs=[vm] * 3,
        out_specs=(anywhere, vm, pl.BlockSpec(memory_space=pltpu.SMEM)),
        scratch_shapes=[pltpu.SemaphoreType.DMA],
        compiler_params=pltpu.CompilerParams(vmem_limit_bytes=8 * 1024 * 1024),
        name="store",
    )(ov, obs, trace)


def body(fields, rows, cols, rf, cf, w, order):
    ov, obs, trace = run_main(fields, rows, cols, rf, cf, w, order)
    adjoint, observed, trace = run_store(ov, obs, trace)
    return adjoint, observed, trace.reshape(())


def solution(mesh):
    return jax.shard_map(
        body,
        mesh=mesh,
        in_specs=(P("probe", "slab", None), P(), P(), P(), P(), P(), P()),
        out_specs=(P("probe", "slab", None), P("probe", "slab"), P()),
        check_vma=False,
    )
```

```python
import jax
import jax.numpy as jnp
from jax import lax
from jax.experimental import pallas as pl
from jax.experimental.pallas import tpu as pltpu
from jax.sharding import PartitionSpec as P

F32 = jnp.float32
BF = jnp.bfloat16
I32 = jnp.int32
MESH = pl.DeviceIdType.MESH

OWN = 32
RANK = 16
LIST = OWN * RANK
HALF = LIST // 2


def iota(shape, dim):
    return lax.broadcasted_iota(I32, shape, dim)


def mm(a, b):
    return lax.dot_general(a, b, (((1,), (0,)), ((), ())), preferred_element_type=F32)


def mm_nt(a, b):
    return lax.dot_general(a, b, (((1,), (1,)), ((), ())), preferred_element_type=F32)


def two(x):
    high = x.astype(BF)
    return high, (x - high.astype(F32)).astype(BF)


def mm_two(a, x):
    high, low = two(x)
    return mm(a, high) + mm(a, low)


def row_weights(row, rhi):
    sub = iota((8, row.shape[1]), 0) % 4
    return jnp.where(sub == row, 1.0 - rhi, 0.0) + jnp.where(sub == row + 1, rhi, 0.0)


def times_rows(x, weights8):
    rows, slots = x.shape
    return (x.reshape(rows // 8, 8, slots) * weights8[None]).reshape(rows, slots)


def prep(s, ord_ref, line_ref, rows_ref, cols_ref, rf_ref, cf_ref, w_ref, rscr, rkscr):
    line = line_ref[...]
    onehot = (iota((128, 4096), 0) == (line & 127)).astype(F32).astype(BF)
    found = mm(rows_ref[...].astype(F32).astype(BF), onehot)
    picked = jnp.where(iota((32, 4096), 0) == (line >> 7), found, 0.0)
    slot_rows = jnp.sum(picked, axis=0, keepdims=True)
    for o in range(OWN):
        rscr[o : o + 1, :] = slot_rows[:, o * 128 : o * 128 + 128]
    rows = rscr[...].astype(I32)
    slab = rows >> 2
    upper = (iota((128, 128), 0) < iota((128, 128), 1)).astype(F32).astype(BF)
    sel = []
    for which in range(2):
        mask = slab == s - which
        maskf = jnp.where(mask, 1.0, 0.0)
        rank = mm(maskf.astype(BF), upper)
        rkscr[which] = jnp.where(mask, rank, -1.0)
    lane8 = iota((8, 128), 0).astype(F32)
    for which in range(2):
        for jh in range(2):
            for o in range(OWN):
                sel.append(jnp.where(rkscr[which, o : o + 1, :] == lane8 + 8.0 * jh, 1.0, 0.0))
    sel = jnp.concatenate(sel, axis=0).astype(BF)
    ids = ord_ref[...]
    parts = jnp.concatenate(
        [(ids >> 7).astype(F32), (ids & 127).astype(F32), jnp.ones((32, 128), F32)], axis=0
    ).astype(BF)
    got = mm_nt(parts, sel)
    mine = iota((32, 1024), 0) == ((iota((32, 1024), 1) & 255) >> 3)
    high = jnp.sum(jnp.where(mine, got[0:32], 0.0), axis=0, keepdims=True)
    low = jnp.sum(jnp.where(mine, got[32:64], 0.0), axis=0, keepdims=True)
    valid = jnp.sum(jnp.where(mine, got[64:96], 0.0), axis=0, keepdims=True) > 0.5
    onehot = (iota((128, 1024), 0).astype(F32) == low).astype(F32).astype(BF)
    cols = cols_ref[...]
    rf_hi, rf_lo = two(rf_ref[...])
    w_hi, w_lo = two(w_ref[...])
    cf = cf_ref[...]
    parts = jnp.concatenate(
        [
            (cols >> 7).astype(F32).astype(BF),
            (cols & 127).astype(F32).astype(BF),
            (1.0 - cf).astype(BF),
            cf.astype(BF),
            rf_hi,
            rf_lo,
            w_hi,
            w_lo,
            rows_ref[...].astype(F32).astype(BF),
        ],
        axis=0,
    )
    got = mm(parts, onehot)
    mine = iota((32, 1024), 0).astype(F32) == high
    vals = [
        jnp.sum(jnp.where(mine, got[32 * i : 32 * i + 32], 0.0), axis=0, keepdims=True)
        for i in range(9)
    ]
    rhi = vals[4] + vals[5]
    weight = vals[6] + vals[7]
    grid_row = vals[8].astype(I32) - 4 * s
    second = iota((1, 1024), 1) >= LIST
    use = valid & ((~second) | (grid_row == -1))
    col = jnp.where(use, (vals[0] * 128.0 + vals[1]).astype(I32), -8)
    grid_row = jnp.where(use, grid_row, -8)
    return col, vals[2], vals[3], grid_row, rhi, weight, rows, slab


def reduce_matrix():
    a = iota((512, 128), 0)
    b = iota((512, 128), 1)
    return (b == ((a >> 8) * 64 + ((a & 255) >> 2))).astype(F32).astype(BF)


def fields_chunk(xv, first, count):
    return jnp.concatenate([xv[first + i] for i in range(count)], axis=1)


def spread_out(rows):
    flat = [r for group in rows for r in group]
    where = [i for i, group in enumerate(rows) for _ in group]
    stack = jnp.concatenate([r.astype(F32) for r in flat], axis=0)
    pad = 16 - len(flat)
    stack = jnp.concatenate([stack, jnp.zeros((pad, stack.shape[1]), F32)], axis=0).astype(BF)
    width = 128 * len(rows)
    a = iota((16, width), 0)
    group = jnp.full((16, width), -1, I32)
    for i, g in enumerate(where):
        group = jnp.where(a == i, g, group)
    pick = (group == (iota((16, width), 1) >> 7)).astype(F32).astype(BF)
    out = lax.dot_general(stack, pick, (((0,), (0,)), ((), ())), preferred_element_type=F32)
    return [out[:, 128 * i : 128 * i + 128] for i in range(len(rows))]


def weighted_source(full, weight, weights8, dst):
    a = iota((256, 128), 0)
    b = iota((256, 128), 1)
    high, low = two(full)
    for jh in range(2):
        cut = slice(jh * HALF, jh * HALF + HALF)
        pick = (b == (jh * 64 + (a >> 2))).astype(F32).astype(BF)
        value = mm_nt(pick, high) + mm_nt(pick, low)
        value = value * weight[:, cut]
        dst[:, cut] = times_rows(value, weights8[:, cut]).astype(BF)


def far_first():
    hops = lambda d: min(d, 4 - d)
    steps = [
        (y, x, c, z) for y in range(4) for x in range(4) for c in range(2) for z in range(4)
    ][1:]
    return sorted(steps, key=lambda d: -(hops(d[0]) + hops(d[1]) + hops(d[3])))


STEPS = far_first()


def main_kernel(
    x_ref, ord_ref, line_ref, rows_ref, cols_ref, rf_ref, cf_ref, w_ref,
    ov, obs_ref, trace_ref,
    xv, reps, tabs, partial, src, rscr, rkscr,
    ordv, linev, rowsv, colsv, rfv, cfv, wv,
    mine_a, mine_b, full_a, next_box, prev_box, box, sums, ready,
    x_sem, in_sem, halo_send, halo_recv, own_send, own_recv, sum_send, sum_recv, plane,
):
    s = lax.axis_index("slab")
    z = lax.axis_index("probe")
    small = [
        (ord_ref, ordv), (line_ref, linev), (rows_ref, rowsv), (cols_ref, colsv),
        (rf_ref, rfv), (cf_ref, cfv), (w_ref, wv),
    ]
    small = [pltpu.make_async_copy(a, b, in_sem.at[i]) for i, (a, b) in enumerate(small)]
    for copy in small:
        copy.start()
    barrier = pltpu.get_barrier_semaphore()

    place = (s // 8, lax.rem(s // 2, 4), lax.rem(s, 2), z)
    moved = [
        [lax.rem(at + d, length) for d in range(length)]
        for at, length in zip(place, (4, 4, 2, 4))
    ]

    def other(step):
        y, x, core, level = (m[d] for m, d in zip(moved, step))
        return {"slab": y * 8 + x * 2 + core, "probe": level}

    near = [step for step in STEPS if step[3] == 0 or step[:3] == (0, 0, 0)]
    for step in near:
        pl.semaphore_signal(barrier, inc=1, device_id=other(step), device_id_type=MESH)
    flat = x_ref.reshape(256, 8192)
    for c in range(64):
        pltpu.make_async_copy(
            flat.at[:, pl.ds(c * 128, 128)], xv.at[c], x_sem.at[c // 32]
        ).start()
    for copy in small:
        copy.wait()
    col, clo, chi, grid_row, rhi, weight, rows, slab = prep(
        s, ordv, linev, rowsv, colsv, rfv, cfv, wv, rscr, rkscr
    )
    slabf = slab.astype(F32)
    slot_slab = jnp.sum(jnp.where(iota((32, 128), 0) == s, slabf, 0.0), axis=0, keepdims=True)
    square = jnp.broadcast_to(slot_slab, (128, 128))
    same = (square.T == square) & (iota((128, 128), 0) < iota((128, 128), 1))
    slot_rank = jnp.sum(jnp.where(same, 1.0, 0.0), axis=0, keepdims=True).astype(I32)
    slot_slab = slot_slab.astype(I32)
    weights8 = row_weights(grid_row, rhi)
    reduce = reduce_matrix()
    zero = jnp.zeros((), BF)

    def prepare(which):
        cut = slice(which * LIST, which * LIST + LIST)
        columns = col[:, cut]
        rhi_high, rhi_low = two(rhi[:, cut])
        block, lane, low, high, row, upper = spread_out(
            [
                [(columns >> 8).astype(F32).astype(BF)],
                [(columns & 255).astype(F32).astype(BF)],
                [clo[:, cut].astype(BF)],
                [chi[:, cut].astype(BF)],
                [grid_row[:, cut].astype(F32).astype(BF)],
                [rhi_high, rhi_low],
            ]
        )
        block, lane, low, high = [
            jnp.concatenate([x, x], axis=1) for x in (block, lane, low, high)
        ]
        here = iota((LIST, 256), 1).astype(F32)
        reps[which, 0] = block.astype(BF)
        reps[which, 1] = jnp.where(
            here == lane, low, jnp.where(here == lane + 1.0, high, 0.0)
        ).astype(BF)
        reps[which, 2] = jnp.where((lane == 255.0) & (here == 0.0), high, 0.0).astype(BF)
        quarter = (iota((LIST, 128), 1) & 3).astype(F32)
        factor = jnp.where(quarter == row, 1.0 - upper, jnp.where(quarter == row + 1.0, upper, 0.0))
        return factor

    def forward(which, factor, between):
        def build(i):
            for g in range(0, LIST, 64):
                rows = slice(g, g + 64)
                at = reps[which, 0, rows]
                inside = reps[which, 1, rows]
                over = reps[which, 2, rows]
                for j in range(4):
                    b = 4 * i + j
                    tabs[which, b, rows] = jnp.where(
                        at == b, inside, jnp.where(at == b - 1, over, zero)
                    )

        def product(i, half):
            rows = slice(half * HALF, half * HALF + HALF)
            tab = jnp.concatenate([tabs[which, 4 * i + j, rows] for j in range(4)], axis=1)
            return mm_nt(tab, fields_chunk(xv, 8 * i, 8))

        def arrive(i):
            view = xv.at[pl.ds(32 * i, 32)]
            pltpu.make_async_copy(view, view, x_sem.at[i]).wait()

        build(0)
        total = [None, None]
        for i in range(8):
            if which == 1 and i % 4 == 0:
                arrive(i // 4)
            if i < 7:
                build(i + 1)
            if i == 4 and between is not None:
                between()
            for half in range(2):
                part = product(i, half)
                total[half] = part if i == 0 else total[half] + part
        both = []
        for half in range(2):
            scale = factor[half * HALF : half * HALF + HALF]
            both.append(total[half] * jnp.concatenate([scale, scale], axis=1))
        both = jnp.concatenate(both, axis=1)
        high, low = two(both)
        return (mm(high, reduce) + mm(low, reduce)).reshape(OWN, 8, 128)

    factor_b = prepare(1)
    factor_a = []
    mine_b[...] = forward(1, factor_b, lambda: factor_a.append(prepare(0)))
    pl.semaphore_wait(barrier, OWN + 2)
    for d in range(1, 4):
        pl.semaphore_signal(
            plane, inc=1, device_id={"slab": s, "probe": lax.rem(z + d, 4)}, device_id_type=MESH
        )
    to_prev = pltpu.make_async_remote_copy(
        mine_b, next_box, halo_send.at[0], halo_recv.at[0],
        {"slab": lax.rem(s + OWN - 1, OWN), "probe": z}, MESH,
    )
    to_prev.start()
    mine_a[...] = forward(0, factor_a[0], None)
    to_next = pltpu.make_async_remote_copy(
        mine_a, prev_box, halo_send.at[1], halo_recv.at[1],
        {"slab": lax.rem(s + 1, OWN), "probe": z}, MESH,
    )
    to_next.start()
    to_prev.wait_recv()
    complete = mine_a[...] + next_box[...]
    full_a[...] = complete
    value_a = complete.reshape(HALF, 128)
    side = (iota((8, 128), 0) == (iota((8, 128), 1) >> 6)).astype(F32).astype(BF)
    high, low = two(value_a * value_a)
    squares = mm_nt(side, high) + mm_nt(side, low)
    total = jnp.sum(
        squares[0:1] * weight[:, 0:HALF] + squares[1:2] * weight[:, HALF:LIST]
    )
    ready[...] = jnp.full((1, 128), 1.0, F32) * total

    me = s * 4 + z
    pl.semaphore_wait(plane, 3)

    def send_sum(step):
        pltpu.make_async_remote_copy(
            ready, sums.at[me], sum_send, sum_recv, other(step), MESH
        ).start()

    for step in STEPS:
        send_sum(step)
    sums[me] = ready[...]
    for step in near:
        if step[3] == 0:
            there = other(step)
            pltpu.make_async_remote_copy(
                full_a.at[there["slab"]], box.at[s], own_send, own_recv, there, MESH
            ).start()
    box[s] = full_a[s]
    weighted_source(value_a, weight[:, 0:LIST], weights8[:, 0:LIST], src)
    to_prev.wait_send()

    for i in range(32):
        partial[i] = mm(src[...], tabs[0, i])
    to_next.wait_recv()
    value_b = (mine_b[...] + prev_box[...]).reshape(HALF, 128)
    weighted_source(value_b, weight[:, LIST:], weights8[:, LIST:], src)

    for i in range(32):
        ov[i] = (partial[i] + mm(src[...], tabs[1, i])).astype(BF)
    view = box.at[pl.ds(0, OWN - 1)]
    pltpu.make_async_copy(view, view, own_recv).wait()
    full = box[...].reshape(HALF, 128).T
    sub = iota((HALF, 128), 0)
    pick = ((sub >> 3) == slot_slab) & ((sub & 7) == (slot_rank & 7))
    pick = jnp.where(pick, 1.0, 0.0).astype(BF)
    high, low = two(full)
    got = mm(high, pick) + mm(low, pick)
    obs_ref[...] = jnp.where(slot_rank < 8, got[0:64], got[64:128])
    view = sums.at[pl.ds(0, 127)]
    pltpu.make_async_copy(view, view, sum_recv).wait()
    trace_ref[...] = jnp.sum(sums[...], axis=0) * (1.0 / 1048576.0)
    to_next.wait_send()
    pltpu.make_async_copy(view, view, sum_send).wait()
    view = box.at[pl.ds(0, OWN - 1)]
    pltpu.make_async_copy(view, view, own_send).wait()


def store_kernel(ov, obs_in, trace_in, out_ref, obs_ref, trace_ref, sem):
    flat = out_ref.reshape(256, 8192)
    for c in range(64):
        half = ov.at[c // 2, :, pl.ds((c % 2) * 128, 128)]
        pltpu.make_async_copy(half, flat.at[:, pl.ds(c * 128, 128)], sem).start()
    obs_ref[...] = obs_in[...]
    trace_ref[0, 0] = trace_in[0, 0]
    pltpu.make_async_copy(ov, ov, sem).wait()


def run_main(fields, rows, cols, rf, cf, w, order):
    vm = pl.BlockSpec(memory_space=pltpu.VMEM)
    anywhere = pl.BlockSpec(memory_space=pl.ANY)
    dma = pltpu.SemaphoreType.DMA
    sq = lambda x: x.reshape(32, 128)
    block = pltpu.VMEM((OWN, 8, 128), F32)
    return pl.pallas_call(
        main_kernel,
        out_shape=(
            pltpu.VMEM((32, 256, 256), BF),
            pltpu.VMEM((64, 128), F32),
            pltpu.VMEM((1, 128), F32),
        ),
        in_specs=[anywhere] * 8,
        out_specs=(vm, vm, vm),
        scratch_shapes=[
            pltpu.VMEM((64, 256, 128), BF),
            pltpu.VMEM((2, 3, LIST, 256), BF),
            pltpu.VMEM((2, 32, LIST, 256), BF),
            pltpu.VMEM((32, 256, 256), F32),
            pltpu.VMEM((256, LIST), BF),
            pltpu.VMEM((32, 128), F32),
            pltpu.VMEM((2, 32, 128), F32),
            pltpu.VMEM((32, 128), I32),
            pltpu.VMEM((1, 4096), I32),
            pltpu.VMEM((32, 128), I32),
            pltpu.VMEM((32, 128), I32),
            pltpu.VMEM((32, 128), F32),
            pltpu.VMEM((32, 128), F32),
            pltpu.VMEM((32, 128), F32),
            block, block, block, block, block, block,
            pltpu.VMEM((128, 1, 128), F32),
            pltpu.VMEM((1, 128), F32),
            dma((2,)), dma((7,)), dma((2,)), dma((2,)), dma, dma, dma, dma, pltpu.SemaphoreType.REGULAR,
        ],
        compiler_params=pltpu.CompilerParams(
            collective_id=0, has_side_effects=True, vmem_limit_bytes=60000000
        ),
        name="main",
    )(fields, sq(order), order.reshape(1, 4096), sq(rows), sq(cols), sq(rf), sq(cf), sq(w))


def run_store(ov, obs, trace):
    vm = pl.BlockSpec(memory_space=pltpu.VMEM)
    anywhere = pl.BlockSpec(memory_space=pl.ANY)
    return pl.pallas_call(
        store_kernel,
        out_shape=(
            jax.ShapeDtypeStruct((64, 4, 8192), BF),
            jax.ShapeDtypeStruct((64, 128), F32),
            jax.ShapeDtypeStruct((1, 1), F32),
        ),
        in_specs=[vm] * 3,
        out_specs=(anywhere, vm, pl.BlockSpec(memory_space=pltpu.SMEM)),
        scratch_shapes=[pltpu.SemaphoreType.DMA],
        compiler_params=pltpu.CompilerParams(vmem_limit_bytes=8 * 1024 * 1024),
        name="store",
    )(ov, obs, trace)


def body(fields, rows, cols, rf, cf, w, order):
    ov, obs, trace = run_main(fields, rows, cols, rf, cf, w, order)
    adjoint, observed, trace = run_store(ov, obs, trace)
    return adjoint, observed, trace.reshape(())


def solution(mesh):
    return jax.shard_map(
        body,
        mesh=mesh,
        in_specs=(P("probe", "slab", None), P(), P(), P(), P(), P(), P()),
        out_specs=(P("probe", "slab", None), P("probe", "slab"), P()),
        check_vma=False,
    )
```

```python
import jax
import jax.numpy as jnp
from jax import lax
from jax.experimental import pallas as pl
from jax.experimental.pallas import tpu as pltpu
from jax.sharding import PartitionSpec as P

F32 = jnp.float32
BF = jnp.bfloat16
I32 = jnp.int32
MESH = pl.DeviceIdType.MESH

OWN = 32
RANK = 16
LIST = OWN * RANK
HALF = LIST // 2


def iota(shape, dim):
    return lax.broadcasted_iota(I32, shape, dim)


def mm(a, b):
    return lax.dot_general(a, b, (((1,), (0,)), ((), ())), preferred_element_type=F32)


def mm_nt(a, b):
    return lax.dot_general(a, b, (((1,), (1,)), ((), ())), preferred_element_type=F32)


def two(x):
    high = x.astype(BF)
    return high, (x - high.astype(F32)).astype(BF)


def mm_two(a, x):
    high, low = two(x)
    return mm(a, high) + mm(a, low)


def row_weights(row, rhi):
    sub = iota((8, row.shape[1]), 0) % 4
    return jnp.where(sub == row, 1.0 - rhi, 0.0) + jnp.where(sub == row + 1, rhi, 0.0)


def times_rows(x, weights8):
    rows, slots = x.shape
    return (x.reshape(rows // 8, 8, slots) * weights8[None]).reshape(rows, slots)


def prep(s, ord_ref, line_ref, rows_ref, cols_ref, rf_ref, cf_ref, w_ref, rscr, rkscr):
    line = line_ref[...]
    onehot = (iota((128, 4096), 0) == (line & 127)).astype(F32).astype(BF)
    found = mm(rows_ref[...].astype(F32).astype(BF), onehot)
    picked = jnp.where(iota((32, 4096), 0) == (line >> 7), found, 0.0)
    slot_rows = jnp.sum(picked, axis=0, keepdims=True)
    for o in range(OWN):
        rscr[o : o + 1, :] = slot_rows[:, o * 128 : o * 128 + 128]
    rows = rscr[...].astype(I32)
    slab = rows >> 2
    upper = (iota((128, 128), 0) < iota((128, 128), 1)).astype(F32).astype(BF)
    sel = []
    for which in range(2):
        mask = slab == s - which
        maskf = jnp.where(mask, 1.0, 0.0)
        rank = mm(maskf.astype(BF), upper)
        rkscr[which] = jnp.where(mask, rank, -1.0)
    lane8 = iota((8, 128), 0).astype(F32)
    for which in range(2):
        for jh in range(2):
            for o in range(OWN):
                sel.append(jnp.where(rkscr[which, o : o + 1, :] == lane8 + 8.0 * jh, 1.0, 0.0))
    sel = jnp.concatenate(sel, axis=0).astype(BF)
    ids = ord_ref[...]
    parts = jnp.concatenate(
        [(ids >> 7).astype(F32), (ids & 127).astype(F32), jnp.ones((32, 128), F32)], axis=0
    ).astype(BF)
    got = mm_nt(parts, sel)
    mine = iota((32, 1024), 0) == ((iota((32, 1024), 1) & 255) >> 3)
    high = jnp.sum(jnp.where(mine, got[0:32], 0.0), axis=0, keepdims=True)
    low = jnp.sum(jnp.where(mine, got[32:64], 0.0), axis=0, keepdims=True)
    valid = jnp.sum(jnp.where(mine, got[64:96], 0.0), axis=0, keepdims=True) > 0.5
    onehot = (iota((128, 1024), 0).astype(F32) == low).astype(F32).astype(BF)
    cols = cols_ref[...]
    rf_hi, rf_lo = two(rf_ref[...])
    w_hi, w_lo = two(w_ref[...])
    cf = cf_ref[...]
    parts = jnp.concatenate(
        [
            (cols >> 7).astype(F32).astype(BF),
            (cols & 127).astype(F32).astype(BF),
            (1.0 - cf).astype(BF),
            cf.astype(BF),
            rf_hi,
            rf_lo,
            w_hi,
            w_lo,
            rows_ref[...].astype(F32).astype(BF),
        ],
        axis=0,
    )
    got = mm(parts, onehot)
    mine = iota((32, 1024), 0).astype(F32) == high
    vals = [
        jnp.sum(jnp.where(mine, got[32 * i : 32 * i + 32], 0.0), axis=0, keepdims=True)
        for i in range(9)
    ]
    rhi = vals[4] + vals[5]
    weight = vals[6] + vals[7]
    grid_row = vals[8].astype(I32) - 4 * s
    second = iota((1, 1024), 1) >= LIST
    use = valid & ((~second) | (grid_row == -1))
    col = jnp.where(use, (vals[0] * 128.0 + vals[1]).astype(I32), -8)
    grid_row = jnp.where(use, grid_row, -8)
    return col, vals[2], vals[3], grid_row, rhi, weight, rows, slab


def reduce_matrix():
    a = iota((512, 128), 0)
    b = iota((512, 128), 1)
    return (b == ((a >> 8) * 64 + ((a & 255) >> 2))).astype(F32).astype(BF)


def fields_chunk(xv, first, count):
    return jnp.concatenate([xv[first + i] for i in range(count)], axis=1)


def spread_out(rows):
    flat = [r for group in rows for r in group]
    where = [i for i, group in enumerate(rows) for _ in group]
    stack = jnp.concatenate([r.astype(F32) for r in flat], axis=0)
    pad = 16 - len(flat)
    stack = jnp.concatenate([stack, jnp.zeros((pad, stack.shape[1]), F32)], axis=0).astype(BF)
    width = 128 * len(rows)
    a = iota((16, width), 0)
    group = jnp.full((16, width), -1, I32)
    for i, g in enumerate(where):
        group = jnp.where(a == i, g, group)
    pick = (group == (iota((16, width), 1) >> 7)).astype(F32).astype(BF)
    out = lax.dot_general(stack, pick, (((0,), (0,)), ((), ())), preferred_element_type=F32)
    return [out[:, 128 * i : 128 * i + 128] for i in range(len(rows))]


def weighted_source(full, weight, weights8, dst):
    a = iota((256, 128), 0)
    b = iota((256, 128), 1)
    high, low = two(full)
    for jh in range(2):
        cut = slice(jh * HALF, jh * HALF + HALF)
        pick = (b == (jh * 64 + (a >> 2))).astype(F32).astype(BF)
        value = mm_nt(pick, high) + mm_nt(pick, low)
        value = value * weight[:, cut]
        dst[:, cut] = times_rows(value, weights8[:, cut]).astype(BF)


def far_first():
    hops = lambda d: min(d, 4 - d)
    steps = [
        (y, x, c, z) for y in range(4) for x in range(4) for c in range(2) for z in range(4)
    ][1:]
    return sorted(steps, key=lambda d: -(hops(d[0]) + hops(d[1]) + hops(d[3])))


STEPS = far_first()


def main_kernel(
    x_ref, ord_ref, line_ref, rows_ref, cols_ref, rf_ref, cf_ref, w_ref,
    ov, obs_ref, trace_ref,
    xv, reps, tabs, partial, src, rscr, rkscr,
    ordv, linev, rowsv, colsv, rfv, cfv, wv,
    mine_a, mine_b, full_a, next_box, prev_box, box, sums, ready,
    x_sem, in_sem, halo_send, halo_recv, own_send, own_recv, sum_send, sum_recv, plane,
):
    s = lax.axis_index("slab")
    z = lax.axis_index("probe")
    small = [
        (ord_ref, ordv), (line_ref, linev), (rows_ref, rowsv), (cols_ref, colsv),
        (rf_ref, rfv), (cf_ref, cfv), (w_ref, wv),
    ]
    small = [pltpu.make_async_copy(a, b, in_sem.at[i]) for i, (a, b) in enumerate(small)]
    for copy in small:
        copy.start()
    barrier = pltpu.get_barrier_semaphore()

    place = (s // 8, lax.rem(s // 2, 4), lax.rem(s, 2), z)
    moved = [
        [lax.rem(at + d, length) for d in range(length)]
        for at, length in zip(place, (4, 4, 2, 4))
    ]

    def other(step):
        y, x, core, level = (m[d] for m, d in zip(moved, step))
        return {"slab": y * 8 + x * 2 + core, "probe": level}

    near = [step for step in STEPS if step[3] == 0 or step[:3] == (0, 0, 0)]
    for step in near:
        pl.semaphore_signal(barrier, inc=1, device_id=other(step), device_id_type=MESH)
    flat = x_ref.reshape(256, 8192)
    for c in range(64):
        pltpu.make_async_copy(
            flat.at[:, pl.ds(c * 128, 128)], xv.at[c], x_sem.at[c // 32]
        ).start()
    for copy in small:
        copy.wait()
    col, clo, chi, grid_row, rhi, weight, rows, slab = prep(
        s, ordv, linev, rowsv, colsv, rfv, cfv, wv, rscr, rkscr
    )
    slabf = slab.astype(F32)
    slot_slab = jnp.sum(jnp.where(iota((32, 128), 0) == s, slabf, 0.0), axis=0, keepdims=True)
    square = jnp.broadcast_to(slot_slab, (128, 128))
    same = (square.T == square) & (iota((128, 128), 0) < iota((128, 128), 1))
    slot_rank = jnp.sum(jnp.where(same, 1.0, 0.0), axis=0, keepdims=True).astype(I32)
    slot_slab = slot_slab.astype(I32)
    weights8 = row_weights(grid_row, rhi)
    reduce = reduce_matrix()
    zero = jnp.zeros((), BF)

    def prepare(which):
        cut = slice(which * LIST, which * LIST + LIST)
        columns = col[:, cut]
        rhi_high, rhi_low = two(rhi[:, cut])
        block, lane, low, high, row, upper = spread_out(
            [
                [(columns >> 8).astype(F32).astype(BF)],
                [(columns & 255).astype(F32).astype(BF)],
                [clo[:, cut].astype(BF)],
                [chi[:, cut].astype(BF)],
                [grid_row[:, cut].astype(F32).astype(BF)],
                [rhi_high, rhi_low],
            ]
        )
        block, lane, low, high = [
            jnp.concatenate([x, x], axis=1) for x in (block, lane, low, high)
        ]
        here = iota((LIST, 256), 1).astype(F32)
        reps[which, 0] = block.astype(BF)
        reps[which, 1] = jnp.where(
            here == lane, low, jnp.where(here == lane + 1.0, high, 0.0)
        ).astype(BF)
        reps[which, 2] = jnp.where((lane == 255.0) & (here == 0.0), high, 0.0).astype(BF)
        quarter = (iota((LIST, 128), 1) & 3).astype(F32)
        factor = jnp.where(quarter == row, 1.0 - upper, jnp.where(quarter == row + 1.0, upper, 0.0))
        return factor

    def forward(which, factor, between):
        def build(i):
            for g in range(0, LIST, 64):
                rows = slice(g, g + 64)
                at = reps[which, 0, rows]
                inside = reps[which, 1, rows]
                over = reps[which, 2, rows]
                for j in range(4):
                    b = 4 * i + j
                    tabs[which, b, rows] = jnp.where(
                        at == b, inside, jnp.where(at == b - 1, over, zero)
                    )

        def product(i, half):
            rows = slice(half * HALF, half * HALF + HALF)
            tab = jnp.concatenate([tabs[which, 4 * i + j, rows] for j in range(4)], axis=1)
            return mm_nt(tab, fields_chunk(xv, 8 * i, 8))

        def arrive(i):
            view = xv.at[pl.ds(32 * i, 32)]
            pltpu.make_async_copy(view, view, x_sem.at[i]).wait()

        build(0)
        total = [None, None]
        for i in range(8):
            if which == 1 and i % 4 == 0:
                arrive(i // 4)
            if i < 7:
                build(i + 1)
            if i == 4 and between is not None:
                between()
            for half in range(2):
                part = product(i, half)
                total[half] = part if i == 0 else total[half] + part
        both = []
        for half in range(2):
            scale = factor[half * HALF : half * HALF + HALF]
            both.append(total[half] * jnp.concatenate([scale, scale], axis=1))
        both = jnp.concatenate(both, axis=1)
        high, low = two(both)
        return (mm(high, reduce) + mm(low, reduce)).reshape(OWN, 8, 128)

    factor_b = prepare(1)
    factor_a = []
    mine_b[...] = forward(1, factor_b, lambda: factor_a.append(prepare(0)))
    pl.semaphore_wait(barrier, OWN + 2)
    for d in range(1, 4):
        pl.semaphore_signal(
            plane, inc=1, device_id={"slab": s, "probe": lax.rem(z + d, 4)}, device_id_type=MESH
        )
    to_prev = pltpu.make_async_remote_copy(
        mine_b, next_box, halo_send.at[0], halo_recv.at[0],
        {"slab": lax.rem(s + OWN - 1, OWN), "probe": z}, MESH,
    )
    to_prev.start()
    mine_a[...] = forward(0, factor_a[0], None)
    to_next = pltpu.make_async_remote_copy(
        mine_a, prev_box, halo_send.at[1], halo_recv.at[1],
        {"slab": lax.rem(s + 1, OWN), "probe": z}, MESH,
    )
    to_next.start()
    to_prev.wait_recv()
    complete = mine_a[...] + next_box[...]
    full_a[...] = complete
    value_a = complete.reshape(HALF, 128)
    side = (iota((8, 128), 0) == (iota((8, 128), 1) >> 6)).astype(F32).astype(BF)
    high, low = two(value_a * value_a)
    squares = mm_nt(side, high) + mm_nt(side, low)
    total = jnp.sum(
        squares[0:1] * weight[:, 0:HALF] + squares[1:2] * weight[:, HALF:LIST]
    )
    ready[...] = jnp.full((1, 128), 1.0, F32) * total

    me = s * 4 + z
    pl.semaphore_wait(plane, 3)

    def send_sum(step):
        pltpu.make_async_remote_copy(
            ready, sums.at[me], sum_send, sum_recv, other(step), MESH
        ).start()

    for step in STEPS:
        send_sum(step)
    sums[me] = ready[...]
    for step in near:
        if step[3] == 0:
            there = other(step)
            pltpu.make_async_remote_copy(
                full_a.at[there["slab"]], box.at[s], own_send, own_recv, there, MESH
            ).start()
    box[s] = full_a[s]
    weighted_source(value_a, weight[:, 0:LIST], weights8[:, 0:LIST], src)
    to_prev.wait_send()

    for i in range(32):
        partial[i] = mm(src[...], tabs[0, i])
    to_next.wait_recv()
    value_b = (mine_b[...] + prev_box[...]).reshape(HALF, 128)
    weighted_source(value_b, weight[:, LIST:], weights8[:, LIST:], src)

    for i in range(32):
        got = (partial[i] + mm(src[...], tabs[1, i])).astype(BF)
        ov[:, :, 256 * i : 256 * i + 256] = got.reshape(64, 4, 256)
    view = box.at[pl.ds(0, OWN - 1)]
    pltpu.make_async_copy(view, view, own_recv).wait()
    full = box[...].reshape(HALF, 128).T
    sub = iota((HALF, 128), 0)
    pick = ((sub >> 3) == slot_slab) & ((sub & 7) == (slot_rank & 7))
    pick = jnp.where(pick, 1.0, 0.0).astype(BF)
    high, low = two(full)
    got = mm(high, pick) + mm(low, pick)
    obs_ref[...] = jnp.where(slot_rank < 8, got[0:64], got[64:128])
    view = sums.at[pl.ds(0, 127)]
    pltpu.make_async_copy(view, view, sum_recv).wait()
    trace_ref[...] = jnp.sum(sums[...], axis=0) * (1.0 / 1048576.0)
    to_next.wait_send()
    pltpu.make_async_copy(view, view, sum_send).wait()
    view = box.at[pl.ds(0, OWN - 1)]
    pltpu.make_async_copy(view, view, own_send).wait()


def store_kernel(ov, obs_in, trace_in, out_ref, obs_ref, trace_ref, sem):
    for c in range(8):
        rows = pl.ds(8 * c, 8)
        pltpu.make_async_copy(ov.at[rows], out_ref.at[rows], sem).start()
    obs_ref[...] = obs_in[...]
    trace_ref[0, 0] = trace_in[0, 0]
    pltpu.make_async_copy(ov, ov, sem).wait()


def run_main(fields, rows, cols, rf, cf, w, order):
    vm = pl.BlockSpec(memory_space=pltpu.VMEM)
    anywhere = pl.BlockSpec(memory_space=pl.ANY)
    dma = pltpu.SemaphoreType.DMA
    sq = lambda x: x.reshape(32, 128)
    block = pltpu.VMEM((OWN, 8, 128), F32)
    return pl.pallas_call(
        main_kernel,
        out_shape=(
            pltpu.VMEM((64, 4, 8192), BF),
            pltpu.VMEM((64, 128), F32),
            pltpu.VMEM((1, 128), F32),
        ),
        in_specs=[anywhere] * 8,
        out_specs=(vm, vm, vm),
        scratch_shapes=[
            pltpu.VMEM((64, 256, 128), BF),
            pltpu.VMEM((2, 3, LIST, 256), BF),
            pltpu.VMEM((2, 32, LIST, 256), BF),
            pltpu.VMEM((32, 256, 256), F32),
            pltpu.VMEM((256, LIST), BF),
            pltpu.VMEM((32, 128), F32),
            pltpu.VMEM((2, 32, 128), F32),
            pltpu.VMEM((32, 128), I32),
            pltpu.VMEM((1, 4096), I32),
            pltpu.VMEM((32, 128), I32),
            pltpu.VMEM((32, 128), I32),
            pltpu.VMEM((32, 128), F32),
            pltpu.VMEM((32, 128), F32),
            pltpu.VMEM((32, 128), F32),
            block, block, block, block, block, block,
            pltpu.VMEM((128, 1, 128), F32),
            pltpu.VMEM((1, 128), F32),
            dma((2,)), dma((7,)), dma((2,)), dma((2,)), dma, dma, dma, dma, pltpu.SemaphoreType.REGULAR,
        ],
        compiler_params=pltpu.CompilerParams(
            collective_id=0, has_side_effects=True, vmem_limit_bytes=60000000
        ),
        name="main",
    )(fields, sq(order), order.reshape(1, 4096), sq(rows), sq(cols), sq(rf), sq(cf), sq(w))


def run_store(ov, obs, trace):
    vm = pl.BlockSpec(memory_space=pltpu.VMEM)
    anywhere = pl.BlockSpec(memory_space=pl.ANY)
    return pl.pallas_call(
        store_kernel,
        out_shape=(
            jax.ShapeDtypeStruct((64, 4, 8192), BF),
            jax.ShapeDtypeStruct((64, 128), F32),
            jax.ShapeDtypeStruct((1, 1), F32),
        ),
        in_specs=[vm] * 3,
        out_specs=(anywhere, vm, pl.BlockSpec(memory_space=pltpu.SMEM)),
        scratch_shapes=[pltpu.SemaphoreType.DMA],
        compiler_params=pltpu.CompilerParams(vmem_limit_bytes=8 * 1024 * 1024),
        name="store",
    )(ov, obs, trace)


def body(fields, rows, cols, rf, cf, w, order):
    ov, obs, trace = run_main(fields, rows, cols, rf, cf, w, order)
    adjoint, observed, trace = run_store(ov, obs, trace)
    return adjoint, observed, trace.reshape(())


def solution(mesh):
    return jax.shard_map(
        body,
        mesh=mesh,
        in_specs=(P("probe", "slab", None), P(), P(), P(), P(), P(), P()),
        out_specs=(P("probe", "slab", None), P("probe", "slab"), P()),
        check_vma=False,
    )
```

```python
import jax
import jax.numpy as jnp
from jax import lax
from jax.experimental import pallas as pl
from jax.experimental.pallas import tpu as pltpu
from jax.sharding import PartitionSpec as P

F32 = jnp.float32
BF = jnp.bfloat16
I32 = jnp.int32
MESH = pl.DeviceIdType.MESH

OWN = 32
RANK = 16
LIST = OWN * RANK
HALF = LIST // 2


def iota(shape, dim):
    return lax.broadcasted_iota(I32, shape, dim)


def mm(a, b):
    return lax.dot_general(a, b, (((1,), (0,)), ((), ())), preferred_element_type=F32)


def mm_nt(a, b):
    return lax.dot_general(a, b, (((1,), (1,)), ((), ())), preferred_element_type=F32)


def two(x):
    high = x.astype(BF)
    return high, (x - high.astype(F32)).astype(BF)


def mm_two(a, x):
    high, low = two(x)
    return mm(a, high) + mm(a, low)


def row_weights(row, rhi):
    sub = iota((8, row.shape[1]), 0) % 4
    return jnp.where(sub == row, 1.0 - rhi, 0.0) + jnp.where(sub == row + 1, rhi, 0.0)


def times_rows(x, weights8):
    rows, slots = x.shape
    return (x.reshape(rows // 8, 8, slots) * weights8[None]).reshape(rows, slots)


def prep(s, ord_ref, line_ref, rows_ref, cols_ref, rf_ref, cf_ref, w_ref, rscr, rkscr):
    line = line_ref[...]
    onehot = (iota((128, 4096), 0) == (line & 127)).astype(F32).astype(BF)
    found = mm(rows_ref[...].astype(F32).astype(BF), onehot)
    picked = jnp.where(iota((32, 4096), 0) == (line >> 7), found, 0.0)
    slot_rows = jnp.sum(picked, axis=0, keepdims=True)
    for o in range(OWN):
        rscr[o : o + 1, :] = slot_rows[:, o * 128 : o * 128 + 128]
    rows = rscr[...].astype(I32)
    slab = rows >> 2
    upper = (iota((128, 128), 0) < iota((128, 128), 1)).astype(F32).astype(BF)
    sel = []
    for which in range(2):
        mask = slab == s - which
        maskf = jnp.where(mask, 1.0, 0.0)
        rank = mm(maskf.astype(BF), upper)
        rkscr[which] = jnp.where(mask, rank, -1.0)
    lane8 = iota((8, 128), 0).astype(F32)
    for which in range(2):
        for jh in range(2):
            for o in range(OWN):
                sel.append(jnp.where(rkscr[which, o : o + 1, :] == lane8 + 8.0 * jh, 1.0, 0.0))
    sel = jnp.concatenate(sel, axis=0).astype(BF)
    ids = ord_ref[...]
    parts = jnp.concatenate(
        [(ids >> 7).astype(F32), (ids & 127).astype(F32), jnp.ones((32, 128), F32)], axis=0
    ).astype(BF)
    got = mm_nt(parts, sel)
    mine = iota((32, 1024), 0) == ((iota((32, 1024), 1) & 255) >> 3)
    high = jnp.sum(jnp.where(mine, got[0:32], 0.0), axis=0, keepdims=True)
    low = jnp.sum(jnp.where(mine, got[32:64], 0.0), axis=0, keepdims=True)
    valid = jnp.sum(jnp.where(mine, got[64:96], 0.0), axis=0, keepdims=True) > 0.5
    onehot = (iota((128, 1024), 0).astype(F32) == low).astype(F32).astype(BF)
    cols = cols_ref[...]
    rf_hi, rf_lo = two(rf_ref[...])
    w_hi, w_lo = two(w_ref[...])
    cf = cf_ref[...]
    parts = jnp.concatenate(
        [
            (cols >> 7).astype(F32).astype(BF),
            (cols & 127).astype(F32).astype(BF),
            (1.0 - cf).astype(BF),
            cf.astype(BF),
            rf_hi,
            rf_lo,
            w_hi,
            w_lo,
            rows_ref[...].astype(F32).astype(BF),
        ],
        axis=0,
    )
    got = mm(parts, onehot)
    mine = iota((32, 1024), 0).astype(F32) == high
    vals = [
        jnp.sum(jnp.where(mine, got[32 * i : 32 * i + 32], 0.0), axis=0, keepdims=True)
        for i in range(9)
    ]
    rhi = vals[4] + vals[5]
    weight = vals[6] + vals[7]
    grid_row = vals[8].astype(I32) - 4 * s
    second = iota((1, 1024), 1) >= LIST
    use = valid & ((~second) | (grid_row == -1))
    col = jnp.where(use, (vals[0] * 128.0 + vals[1]).astype(I32), -8)
    grid_row = jnp.where(use, grid_row, -8)
    return col, vals[2], vals[3], grid_row, rhi, weight, rows, slab


def reduce_matrix():
    a = iota((512, 128), 0)
    b = iota((512, 128), 1)
    return (b == ((a >> 8) * 64 + ((a & 255) >> 2))).astype(F32).astype(BF)


def fields_chunk(xv, first, count):
    return jnp.concatenate([xv[first + i] for i in range(count)], axis=1)


def spread_out(rows):
    flat = [r for group in rows for r in group]
    where = [i for i, group in enumerate(rows) for _ in group]
    stack = jnp.concatenate([r.astype(F32) for r in flat], axis=0)
    pad = 16 - len(flat)
    stack = jnp.concatenate([stack, jnp.zeros((pad, stack.shape[1]), F32)], axis=0).astype(BF)
    width = 128 * len(rows)
    a = iota((16, width), 0)
    group = jnp.full((16, width), -1, I32)
    for i, g in enumerate(where):
        group = jnp.where(a == i, g, group)
    pick = (group == (iota((16, width), 1) >> 7)).astype(F32).astype(BF)
    out = lax.dot_general(stack, pick, (((0,), (0,)), ((), ())), preferred_element_type=F32)
    return [out[:, 128 * i : 128 * i + 128] for i in range(len(rows))]


def weighted_source(full, weight, weights8, dst):
    a = iota((256, 128), 0)
    b = iota((256, 128), 1)
    high, low = two(full)
    for jh in range(2):
        cut = slice(jh * HALF, jh * HALF + HALF)
        pick = (b == (jh * 64 + (a >> 2))).astype(F32).astype(BF)
        value = mm_nt(pick, high) + mm_nt(pick, low)
        value = value * weight[:, cut]
        dst[:, cut] = times_rows(value, weights8[:, cut]).astype(BF)


def far_first():
    hops = lambda d: min(d, 4 - d)
    steps = [
        (y, x, c, z) for y in range(4) for x in range(4) for c in range(2) for z in range(4)
    ][1:]
    return sorted(steps, key=lambda d: -(hops(d[0]) + hops(d[1]) + hops(d[3])))


STEPS = far_first()


def main_kernel(
    x_ref, ord_ref, line_ref, rows_ref, cols_ref, rf_ref, cf_ref, w_ref,
    ov, box_ref, info_ref, trace_ref,
    xv, reps, tabs, partial, src, rscr, rkscr,
    ordv, linev, rowsv, colsv, rfv, cfv, wv,
    mine_a, mine_b, full_a, next_box, prev_box, box, sums, ready,
    x_sem, in_sem, halo_send, halo_recv, own_send, own_recv, sum_send, sum_recv, plane,
):
    s = lax.axis_index("slab")
    z = lax.axis_index("probe")
    small = [
        (ord_ref, ordv), (line_ref, linev), (rows_ref, rowsv), (cols_ref, colsv),
        (rf_ref, rfv), (cf_ref, cfv), (w_ref, wv),
    ]
    small = [pltpu.make_async_copy(a, b, in_sem.at[i]) for i, (a, b) in enumerate(small)]
    for copy in small:
        copy.start()
    barrier = pltpu.get_barrier_semaphore()

    place = (s // 8, lax.rem(s // 2, 4), lax.rem(s, 2), z)
    moved = [
        [lax.rem(at + d, length) for d in range(length)]
        for at, length in zip(place, (4, 4, 2, 4))
    ]

    def other(step):
        y, x, core, level = (m[d] for m, d in zip(moved, step))
        return {"slab": y * 8 + x * 2 + core, "probe": level}

    near = [step for step in STEPS if step[3] == 0 or step[:3] == (0, 0, 0)]
    for step in near:
        pl.semaphore_signal(barrier, inc=1, device_id=other(step), device_id_type=MESH)
    flat = x_ref.reshape(256, 8192)
    for c in range(64):
        pltpu.make_async_copy(
            flat.at[:, pl.ds(c * 128, 128)], xv.at[c], x_sem.at[c // 32]
        ).start()
    for copy in small:
        copy.wait()
    col, clo, chi, grid_row, rhi, weight, rows, slab = prep(
        s, ordv, linev, rowsv, colsv, rfv, cfv, wv, rscr, rkscr
    )
    weights8 = row_weights(grid_row, rhi)
    reduce = reduce_matrix()
    zero = jnp.zeros((), BF)

    def prepare(which):
        cut = slice(which * LIST, which * LIST + LIST)
        columns = col[:, cut]
        rhi_high, rhi_low = two(rhi[:, cut])
        block, lane, low, high, row, upper = spread_out(
            [
                [(columns >> 8).astype(F32).astype(BF)],
                [(columns & 255).astype(F32).astype(BF)],
                [clo[:, cut].astype(BF)],
                [chi[:, cut].astype(BF)],
                [grid_row[:, cut].astype(F32).astype(BF)],
                [rhi_high, rhi_low],
            ]
        )
        block, lane, low, high = [
            jnp.concatenate([x, x], axis=1) for x in (block, lane, low, high)
        ]
        here = iota((LIST, 256), 1).astype(F32)
        reps[which, 0] = block.astype(BF)
        reps[which, 1] = jnp.where(
            here == lane, low, jnp.where(here == lane + 1.0, high, 0.0)
        ).astype(BF)
        reps[which, 2] = jnp.where((lane == 255.0) & (here == 0.0), high, 0.0).astype(BF)
        quarter = (iota((LIST, 128), 1) & 3).astype(F32)
        factor = jnp.where(quarter == row, 1.0 - upper, jnp.where(quarter == row + 1.0, upper, 0.0))
        return factor

    def forward(which, factor, between):
        def build(i):
            for g in range(0, LIST, 64):
                rows = slice(g, g + 64)
                at = reps[which, 0, rows]
                inside = reps[which, 1, rows]
                over = reps[which, 2, rows]
                for j in range(4):
                    b = 4 * i + j
                    tabs[which, b, rows] = jnp.where(
                        at == b, inside, jnp.where(at == b - 1, over, zero)
                    )

        def product(i, half):
            rows = slice(half * HALF, half * HALF + HALF)
            tab = jnp.concatenate([tabs[which, 4 * i + j, rows] for j in range(4)], axis=1)
            return mm_nt(tab, fields_chunk(xv, 8 * i, 8))

        def arrive(i):
            view = xv.at[pl.ds(32 * i, 32)]
            pltpu.make_async_copy(view, view, x_sem.at[i]).wait()

        build(0)
        total = [None, None]
        for i in range(8):
            if which == 1 and i % 4 == 0:
                arrive(i // 4)
            if i < 7:
                build(i + 1)
            if i == 4 and between is not None:
                between()
            for half in range(2):
                part = product(i, half)
                total[half] = part if i == 0 else total[half] + part
        both = []
        for half in range(2):
            scale = factor[half * HALF : half * HALF + HALF]
            both.append(total[half] * jnp.concatenate([scale, scale], axis=1))
        both = jnp.concatenate(both, axis=1)
        high, low = two(both)
        return (mm(high, reduce) + mm(low, reduce)).reshape(OWN, 8, 128)

    factor_b = prepare(1)
    factor_a = []
    mine_b[...] = forward(1, factor_b, lambda: factor_a.append(prepare(0)))
    pl.semaphore_wait(barrier, OWN + 2)
    for d in range(1, 4):
        pl.semaphore_signal(
            plane, inc=1, device_id={"slab": s, "probe": lax.rem(z + d, 4)}, device_id_type=MESH
        )
    to_prev = pltpu.make_async_remote_copy(
        mine_b, next_box, halo_send.at[0], halo_recv.at[0],
        {"slab": lax.rem(s + OWN - 1, OWN), "probe": z}, MESH,
    )
    to_prev.start()
    mine_a[...] = forward(0, factor_a[0], None)
    to_next = pltpu.make_async_remote_copy(
        mine_a, prev_box, halo_send.at[1], halo_recv.at[1],
        {"slab": lax.rem(s + 1, OWN), "probe": z}, MESH,
    )
    to_next.start()
    to_prev.wait_recv()
    complete = mine_a[...] + next_box[...]
    full_a[...] = complete
    value_a = complete.reshape(HALF, 128)
    side = (iota((8, 128), 0) == (iota((8, 128), 1) >> 6)).astype(F32).astype(BF)
    high, low = two(value_a * value_a)
    squares = mm_nt(side, high) + mm_nt(side, low)
    lanes = squares[0:1] * weight[:, 0:HALF] + squares[1:2] * weight[:, HALF:LIST]
    ready[...] = lanes[:, 0:128] + lanes[:, 128:256]
    me = s * 4 + z
    pl.semaphore_wait(plane, 3)

    def send_sum(step):
        pltpu.make_async_remote_copy(
            ready, sums.at[me], sum_send, sum_recv, other(step), MESH
        ).start()

    for step in STEPS:
        send_sum(step)
    sums[me] = ready[...]
    for step in near:
        if step[3] == 0:
            there = other(step)
            pltpu.make_async_remote_copy(
                full_a.at[there["slab"]], box.at[s], own_send, own_recv, there, MESH
            ).start()
    box[s] = full_a[s]
    weighted_source(value_a, weight[:, 0:LIST], weights8[:, 0:LIST], src)
    slabf = (rscr[...].astype(I32) >> 2).astype(F32)
    slot_slab = jnp.sum(jnp.where(iota((32, 128), 0) == s, slabf, 0.0), axis=0, keepdims=True)
    square = jnp.broadcast_to(slot_slab, (128, 128))
    same = (square.T == square) & (iota((128, 128), 0) < iota((128, 128), 1))
    slot_rank = jnp.sum(jnp.where(same, 1.0, 0.0), axis=0, keepdims=True)
    info_ref[0:1] = slot_slab
    info_ref[1:2] = slot_rank
    to_prev.wait_send()

    for i in range(32):
        partial[i] = mm(src[...], tabs[0, i])
    to_next.wait_recv()
    value_b = (mine_b[...] + prev_box[...]).reshape(HALF, 128)
    weighted_source(value_b, weight[:, LIST:], weights8[:, LIST:], src)

    for i in range(32):
        got = (partial[i] + mm(src[...], tabs[1, i])).astype(BF)
        ov[:, :, 256 * i : 256 * i + 256] = got.reshape(64, 4, 256)
    view = box.at[pl.ds(0, OWN - 1)]
    pltpu.make_async_copy(view, view, own_recv).wait()
    box_ref[...] = box[...]
    view = sums.at[pl.ds(0, 127)]
    pltpu.make_async_copy(view, view, sum_recv).wait()
    trace_ref[...] = jnp.sum(sums[...], axis=0) * (1.0 / 1048576.0)
    to_next.wait_send()
    pltpu.make_async_copy(view, view, sum_send).wait()
    view = box.at[pl.ds(0, OWN - 1)]
    pltpu.make_async_copy(view, view, own_send).wait()


def store_kernel(ov, box, info, trace_in, out_ref, obs_ref, trace_ref, sem):
    for c in range(8):
        rows = pl.ds(8 * c, 8)
        pltpu.make_async_copy(ov.at[rows], out_ref.at[rows], sem).start()
    full = box[...].reshape(HALF, 128).T
    slot_slab = info[0:1].astype(I32)
    slot_rank = info[1:2].astype(I32)
    sub = iota((HALF, 128), 0)
    pick = ((sub >> 3) == slot_slab) & ((sub & 7) == (slot_rank & 7))
    pick = jnp.where(pick, 1.0, 0.0).astype(BF)
    high, low = two(full)
    got = mm(high, pick) + mm(low, pick)
    obs_ref[...] = jnp.where(slot_rank < 8, got[0:64], got[64:128])
    trace_ref[0, 0] = jnp.sum(trace_in[...])
    pltpu.make_async_copy(ov, ov, sem).wait()


def run_main(fields, rows, cols, rf, cf, w, order):
    vm = pl.BlockSpec(memory_space=pltpu.VMEM)
    anywhere = pl.BlockSpec(memory_space=pl.ANY)
    dma = pltpu.SemaphoreType.DMA
    sq = lambda x: x.reshape(32, 128)
    block = pltpu.VMEM((OWN, 8, 128), F32)
    return pl.pallas_call(
        main_kernel,
        out_shape=(
            pltpu.VMEM((64, 4, 8192), BF),
            pltpu.VMEM((OWN, 8, 128), F32),
            pltpu.VMEM((8, 128), F32),
            pltpu.VMEM((1, 128), F32),
        ),
        in_specs=[anywhere] * 8,
        out_specs=(vm, vm, vm, vm),
        scratch_shapes=[
            pltpu.VMEM((64, 256, 128), BF),
            pltpu.VMEM((2, 3, LIST, 256), BF),
            pltpu.VMEM((2, 32, LIST, 256), BF),
            pltpu.VMEM((32, 256, 256), F32),
            pltpu.VMEM((256, LIST), BF),
            pltpu.VMEM((32, 128), F32),
            pltpu.VMEM((2, 32, 128), F32),
            pltpu.VMEM((32, 128), I32),
            pltpu.VMEM((1, 4096), I32),
            pltpu.VMEM((32, 128), I32),
            pltpu.VMEM((32, 128), I32),
            pltpu.VMEM((32, 128), F32),
            pltpu.VMEM((32, 128), F32),
            pltpu.VMEM((32, 128), F32),
            block, block, block, block, block, block,
            pltpu.VMEM((128, 1, 128), F32),
            pltpu.VMEM((1, 128), F32),
            dma((2,)), dma((7,)), dma((2,)), dma((2,)), dma, dma, dma, dma, pltpu.SemaphoreType.REGULAR,
        ],
        compiler_params=pltpu.CompilerParams(
            collective_id=0, has_side_effects=True, vmem_limit_bytes=60000000
        ),
        name="main",
    )(fields, sq(order), order.reshape(1, 4096), sq(rows), sq(cols), sq(rf), sq(cf), sq(w))


def run_store(ov, box, info, trace):
    vm = pl.BlockSpec(memory_space=pltpu.VMEM)
    anywhere = pl.BlockSpec(memory_space=pl.ANY)
    return pl.pallas_call(
        store_kernel,
        out_shape=(
            jax.ShapeDtypeStruct((64, 4, 8192), BF),
            jax.ShapeDtypeStruct((64, 128), F32),
            jax.ShapeDtypeStruct((1, 1), F32),
        ),
        in_specs=[vm] * 4,
        out_specs=(anywhere, vm, pl.BlockSpec(memory_space=pltpu.SMEM)),
        scratch_shapes=[pltpu.SemaphoreType.DMA],
        compiler_params=pltpu.CompilerParams(vmem_limit_bytes=8 * 1024 * 1024),
        name="store",
    )(ov, box, info, trace)


def body(fields, rows, cols, rf, cf, w, order):
    ov, box, info, trace = run_main(fields, rows, cols, rf, cf, w, order)
    adjoint, observed, trace = run_store(ov, box, info, trace)
    return adjoint, observed, trace.reshape(())


def solution(mesh):
    return jax.shard_map(
        body,
        mesh=mesh,
        in_specs=(P("probe", "slab", None), P(), P(), P(), P(), P(), P()),
        out_specs=(P("probe", "slab", None), P("probe", "slab"), P()),
        check_vma=False,
    )
```

```python
import jax
import jax.numpy as jnp
from jax import lax
from jax.experimental import pallas as pl
from jax.experimental.pallas import tpu as pltpu
from jax.sharding import PartitionSpec as P

F32 = jnp.float32
BF = jnp.bfloat16
I32 = jnp.int32
MESH = pl.DeviceIdType.MESH

OWN = 32
RANK = 16
LIST = OWN * RANK
HALF = LIST // 2


def iota(shape, dim):
    return lax.broadcasted_iota(I32, shape, dim)


def mm(a, b):
    return lax.dot_general(a, b, (((1,), (0,)), ((), ())), preferred_element_type=F32)


def mm_nt(a, b):
    return lax.dot_general(a, b, (((1,), (1,)), ((), ())), preferred_element_type=F32)


def two(x):
    high = x.astype(BF)
    return high, (x - high.astype(F32)).astype(BF)


def mm_two(a, x):
    high, low = two(x)
    return mm(a, high) + mm(a, low)


def row_weights(row, rhi):
    sub = iota((8, row.shape[1]), 0) % 4
    return jnp.where(sub == row, 1.0 - rhi, 0.0) + jnp.where(sub == row + 1, rhi, 0.0)


def times_rows(x, weights8):
    rows, slots = x.shape
    return (x.reshape(rows // 8, 8, slots) * weights8[None]).reshape(rows, slots)


def prep(s, ord_ref, line_ref, rows_ref, cols_ref, rf_ref, cf_ref, w_ref, rscr, rkscr):
    line = line_ref[...]
    onehot = (iota((128, 4096), 0) == (line & 127)).astype(F32).astype(BF)
    found = mm(rows_ref[...].astype(F32).astype(BF), onehot)
    picked = jnp.where(iota((32, 4096), 0) == (line >> 7), found, 0.0)
    slot_rows = jnp.sum(picked, axis=0, keepdims=True)
    for o in range(OWN):
        rscr[o : o + 1, :] = slot_rows[:, o * 128 : o * 128 + 128]
    rows = rscr[...].astype(I32)
    slab = rows >> 2
    upper = (iota((128, 128), 0) < iota((128, 128), 1)).astype(F32).astype(BF)
    sel = []
    for which in range(2):
        mask = slab == s - which
        maskf = jnp.where(mask, 1.0, 0.0)
        rank = mm(maskf.astype(BF), upper)
        rkscr[which] = jnp.where(mask, rank, -1.0)
    lane8 = iota((8, 128), 0).astype(F32)
    for which in range(2):
        for jh in range(2):
            for o in range(OWN):
                sel.append(jnp.where(rkscr[which, o : o + 1, :] == lane8 + 8.0 * jh, 1.0, 0.0))
    sel = jnp.concatenate(sel, axis=0).astype(BF)
    ids = ord_ref[...]
    parts = jnp.concatenate(
        [(ids >> 7).astype(F32), (ids & 127).astype(F32), jnp.ones((32, 128), F32)], axis=0
    ).astype(BF)
    got = mm_nt(parts, sel)
    mine = iota((32, 1024), 0) == ((iota((32, 1024), 1) & 255) >> 3)
    high = jnp.sum(jnp.where(mine, got[0:32], 0.0), axis=0, keepdims=True)
    low = jnp.sum(jnp.where(mine, got[32:64], 0.0), axis=0, keepdims=True)
    valid = jnp.sum(jnp.where(mine, got[64:96], 0.0), axis=0, keepdims=True) > 0.5
    onehot = (iota((128, 1024), 0).astype(F32) == low).astype(F32).astype(BF)
    cols = cols_ref[...]
    rf_hi, rf_lo = two(rf_ref[...])
    w_hi, w_lo = two(w_ref[...])
    cf = cf_ref[...]
    parts = jnp.concatenate(
        [
            (cols >> 7).astype(F32).astype(BF),
            (cols & 127).astype(F32).astype(BF),
            (1.0 - cf).astype(BF),
            cf.astype(BF),
            rf_hi,
            rf_lo,
            w_hi,
            w_lo,
            rows_ref[...].astype(F32).astype(BF),
        ],
        axis=0,
    )
    got = mm(parts, onehot)
    mine = iota((32, 1024), 0).astype(F32) == high
    vals = [
        jnp.sum(jnp.where(mine, got[32 * i : 32 * i + 32], 0.0), axis=0, keepdims=True)
        for i in range(9)
    ]
    rhi = vals[4] + vals[5]
    weight = vals[6] + vals[7]
    grid_row = vals[8].astype(I32) - 4 * s
    second = iota((1, 1024), 1) >= LIST
    use = valid & ((~second) | (grid_row == -1))
    col = jnp.where(use, (vals[0] * 128.0 + vals[1]).astype(I32), -8)
    grid_row = jnp.where(use, grid_row, -8)
    return col, vals[2], vals[3], grid_row, rhi, weight, rows, slab


def reduce_matrix():
    a = iota((512, 128), 0)
    b = iota((512, 128), 1)
    return (b == ((a >> 8) * 64 + ((a & 255) >> 2))).astype(F32).astype(BF)


def fields_chunk(xv, first, count):
    return jnp.concatenate([xv[first + i] for i in range(count)], axis=1)


def spread_out(rows):
    flat = [r for group in rows for r in group]
    where = [i for i, group in enumerate(rows) for _ in group]
    stack = jnp.concatenate([r.astype(F32) for r in flat], axis=0)
    pad = 16 - len(flat)
    stack = jnp.concatenate([stack, jnp.zeros((pad, stack.shape[1]), F32)], axis=0).astype(BF)
    width = 128 * len(rows)
    a = iota((16, width), 0)
    group = jnp.full((16, width), -1, I32)
    for i, g in enumerate(where):
        group = jnp.where(a == i, g, group)
    pick = (group == (iota((16, width), 1) >> 7)).astype(F32).astype(BF)
    out = lax.dot_general(stack, pick, (((0,), (0,)), ((), ())), preferred_element_type=F32)
    return [out[:, 128 * i : 128 * i + 128] for i in range(len(rows))]


def weighted_source(full, weight, weights8, dst):
    a = iota((256, 128), 0)
    b = iota((256, 128), 1)
    high, low = two(full)
    for jh in range(2):
        cut = slice(jh * HALF, jh * HALF + HALF)
        pick = (b == (jh * 64 + (a >> 2))).astype(F32).astype(BF)
        value = mm_nt(pick, high) + mm_nt(pick, low)
        value = value * weight[:, cut]
        dst[:, cut] = times_rows(value, weights8[:, cut]).astype(BF)


def far_first():
    hops = lambda d: min(d, 4 - d)
    steps = [
        (y, x, c, z) for y in range(4) for x in range(4) for c in range(2) for z in range(4)
    ][1:]
    return sorted(steps, key=lambda d: -(hops(d[0]) + hops(d[1]) + hops(d[3])))


STEPS = far_first()


def main_kernel(
    x_ref, ord_ref, line_ref, rows_ref, cols_ref, rf_ref, cf_ref, w_ref,
    ov, box_ref, info_ref, trace_ref,
    xv, reps, tabs, partial, src, rscr, rkscr,
    ordv, linev, rowsv, colsv, rfv, cfv, wv,
    mine_a, mine_b, full_a, next_box, prev_box, box, sums, ready,
    x_sem, in_sem, halo_send, halo_recv, own_send, own_recv, sum_send, sum_recv, plane,
):
    s = lax.axis_index("slab")
    z = lax.axis_index("probe")
    small = [
        (ord_ref, ordv), (line_ref, linev), (rows_ref, rowsv), (cols_ref, colsv),
        (rf_ref, rfv), (cf_ref, cfv), (w_ref, wv),
    ]
    small = [pltpu.make_async_copy(a, b, in_sem.at[i]) for i, (a, b) in enumerate(small)]
    for copy in small:
        copy.start()
    barrier = pltpu.get_barrier_semaphore()

    place = (s // 8, lax.rem(s // 2, 4), lax.rem(s, 2), z)
    moved = [
        [lax.rem(at + d, length) for d in range(length)]
        for at, length in zip(place, (4, 4, 2, 4))
    ]

    def other(step):
        y, x, core, level = (m[d] for m, d in zip(moved, step))
        return {"slab": y * 8 + x * 2 + core, "probe": level}

    near = [step for step in STEPS if step[3] == 0 or step[:3] == (0, 0, 0)]
    for step in near:
        pl.semaphore_signal(barrier, inc=1, device_id=other(step), device_id_type=MESH)
    flat = x_ref.reshape(256, 8192)
    for c in range(64):
        pltpu.make_async_copy(
            flat.at[:, pl.ds(c * 128, 128)], xv.at[c], x_sem.at[c // 32]
        ).start()
    for copy in small:
        copy.wait()
    col, clo, chi, grid_row, rhi, weight, rows, slab = prep(
        s, ordv, linev, rowsv, colsv, rfv, cfv, wv, rscr, rkscr
    )
    weights8 = row_weights(grid_row, rhi)
    reduce = reduce_matrix()
    zero = jnp.zeros((), BF)

    def prepare(which):
        cut = slice(which * LIST, which * LIST + LIST)
        columns = col[:, cut]
        rhi_high, rhi_low = two(rhi[:, cut])
        block, lane, low, high, row, upper = spread_out(
            [
                [(columns >> 8).astype(F32).astype(BF)],
                [(columns & 255).astype(F32).astype(BF)],
                [clo[:, cut].astype(BF)],
                [chi[:, cut].astype(BF)],
                [grid_row[:, cut].astype(F32).astype(BF)],
                [rhi_high, rhi_low],
            ]
        )
        block, lane, low, high = [
            jnp.concatenate([x, x], axis=1) for x in (block, lane, low, high)
        ]
        here = iota((LIST, 256), 1).astype(F32)
        reps[which, 0] = block.astype(BF)
        reps[which, 1] = jnp.where(
            here == lane, low, jnp.where(here == lane + 1.0, high, 0.0)
        ).astype(BF)
        reps[which, 2] = jnp.where((lane == 255.0) & (here == 0.0), high, 0.0).astype(BF)
        quarter = (iota((LIST, 128), 1) & 3).astype(F32)
        factor = jnp.where(quarter == row, 1.0 - upper, jnp.where(quarter == row + 1.0, upper, 0.0))
        return factor

    def forward(which, factor, between):
        def build(i):
            for g in range(0, LIST, 64):
                rows = slice(g, g + 64)
                at = reps[which, 0, rows]
                inside = reps[which, 1, rows]
                over = reps[which, 2, rows]
                for j in range(4):
                    b = 4 * i + j
                    tabs[which, b, rows] = jnp.where(
                        at == b, inside, jnp.where(at == b - 1, over, zero)
                    )

        def product(i, half):
            rows = slice(half * HALF, half * HALF + HALF)
            tab = jnp.concatenate([tabs[which, 4 * i + j, rows] for j in range(4)], axis=1)
            return mm_nt(tab, fields_chunk(xv, 8 * i, 8))

        def arrive(i):
            view = xv.at[pl.ds(32 * i, 32)]
            pltpu.make_async_copy(view, view, x_sem.at[i]).wait()

        build(0)
        total = [None, None]
        for i in range(8):
            if which == 1 and i % 4 == 0:
                arrive(i // 4)
            if i < 7:
                build(i + 1)
            if i == 4 and between is not None:
                between()
            for half in range(2):
                part = product(i, half)
                total[half] = part if i == 0 else total[half] + part
        both = []
        for half in range(2):
            scale = factor[half * HALF : half * HALF + HALF]
            both.append(total[half] * jnp.concatenate([scale, scale], axis=1))
        both = jnp.concatenate(both, axis=1)
        high, low = two(both)
        return (mm(high, reduce) + mm(low, reduce)).reshape(OWN, 8, 128)

    factor_b = prepare(1)
    mine_b[...] = forward(1, factor_b, None)
    pl.semaphore_wait(barrier, OWN + 2)
    for d in range(1, 4):
        pl.semaphore_signal(
            plane, inc=1, device_id={"slab": s, "probe": lax.rem(z + d, 4)}, device_id_type=MESH
        )
    to_prev = pltpu.make_async_remote_copy(
        mine_b, next_box, halo_send.at[0], halo_recv.at[0],
        {"slab": lax.rem(s + OWN - 1, OWN), "probe": z}, MESH,
    )
    to_prev.start()
    factor_a = prepare(0)
    mine_a[...] = forward(0, factor_a, None)
    to_next = pltpu.make_async_remote_copy(
        mine_a, prev_box, halo_send.at[1], halo_recv.at[1],
        {"slab": lax.rem(s + 1, OWN), "probe": z}, MESH,
    )
    to_next.start()
    to_prev.wait_recv()
    complete = mine_a[...] + next_box[...]
    full_a[...] = complete
    value_a = complete.reshape(HALF, 128)
    side = (iota((8, 128), 0) == (iota((8, 128), 1) >> 6)).astype(F32).astype(BF)
    high, low = two(value_a * value_a)
    squares = mm_nt(side, high) + mm_nt(side, low)
    lanes = squares[0:1] * weight[:, 0:HALF] + squares[1:2] * weight[:, HALF:LIST]
    ready[...] = lanes[:, 0:128] + lanes[:, 128:256]
    me = s * 4 + z
    pl.semaphore_wait(plane, 3)

    def send_sum(step):
        pltpu.make_async_remote_copy(
            ready, sums.at[me], sum_send, sum_recv, other(step), MESH
        ).start()

    for step in STEPS:
        send_sum(step)
    sums[me] = ready[...]
    for step in near:
        if step[3] == 0:
            there = other(step)
            pltpu.make_async_remote_copy(
                full_a.at[there["slab"]], box.at[s], own_send, own_recv, there, MESH
            ).start()
    box[s] = full_a[s]
    weighted_source(value_a, weight[:, 0:LIST], weights8[:, 0:LIST], src)
    slabf = (rscr[...].astype(I32) >> 2).astype(F32)
    slot_slab = jnp.sum(jnp.where(iota((32, 128), 0) == s, slabf, 0.0), axis=0, keepdims=True)
    square = jnp.broadcast_to(slot_slab, (128, 128))
    same = (square.T == square) & (iota((128, 128), 0) < iota((128, 128), 1))
    slot_rank = jnp.sum(jnp.where(same, 1.0, 0.0), axis=0, keepdims=True)
    info_ref[0:1] = slot_slab
    info_ref[1:2] = slot_rank
    to_prev.wait_send()

    for i in range(32):
        partial[i] = mm(src[...], tabs[0, i])
    to_next.wait_recv()
    value_b = (mine_b[...] + prev_box[...]).reshape(HALF, 128)
    weighted_source(value_b, weight[:, LIST:], weights8[:, LIST:], src)

    for i in range(32):
        got = (partial[i] + mm(src[...], tabs[1, i])).astype(BF)
        ov[:, :, 256 * i : 256 * i + 256] = got.reshape(64, 4, 256)
    view = box.at[pl.ds(0, OWN - 1)]
    pltpu.make_async_copy(view, view, own_recv).wait()
    box_ref[...] = box[...]
    view = sums.at[pl.ds(0, 127)]
    pltpu.make_async_copy(view, view, sum_recv).wait()
    trace_ref[...] = jnp.sum(sums[...], axis=0) * (1.0 / 1048576.0)
    to_next.wait_send()
    pltpu.make_async_copy(view, view, sum_send).wait()
    view = box.at[pl.ds(0, OWN - 1)]
    pltpu.make_async_copy(view, view, own_send).wait()


def store_kernel(ov, box, info, trace_in, out_ref, obs_ref, trace_ref, sem):
    for c in range(8):
        rows = pl.ds(8 * c, 8)
        pltpu.make_async_copy(ov.at[rows], out_ref.at[rows], sem).start()
    full = box[...].reshape(HALF, 128).T
    slot_slab = info[0:1].astype(I32)
    slot_rank = info[1:2].astype(I32)
    sub = iota((HALF, 128), 0)
    pick = ((sub >> 3) == slot_slab) & ((sub & 7) == (slot_rank & 7))
    pick = jnp.where(pick, 1.0, 0.0).astype(BF)
    high, low = two(full)
    got = mm(high, pick) + mm(low, pick)
    obs_ref[...] = jnp.where(slot_rank < 8, got[0:64], got[64:128])
    trace_ref[0, 0] = jnp.sum(trace_in[...])
    pltpu.make_async_copy(ov, ov, sem).wait()


def run_main(fields, rows, cols, rf, cf, w, order):
    vm = pl.BlockSpec(memory_space=pltpu.VMEM)
    anywhere = pl.BlockSpec(memory_space=pl.ANY)
    dma = pltpu.SemaphoreType.DMA
    sq = lambda x: x.reshape(32, 128)
    block = pltpu.VMEM((OWN, 8, 128), F32)
    return pl.pallas_call(
        main_kernel,
        out_shape=(
            pltpu.VMEM((64, 4, 8192), BF),
            pltpu.VMEM((OWN, 8, 128), F32),
            pltpu.VMEM((8, 128), F32),
            pltpu.VMEM((1, 128), F32),
        ),
        in_specs=[anywhere] * 8,
        out_specs=(vm, vm, vm, vm),
        scratch_shapes=[
            pltpu.VMEM((64, 256, 128), BF),
            pltpu.VMEM((2, 3, LIST, 256), BF),
            pltpu.VMEM((2, 32, LIST, 256), BF),
            pltpu.VMEM((32, 256, 256), F32),
            pltpu.VMEM((256, LIST), BF),
            pltpu.VMEM((32, 128), F32),
            pltpu.VMEM((2, 32, 128), F32),
            pltpu.VMEM((32, 128), I32),
            pltpu.VMEM((1, 4096), I32),
            pltpu.VMEM((32, 128), I32),
            pltpu.VMEM((32, 128), I32),
            pltpu.VMEM((32, 128), F32),
            pltpu.VMEM((32, 128), F32),
            pltpu.VMEM((32, 128), F32),
            block, block, block, block, block, block,
            pltpu.VMEM((128, 1, 128), F32),
            pltpu.VMEM((1, 128), F32),
            dma((2,)), dma((7,)), dma((2,)), dma((2,)), dma, dma, dma, dma, pltpu.SemaphoreType.REGULAR,
        ],
        compiler_params=pltpu.CompilerParams(
            collective_id=0, has_side_effects=True, vmem_limit_bytes=60000000
        ),
        name="main",
    )(fields, sq(order), order.reshape(1, 4096), sq(rows), sq(cols), sq(rf), sq(cf), sq(w))


def run_store(ov, box, info, trace):
    vm = pl.BlockSpec(memory_space=pltpu.VMEM)
    anywhere = pl.BlockSpec(memory_space=pl.ANY)
    return pl.pallas_call(
        store_kernel,
        out_shape=(
            jax.ShapeDtypeStruct((64, 4, 8192), BF),
            jax.ShapeDtypeStruct((64, 128), F32),
            jax.ShapeDtypeStruct((1, 1), F32),
        ),
        in_specs=[vm] * 4,
        out_specs=(anywhere, vm, pl.BlockSpec(memory_space=pltpu.SMEM)),
        scratch_shapes=[pltpu.SemaphoreType.DMA],
        compiler_params=pltpu.CompilerParams(vmem_limit_bytes=8 * 1024 * 1024),
        name="store",
    )(ov, box, info, trace)


def body(fields, rows, cols, rf, cf, w, order):
    ov, box, info, trace = run_main(fields, rows, cols, rf, cf, w, order)
    adjoint, observed, trace = run_store(ov, box, info, trace)
    return adjoint, observed, trace.reshape(())


def solution(mesh):
    return jax.shard_map(
        body,
        mesh=mesh,
        in_specs=(P("probe", "slab", None), P(), P(), P(), P(), P(), P()),
        out_specs=(P("probe", "slab", None), P("probe", "slab"), P()),
        check_vma=False,
    )
```
